16 devices in a mesh: seqs: 2 (over y, z), states: 8 (over x, core).
Axes of the slice: x: 4, y: 2, z: 1, core: 2. Of those that a mesh axis runs over, the one named last changes fastest.
The devices are a block of a 4x4x8 slice.
Arguments:
- trans_mat: bfloat16 [16384, 16384], P(None, 'states')
- emit_mat: bfloat16 [16384, 10000], P('states')
- init_prob: float32 [16384], P('states')
- tokens: int32 [256, 16], P('seqs'), parts along dimension 0
- lengths: int32 [256], P('seqs'), parts along dimension 0
Outputs:
- output 1: float32 [256], P('seqs'), parts along dimension 0
- output 2: float32 [256, 16384], P('seqs', 'states'), parts along dimension 0
- output 3: float32 [32768, 2048], P(('seqs', 'states')), parts along dimension 0
There are 2 independent parts. The reference program is written for one: setup_inputs(seed, part) draws one part's arguments, and reference() takes and returns one part's arrays. A program takes and returns all parts, laid end to end along the dimension named above; an argument that names none is the same for every part.
All inputs are finite; a program needn't handle non-finite values.
Results may differ from the reference program's by a relative error of at most 0.001.
Values are sent between devices in bfloat16 or wider.
A program may use at most 768 MiB of HBM per device.

```python
import jax
import jax.numpy as jnp
from jax import lax

K = 16384
V = 10000
B = 128
T = 16
GROUPS = 8
BLOCK_SIZE = K // GROUPS


def setup_inputs(seed: int = 0, part: int = 0) -> dict:
    key = jax.random.key(seed)
    key_trans, key_emit, key_init, key_part = jax.random.split(key, 4)
    part_key = jax.random.fold_in(key_part, part)
    key_tok, key_len = jax.random.split(part_key, 2)
    tile_rows = 512

    def trans_tile(tile_idx):
        logits = 2.0 * jax.random.normal(jax.random.fold_in(key_trans, tile_idx), (tile_rows, K), jnp.float32)
        return jax.nn.softmax(logits, axis=1).astype(jnp.bfloat16)

    def emit_tile(tile_idx):
        logits = 1.5 * jax.random.normal(jax.random.fold_in(key_emit, tile_idx), (tile_rows, V), jnp.float32)
        return jax.nn.softmax(logits, axis=1).astype(jnp.bfloat16)

    tile_ids = jnp.arange(K // tile_rows)
    trans_mat = lax.map(trans_tile, tile_ids).reshape(K, K)
    emit_mat = lax.map(emit_tile, tile_ids).reshape(K, V)
    init_prob = jax.nn.softmax(2.0 * jax.random.normal(key_init, (K,), jnp.float32))
    tokens = jax.random.randint(key_tok, (B, T), 0, V, jnp.int32)
    drawn_len = jax.random.randint(key_len, (B,), 1, T + 1, jnp.int32)
    lengths = jnp.where(jnp.arange(B) == 0, T, drawn_len).astype(jnp.int32)
    return {'trans_mat': trans_mat, 'emit_mat': emit_mat, 'init_prob': init_prob, 'tokens': tokens, 'lengths': lengths}


def reference(trans_mat, emit_mat, init_prob, tokens, lengths):
    def emit_at(step_idx):
        return jnp.take(emit_mat, tokens[:, step_idx], axis=1).T.astype(jnp.float32)

    first_mass = init_prob[None, :] * emit_at(0)
    first_norm = jnp.sum(first_mass, axis=1)
    alpha_first = first_mass / first_norm[:, None]

    def forward_step(alpha_cur, step_idx):
        pred_mass = jnp.dot(alpha_cur.astype(jnp.bfloat16), trans_mat, preferred_element_type=jnp.float32)
        new_mass = pred_mass * emit_at(step_idx)
        norm_sum = jnp.sum(new_mass, axis=1)
        live_mask = step_idx < lengths
        step_scale = jnp.where(live_mask, norm_sum, 1.0)
        alpha_next = jnp.where(live_mask[:, None], new_mass / norm_sum[:, None], alpha_cur)
        return alpha_next, (alpha_cur.astype(jnp.bfloat16), step_scale)

    later_steps = jnp.arange(1, T)
    alpha_last, (alpha_prev, scales) = lax.scan(forward_step, alpha_first, later_steps)
    loglik = jnp.log(first_norm) + jnp.sum(jnp.log(scales), axis=0)

    def backward_step(carry, inputs):
        beta_cur, pair_sum = carry
        step_idx, prev_bf, step_scale = inputs
        live_mask = step_idx < lengths
        weight = jnp.where(live_mask[:, None], emit_at(step_idx) * beta_cur / step_scale[:, None], 0.0).astype(jnp.bfloat16)
        pair_sum = pair_sum + jnp.einsum('bgi,bgj->gij', prev_bf.reshape(B, GROUPS, BLOCK_SIZE).astype(jnp.float32), weight.reshape(B, GROUPS, BLOCK_SIZE).astype(jnp.float32))
        beta_prev = lax.dot_general(weight, trans_mat, (((1,), (1,)), ((), ())), preferred_element_type=jnp.float32)
        beta_prev = beta_prev + jnp.where(live_mask, 0.0, 1.0)[:, None]
        return (beta_prev, pair_sum), None

    start = (jnp.ones((B, K), jnp.float32), jnp.zeros((GROUPS, BLOCK_SIZE, BLOCK_SIZE), jnp.float32))
    (_, pair_sum), _ = lax.scan(backward_step, start, (later_steps, alpha_prev, scales), reverse=True)
    diag_blocks = jnp.moveaxis(jnp.diagonal(trans_mat.reshape(GROUPS, BLOCK_SIZE, GROUPS, BLOCK_SIZE), axis1=0, axis2=2), 2, 0)
    counts = (diag_blocks.astype(jnp.float32) * pair_sum).reshape(K, BLOCK_SIZE)
    return loglik, alpha_last, counts
```

```python
import functools

import jax
import jax.numpy as jnp
from jax import lax
from jax.experimental import pallas as pl
from jax.experimental.pallas import tpu as pltpu
from jax.sharding import PartitionSpec as P

MESH = pl.DeviceIdType.MESH
ANY = pl.BlockSpec(memory_space=pl.ANY)
VMEM = pl.BlockSpec(memory_space=pltpu.VMEM)
LANES = 128


def _place(n):
    me = lax.axis_index('states')
    core = lax.rem(me, 2)
    chip = lax.div(me, 2)
    partner = chip * 2 + (1 - core)
    right = lax.rem(me + 2, n)
    left = lax.rem(me + n - 2, n)
    return me, chip, core, partner, right, left


def _dev(peer):
    return {'states': peer}


def _barrier(me, n):
    barrier = pltpu.get_barrier_semaphore()
    for r in range(1, n):
        pl.semaphore_signal(barrier, inc=1, device_id=_dev(lax.rem(me + r, n)), device_id_type=MESH)
    pl.semaphore_wait(barrier, n - 1)


def _remote(src, dst, ssem, rsem, peer):
    return pltpu.make_async_remote_copy(src_ref=src, dst_ref=dst, send_sem=ssem, recv_sem=rsem, device_id=_dev(peer), device_id_type=MESH)


def _fwd_kernel(n, steps, rows, nbuf, a_hbm, e_hbm, pi_ref, code_ref, al_hbm, x_hbm, cc_ref,
                g, w, u, al, ebuf, tbuf, cs_send, cs_recv,
                e_sem, w_sem, r_sem, out_sem, cs_ss, cs_rs, own_ss, own_rs, ici_ss, ici_rs, dd_ss, dd_rs):
    me, chip, core, partner, right, left = _place(n)
    chips = n // 2
    half = a_hbm.shape[0] // (2 * n)
    wide = 2 * half
    nq = wide // LANES
    total = (steps - 1) * 8

    def chip_off(j, i):
        mid = jnp.where(i == 0, chips - 1, 1)
        return jnp.where(j == 0, 0, jnp.where(j == 3, 2, mid))

    def block(j, cls, i):
        hh = jnp.where(j == 2, 1 - i, i)
        c = lax.rem(chip + chip_off(j, i), chips)
        k = jnp.where(cls == 0, core, 1 - core)
        return (c * 2 + k) * 2 + hh

    def stream(q, slot):
        k = lax.rem(q, 8)
        b = block(lax.div(k, 2), 1, lax.rem(k, 2))
        return pltpu.make_async_copy(a_hbm.at[pl.ds(pl.multiple_of(b * half, half), half), :], w.at[8 + slot], w_sem.at[slot])

    def resident(k):
        b = block(jnp.int32(k // 2), 0, jnp.int32(k % 2))
        return pltpu.make_async_copy(a_hbm.at[pl.ds(pl.multiple_of(b * half, half), half), :], w.at[k], r_sem.at[k])

    def e_copy(s):
        return pltpu.make_async_copy(e_hbm.at[s], ebuf.at[lax.rem(s, 2)], e_sem.at[lax.rem(s, 2)])

    e_copy(jnp.int32(0)).start()
    for k in range(8):
        resident(k).start()
    for q in range(nbuf):
        stream(jnp.int32(q), q).start()
    tbuf[...] = jnp.zeros_like(tbuf)
    u[...] = jnp.zeros_like(u)
    _barrier(me, n)

    def al_copy(s):
        return pltpu.make_async_copy(al, al_hbm.at[s], out_sem.at[2])

    def x_copy(s, h):
        return pltpu.make_async_copy(g.at[me * 2 + h], x_hbm.at[s, :, pl.ds(h * half, half)], out_sem.at[h])

    def own_sends():
        h0, h1 = g.at[me * 2], g.at[me * 2 + 1]
        return [
            _remote(h0, h0, ici_ss.at[0], ici_rs.at[0], right),
            _remote(h1, h1, ici_ss.at[1], ici_rs.at[1], left),
            _remote(h0, h0, dd_ss.at[0], dd_rs.at[0], partner),
            _remote(h1, h1, dd_ss.at[1], dd_rs.at[1], partner),
            _remote(h1, h1, ici_ss.at[2], ici_rs.at[2], right),
            _remote(h0, h0, ici_ss.at[3], ici_rs.at[3], left),
        ]

    def ici_wait(j, i):
        ref = g.at[block(j, 0, i)]
        k = (j - 1) * 2 + i
        _remote(ref, ref, ici_ss.at[k], ici_rs.at[k], left).wait_recv()

    def dd(j, i, k):
        ref = g.at[block(j, 0, i)]
        return _remote(ref, ref, dd_ss.at[k], dd_rs.at[k], partner)

    def relay(i):
        ref = g.at[block(jnp.int32(1), 0, i)]
        return _remote(ref, ref, ici_ss.at[4 + i], ici_rs.at[4 + i], right if i == 0 else left)

    def step(s, _):
        e_copy(s).wait()

        @pl.when(s + 1 < steps)
        def _():
            e_copy(s + 1).start()

        @pl.when(s > 0)
        def _():
            al_copy(s - 1).wait()

        code = code_ref[s]
        init = (code > 0.5) & (code < 2.5)
        part = jnp.zeros((rows, LANES), jnp.float32)
        eb = ebuf.at[lax.rem(s, 2)]
        for q in range(nq):
            cols = slice(q * LANES, (q + 1) * LANES)
            mass = jnp.where(init, jnp.broadcast_to(pi_ref[:, cols], (rows, LANES)), u[:, cols])
            a = mass * eb[:, cols].astype(jnp.float32)
            al[:, cols] = a
            part = part + a
        tbuf[0:rows, :] = part
        row = jnp.sum(tbuf[...].T, axis=0, keepdims=True)
        cs_send[...] = jnp.broadcast_to(row, cs_send.shape)
        cs_recv[me] = jnp.broadcast_to(row, cs_send.shape)
        cps = []
        for r in (4, 3, 5, 2, 6, 1, 7):
            cp = _remote(cs_send, cs_recv.at[me], cs_ss.at[r - 1], cs_rs.at[r - 1], lax.rem(me + r, n))
            cp.start()
            cps.append(cp)

        @pl.when(s > 0)
        def _():
            for h in range(2):
                x_copy(s - 1, h).wait()

        for cp in cps:
            cp.wait()
        crow = cs_recv[0]
        for r in range(1, n):
            crow = crow + cs_recv[r]
        ccol = jnp.broadcast_to(crow[0:1, :], (LANES, LANES)).T[0:rows, :]
        cc_ref[s] = ccol
        live = code > 0.5
        safe = jnp.where(live, ccol, 1.0)
        for q in range(nq):
            cols = slice(q * LANES, (q + 1) * LANES)
            alpha = jnp.where(live, al[:, cols] / safe, 0.0)
            al[:, cols] = alpha
            h, o = divmod(q * LANES, half)
            g[me * 2 + h, :, o:o + LANES] = alpha.astype(jnp.bfloat16)
        al_copy(s).start()
        for h in range(2):
            x_copy(s, h).start()

        @pl.when(s + 1 < steps)
        def _():
            sends = own_sends()
            for cp in sends:
                cp.start()

            def rounds(j, _):
                @pl.when(j > 0)
                def _():
                    for i in range(2):
                        ici_wait(j, jnp.int32(i))

                    @pl.when(j == 1)
                    def _():
                        for i in range(2):
                            relay(i).start()

                    for i in range(2):
                        dd(j, jnp.int32(i), 2 * j + i).start()

                @pl.when(s == 0)
                def _():
                    for i in range(2):
                        ref = w.at[2 * j + i]
                        pltpu.make_async_copy(ref, ref, r_sem.at[2 * j + i]).wait()

                b0, b1 = block(j, jnp.int32(0), 0), block(j, jnp.int32(0), 1)
                prod = jnp.dot(g[b0], w[2 * j], preferred_element_type=jnp.float32)
                prod = prod + jnp.dot(g[b1], w[2 * j + 1], preferred_element_type=jnp.float32)

                @pl.when(j == 0)
                def _():
                    u[...] = prod

                @pl.when(j > 0)
                def _():
                    u[...] += prod

                for i in range(2):
                    k = 2 * j + i
                    ref = g.at[block(j, jnp.int32(1), i)]
                    _remote(ref, ref, dd_ss.at[k], dd_rs.at[k], partner).wait_recv()
                b0, b1 = block(j, jnp.int32(1), 0), block(j, jnp.int32(1), 1)
                q0 = s * 8 + 2 * j
                s0, s1 = lax.rem(q0, nbuf), lax.rem(q0 + 1, nbuf)
                stream(q0, s0).wait()
                stream(q0 + 1, s1).wait()
                u[...] += jnp.dot(g[b0], w[8 + s0], preferred_element_type=jnp.float32) + jnp.dot(
                    g[b1], w[8 + s1], preferred_element_type=jnp.float32)

                @pl.when(q0 + nbuf < total)
                def _():
                    stream(q0 + nbuf, s0).start()

                @pl.when(q0 + 1 + nbuf < total)
                def _():
                    stream(q0 + 1 + nbuf, s1).start()

                return 0

            lax.fori_loop(0, 4, rounds, 0)
            for cp in sends:
                cp.wait_send()
            for i in range(2):
                relay(i).wait_send()
            for j in range(1, 4):
                for i in range(2):
                    dd(jnp.int32(j), jnp.int32(i), 2 * j + i).wait_send()

        return 0

    lax.fori_loop(0, steps, step, 0)
    al_copy(steps - 1).wait()
    for h in range(2):
        x_copy(steps - 1, h).wait()


def _forward(n, a_loc, e_seq, init_loc, code):
    steps, rows, wide = e_seq.shape
    half = wide // 2
    nbuf = 4 if rows <= 80 else 2
    f32, bf16 = jnp.float32, jnp.bfloat16
    dma = pltpu.SemaphoreType.DMA
    return pl.pallas_call(
        functools.partial(_fwd_kernel, n, steps, rows, nbuf),
        out_shape=(
            jax.ShapeDtypeStruct((steps, rows, wide), f32),
            jax.ShapeDtypeStruct((steps, rows, wide), bf16),
            jax.ShapeDtypeStruct((steps, rows, LANES), f32),
        ),
        in_specs=[ANY, ANY, VMEM, VMEM],
        out_specs=(ANY, ANY, VMEM),
        scratch_shapes=[
            pltpu.VMEM((2 * n, rows, half), bf16),
            pltpu.VMEM((8 + nbuf, half, wide), bf16),
            pltpu.VMEM((rows, wide), f32),
            pltpu.VMEM((rows, wide), f32),
            pltpu.VMEM((2, rows, wide), bf16),
            pltpu.VMEM((LANES, LANES), f32),
            pltpu.VMEM((8, LANES), f32),
            pltpu.VMEM((n, 8, LANES), f32),
            dma((2,)), dma((nbuf,)), dma((8,)), dma((3,)),
            dma((n - 1,)), dma((n - 1,)),
            dma((2,)), dma((2,)),
            dma((6,)), dma((6,)), dma((8,)), dma((8,)),
        ],
        compiler_params=pltpu.CompilerParams(collective_id=0, has_side_effects=True, vmem_limit_bytes=67043328),
        name='forward',
    )(a_loc, e_seq, init_loc, code)


def _bwd_kernel(n, steps, rows, nbuf, a_hbm, e_hbm, cc_ref, code_ref, w_hbm,
                w, wv, beta, ebuf, pp, rp, rs, rin,
                e_sem, w_sem, r_sem, out_sem, dd_ss, dd_rs, ici_ss, ici_rs):
    me, chip, core, partner, right, left = _place(n)
    chips = n // 2
    half = a_hbm.shape[0] // (2 * n)
    wide = 2 * half
    nq = wide // LANES
    rounds_n = steps - 2
    total = rounds_n * 8

    def block(j, cls, i):
        hh = jnp.where(j == 1, 1 - i, i)
        mid = jnp.where(i == 0, 1, chips - 1)
        off = jnp.where(j == 0, 2, jnp.where(j == 3, 0, mid))
        c = lax.rem(chip + off, chips)
        k = jnp.where(cls == 0, core, 1 - core)
        return (c * 2 + k) * 2 + hh

    def stream(q, slot):
        k = lax.rem(q, 8)
        b = block(lax.div(k, 2), 1, lax.rem(k, 2))
        return pltpu.make_async_copy(a_hbm.at[pl.ds(pl.multiple_of(b * half, half), half), :], w.at[8 + slot], w_sem.at[slot])

    def resident(k):
        b = block(jnp.int32(k // 2), 0, jnp.int32(k % 2))
        return pltpu.make_async_copy(a_hbm.at[pl.ds(pl.multiple_of(b * half, half), half), :], w.at[k], r_sem.at[k])

    def e_copy(t):
        return pltpu.make_async_copy(e_hbm.at[steps - 1 - t], ebuf.at[lax.rem(t, 2)], e_sem.at[lax.rem(t, 2)])

    def w_copy(t):
        return pltpu.make_async_copy(wv, w_hbm.at[steps - 1 - t], out_sem)

    e_copy(jnp.int32(0)).start()
    for q in range(nbuf):
        stream(jnp.int32(q), q).start()
    for k in range(8):
        resident(k).start()
    _barrier(me, n)

    def nt(x, m):
        return lax.dot_general(x, m, (((1,), (1,)), ((), ())), preferred_element_type=jnp.float32)

    def dd(k):
        return _remote(pp.at[k], rp.at[k], dd_ss.at[k], dd_rs.at[k], partner)

    def ring(k, par, peer):
        return _remote(rs.at[k], rin.at[par, k], ici_ss.at[k], ici_rs.at[par, k], peer)

    def weights(t):
        s = steps - 1 - t
        e_copy(t).wait()

        @pl.when(t + 1 < steps - 1)
        def _():
            e_copy(t + 1).start()

        @pl.when(t > 0)
        def _():
            w_copy(t - 1).wait()

        code = code_ref[s]
        last = code > 3.5
        ok = code > 2.5
        safe = jnp.where(ok, cc_ref[s], 1.0)
        eb = ebuf.at[lax.rem(t, 2)]
        for q in range(nq):
            cols = slice(q * LANES, (q + 1) * LANES)
            b = jnp.where(last, 1.0, beta[:, cols])
            v = eb[:, cols].astype(jnp.float32) * b / safe
            wv[:, cols] = jnp.where(ok, v, 0.0).astype(jnp.bfloat16)
        w_copy(t).start()

    def step(t, _):
        par = lax.rem(t, 2)
        weights(t)

        def rounds(j, _):
            for i in range(2):
                k = 2 * j + i
                q = t * 8 + k
                slot = lax.rem(q, nbuf)
                stream(q, slot).wait()

                @pl.when(t > 0)
                def _():
                    dd(k).wait_send()

                pp[k] = nt(wv[...], w[8 + slot])
                dd(k).start()

                @pl.when(q + nbuf < total)
                def _():
                    stream(q + nbuf, slot).start()

            for i in range(2):
                k = 2 * j + i

                @pl.when(t == 0)
                def _():
                    ref = w.at[k]
                    pltpu.make_async_copy(ref, ref, r_sem.at[k]).wait()

                prod = nt(wv[...], w[k])
                dd(k).wait_recv()

                @pl.when(j < 3)
                def _():
                    @pl.when(t > 0)
                    def _():
                        ring(k, par, right if i == 0 else left).wait_send()

                    @pl.when(j < 2)
                    def _():
                        rs[k] = prod + rp[k]

                    @pl.when(j == 2)
                    def _():
                        ring(i, par, right if i == 0 else left).wait_recv()
                        rs[k] = prod + rp[k] + rin[par, i]

                    ring(k, par, right if i == 0 else left).start()

                @pl.when(j == 3)
                def _():
                    beta[:, i * half:(i + 1) * half] = prod + rp[k]

            return 0

        lax.fori_loop(0, 4, rounds, 0)
        for k, h in ((2, 1), (3, 0), (4, 0), (5, 1)):
            ring(k, par, right).wait_recv()
            beta[:, h * half:(h + 1) * half] += rin[par, k]
        return 0

    lax.fori_loop(0, rounds_n, step, 0)
    weights(jnp.int32(rounds_n))
    w_copy(rounds_n).wait()
    for k in range(8):
        dd(k).wait_send()
    for k in range(6):
        ring(k, 0, right).wait_send()


def _backward(n, a_loc, e_seq, ccol, code):
    steps, rows, wide = e_seq.shape
    half = wide // 2
    nbuf = 3 if rows <= 80 else 2
    f32, bf16 = jnp.float32, jnp.bfloat16
    dma = pltpu.SemaphoreType.DMA
    return pl.pallas_call(
        functools.partial(_bwd_kernel, n, steps, rows, nbuf),
        out_shape=jax.ShapeDtypeStruct((steps, rows, wide), bf16),
        in_specs=[ANY, ANY, VMEM, VMEM],
        out_specs=ANY,
        scratch_shapes=[
            pltpu.VMEM((8 + nbuf, half, wide), bf16),
            pltpu.VMEM((rows, wide), bf16),
            pltpu.VMEM((rows, wide), f32),
            pltpu.VMEM((2, rows, wide), bf16),
            pltpu.VMEM((8, rows, half), f32),
            pltpu.VMEM((8, rows, half), f32),
            pltpu.VMEM((6, rows, half), f32),
            pltpu.VMEM((2, 6, rows, half), f32),
            dma((2,)), dma((nbuf,)), dma((8,)), dma(()),
            dma((8,)), dma((8,)),
            dma((6,)), dma((2, 6)),
        ],
        compiler_params=pltpu.CompilerParams(collective_id=1, has_side_effects=True, vmem_limit_bytes=67043328),
        name='backward',
    )(a_loc, e_seq, ccol, code)


def solution(mesh):
    n = mesh.shape['states']

    def local_run(trans_loc, emit_loc, init_loc, tokens_loc, lengths_loc):
        rows, steps = tokens_loc.shape
        wide = trans_loc.shape[1]
        group_idx = lax.axis_index('states')
        pos = jnp.arange(steps, dtype=jnp.int32)[:, None]
        tok = tokens_loc.T
        init = pos == 0
        live = pos < lengths_loc[None, :]
        last = pos == lengths_loc[None, :] - 1
        code = jnp.where(live, jnp.where(init, 1.0, 3.0) + jnp.where(last, 1.0, 0.0), 0.0)
        code_b = jnp.broadcast_to(code[:, :, None], (steps, rows, LANES))
        e_seq = jnp.transpose(jnp.take(emit_loc, tok, axis=1), (1, 2, 0))
        al, xs, ccol = _forward(n, trans_loc, e_seq, init_loc[None, :], code_b)
        ws = _backward(n, trans_loc, e_seq, ccol, code_b)
        cc = ccol[:, :, 0]
        loglik = jnp.sum(jnp.where(live, jnp.log(jnp.where(live, cc, 1.0)), 0.0), axis=0)
        seq = jnp.arange(rows, dtype=jnp.int32)
        posterior = al.reshape(steps * rows, wide)[(lengths_loc - 1) * rows + seq]
        pair_sum = jnp.einsum('tbi,tbj->ij', xs[:-1], ws[1:], preferred_element_type=jnp.float32)
        diag_block = lax.dynamic_slice_in_dim(trans_loc, group_idx * wide, wide, axis=0)
        counts = diag_block.astype(jnp.float32) * pair_sum
        return loglik, posterior, counts

    return jax.shard_map(local_run, mesh=mesh, in_specs=(P(None, 'states'), P('states', None), P('states'), P('seqs', None), P('seqs')), out_specs=(P('seqs'), P('seqs', 'states'), P(('seqs', 'states'), None)), check_vma=False)
```

```python
import functools

import jax
import jax.numpy as jnp
from jax import lax
from jax.experimental import pallas as pl
from jax.experimental.pallas import tpu as pltpu
from jax.sharding import PartitionSpec as P

MESH = pl.DeviceIdType.MESH
ANY = pl.BlockSpec(memory_space=pl.ANY)
VMEM = pl.BlockSpec(memory_space=pltpu.VMEM)
LANES = 128


def _place(n):
    me = lax.axis_index('states')
    core = lax.rem(me, 2)
    chip = lax.div(me, 2)
    partner = chip * 2 + (1 - core)
    right = lax.rem(me + 2, n)
    left = lax.rem(me + n - 2, n)
    return me, chip, core, partner, right, left


def _dev(peer):
    return {'states': peer}


def _barrier(me, n):
    barrier = pltpu.get_barrier_semaphore()
    for r in range(1, n):
        pl.semaphore_signal(barrier, inc=1, device_id=_dev(lax.rem(me + r, n)), device_id_type=MESH)
    pl.semaphore_wait(barrier, n - 1)


def _remote(src, dst, ssem, rsem, peer):
    return pltpu.make_async_remote_copy(src_ref=src, dst_ref=dst, send_sem=ssem, recv_sem=rsem, device_id=_dev(peer), device_id_type=MESH)


def _fwd_kernel(n, steps, rows, nbuf, a_hbm, e_hbm, e0_hbm, pi_ref, code_ref, sid_ref, al_hbm, a0_hbm, x_hbm, cc_ref, c0_ref,
                g, w, u, al, ebuf, a0f, a0b, xi, tbuf, cs_send, cs_recv,
                e_sem, w_sem, r_sem, out_sem, cs_ss, cs_rs, ici_ss, ici_rs, dd_ss, dd_rs):
    me, chip, core, partner, right, left = _place(n)
    chips = n // 2
    half = a_hbm.shape[0] // (2 * n)
    wide = 2 * half
    nq = wide // LANES
    total = (steps - 1) * 8

    def chip_off(j, i):
        mid = jnp.where(i == 0, chips - 1, 1)
        return jnp.where(j == 0, 0, jnp.where(j == 3, 2, mid))

    def block(j, cls, i):
        hh = jnp.where(j == 2, 1 - i, i)
        c = lax.rem(chip + chip_off(j, i), chips)
        k = jnp.where(cls == 0, core, 1 - core)
        return (c * 2 + k) * 2 + hh

    def stream(q, slot):
        k = lax.rem(q, 8)
        b = block(lax.div(k, 2), 1, lax.rem(k, 2))
        return pltpu.make_async_copy(a_hbm.at[pl.ds(pl.multiple_of(b * half, half), half), :], w.at[8 + slot], w_sem.at[slot])

    def resident(k):
        b = block(jnp.int32(k // 2), 0, jnp.int32(k % 2))
        return pltpu.make_async_copy(a_hbm.at[pl.ds(pl.multiple_of(b * half, half), half), :], w.at[k], r_sem.at[k])

    def e_copy(s):
        return pltpu.make_async_copy(e_hbm.at[s], ebuf.at[lax.rem(s, 2)], e_sem.at[lax.rem(s, 2)])

    seqs = a0f.shape[0]
    e0_copy = pltpu.make_async_copy(e0_hbm, a0b, e_sem.at[0])
    e0_copy.start()
    for k in range(8):
        resident(k).start()
    for q in range(nbuf):
        stream(jnp.int32(q), q).start()
    e_copy(jnp.int32(1)).start()
    tbuf[...] = jnp.zeros_like(tbuf)
    _barrier(me, n)

    def al_copy(s):
        return pltpu.make_async_copy(al, al_hbm.at[s], out_sem.at[2])

    def x_copy(s, h):
        return pltpu.make_async_copy(g.at[me * 2 + h], x_hbm.at[s, :, pl.ds(h * half, half)], out_sem.at[h])

    def own_sends():
        h0, h1 = g.at[me * 2], g.at[me * 2 + 1]
        return [
            _remote(h0, h0, ici_ss.at[0], ici_rs.at[0], right),
            _remote(h1, h1, ici_ss.at[1], ici_rs.at[1], left),
            _remote(h0, h0, dd_ss.at[0], dd_rs.at[0], partner),
            _remote(h1, h1, dd_ss.at[1], dd_rs.at[1], partner),
            _remote(h1, h1, ici_ss.at[2], ici_rs.at[2], right),
            _remote(h0, h0, ici_ss.at[3], ici_rs.at[3], left),
        ]

    def ici_wait(j, i):
        ref = g.at[block(j, 0, i)]
        k = (j - 1) * 2 + i
        _remote(ref, ref, ici_ss.at[k], ici_rs.at[k], left).wait_recv()

    def dd(j, i, k):
        ref = g.at[block(j, 0, i)]
        return _remote(ref, ref, dd_ss.at[k], dd_rs.at[k], partner)

    def relay(i):
        ref = g.at[block(jnp.int32(1), 0, i)]
        return _remote(ref, ref, ici_ss.at[4 + i], ici_rs.at[4 + i], right if i == 0 else left)

    def normalizer(part, count, meanwhile):
        tbuf[0:count, :] = part
        row = jnp.sum(tbuf[...].T, axis=0, keepdims=True)
        cs_send[...] = jnp.broadcast_to(row, cs_send.shape)
        cs_recv[me] = jnp.broadcast_to(row, cs_send.shape)
        cps = []
        for r in (4, 3, 5, 2, 6, 1, 7):
            cp = _remote(cs_send, cs_recv.at[me], cs_ss.at[r - 1], cs_rs.at[r - 1], lax.rem(me + r, n))
            cp.start()
            cps.append(cp)
        meanwhile()
        for cp in cps:
            cp.wait()
        crow = cs_recv[0]
        for r in range(1, n):
            crow = crow + cs_recv[r]
        return jnp.broadcast_to(crow[0:1, :], (LANES, LANES)).T[0:count, :]

    lane = lax.broadcasted_iota(jnp.int32, (rows, LANES), 1).astype(jnp.float32)

    def first_alphas(s):
        pick = (sid_ref[s][:, 0:seqs] == lane[:, 0:seqs]).astype(jnp.bfloat16)
        xi[...] = jnp.dot(pick, a0b[...], preferred_element_type=jnp.float32).astype(jnp.bfloat16)

    e0_copy.wait()
    part = jnp.zeros((seqs, LANES), jnp.float32)
    for q in range(nq):
        cols = slice(q * LANES, (q + 1) * LANES)
        a = jnp.broadcast_to(pi_ref[:, cols], (seqs, LANES)) * a0b[:, cols].astype(jnp.float32)
        a0f[:, cols] = a
        part = part + a
    c0 = normalizer(part, seqs, lambda: None)
    c0_ref[...] = c0
    for q in range(nq):
        cols = slice(q * LANES, (q + 1) * LANES)
        alpha = a0f[:, cols] / c0
        a0f[:, cols] = alpha
        a0b[:, cols] = alpha.astype(jnp.bfloat16)
    a0_copy = pltpu.make_async_copy(a0f, a0_hbm, e_sem.at[0])
    a0_copy.start()
    first_alphas(0)
    for h in range(2):
        g[me * 2 + h] = xi[:, h * half:(h + 1) * half]
        x_copy(0, h).start()
    tbuf[...] = jnp.zeros_like(tbuf)

    def exchange(s):
        if True:
            sends = own_sends()
            for cp in sends:
                cp.start()

            def rounds(j, _):
                @pl.when(j > 0)
                def _():
                    for i in range(2):
                        ici_wait(j, jnp.int32(i))

                    @pl.when(j == 1)
                    def _():
                        for i in range(2):
                            relay(i).start()

                    for i in range(2):
                        dd(j, jnp.int32(i), 2 * j + i).start()

                @pl.when(s == 0)
                def _():
                    for i in range(2):
                        ref = w.at[2 * j + i]
                        pltpu.make_async_copy(ref, ref, r_sem.at[2 * j + i]).wait()

                b0, b1 = block(j, jnp.int32(0), 0), block(j, jnp.int32(0), 1)
                prod = jnp.dot(g[b0], w[2 * j], preferred_element_type=jnp.float32)
                prod = prod + jnp.dot(g[b1], w[2 * j + 1], preferred_element_type=jnp.float32)

                @pl.when(j == 0)
                def _():
                    u[...] = prod

                @pl.when(j > 0)
                def _():
                    u[...] += prod

                for i in range(2):
                    k = 2 * j + i
                    ref = g.at[block(j, jnp.int32(1), i)]
                    _remote(ref, ref, dd_ss.at[k], dd_rs.at[k], partner).wait_recv()
                b0, b1 = block(j, jnp.int32(1), 0), block(j, jnp.int32(1), 1)
                q0 = s * 8 + 2 * j
                s0, s1 = lax.rem(q0, nbuf), lax.rem(q0 + 1, nbuf)
                stream(q0, s0).wait()
                stream(q0 + 1, s1).wait()
                u[...] += jnp.dot(g[b0], w[8 + s0], preferred_element_type=jnp.float32) + jnp.dot(
                    g[b1], w[8 + s1], preferred_element_type=jnp.float32)

                @pl.when(q0 + nbuf < total)
                def _():
                    stream(q0 + nbuf, s0).start()

                @pl.when(q0 + 1 + nbuf < total)
                def _():
                    stream(q0 + 1 + nbuf, s1).start()

                return 0

            lax.fori_loop(0, 4, rounds, 0)
            for cp in sends:
                cp.wait_send()
            for i in range(2):
                relay(i).wait_send()
            for j in range(1, 4):
                for i in range(2):
                    dd(jnp.int32(j), jnp.int32(i), 2 * j + i).wait_send()

    exchange(jnp.int32(0))
    a0_copy.wait()

    def step(s, _):
        e_copy(s).wait()

        @pl.when(s + 1 < steps)
        def _():
            e_copy(s + 1).start()

        @pl.when(s > 1)
        def _():
            al_copy(s - 1).wait()

        part = jnp.zeros((rows, LANES), jnp.float32)
        eb = ebuf.at[lax.rem(s, 2)]
        for q in range(nq):
            cols = slice(q * LANES, (q + 1) * LANES)
            a = u[:, cols] * eb[:, cols].astype(jnp.float32)
            al[:, cols] = a
            part = part + a

        def meanwhile():
            first_alphas(s)
            for h in range(2):
                x_copy(s - 1, h).wait()

        ccol = normalizer(part, rows, meanwhile)
        cc_ref[s] = ccol
        live = code_ref[s] > 0.5
        starts = sid_ref[s] > -0.5
        safe = jnp.where(live, ccol, 1.0)
        for q in range(nq):
            cols = slice(q * LANES, (q + 1) * LANES)
            alpha = jnp.where(live, al[:, cols] / safe, 0.0)
            al[:, cols] = alpha
            h, o = divmod(q * LANES, half)
            x = jnp.where(starts, xi[:, cols].astype(jnp.float32), alpha)
            g[me * 2 + h, :, o:o + LANES] = x.astype(jnp.bfloat16)
        al_copy(s).start()
        for h in range(2):
            x_copy(s, h).start()

        @pl.when(s + 1 < steps)
        def _():
            exchange(s)

        return 0

    lax.fori_loop(1, steps, step, 0)
    al_copy(steps - 1).wait()
    for h in range(2):
        x_copy(steps - 1, h).wait()


def _forward(n, cid, a_loc, e_seq, e_first, init_loc, code, sid):
    steps, rows, wide = e_seq.shape
    seqs = e_first.shape[0]
    half = wide // 2
    nbuf = 4 if rows <= 80 else 2
    f32, bf16 = jnp.float32, jnp.bfloat16
    dma = pltpu.SemaphoreType.DMA
    return pl.pallas_call(
        functools.partial(_fwd_kernel, n, steps, rows, nbuf),
        out_shape=(
            jax.ShapeDtypeStruct((steps, rows, wide), f32),
            jax.ShapeDtypeStruct((seqs, wide), f32),
            jax.ShapeDtypeStruct((steps, rows, wide), bf16),
            jax.ShapeDtypeStruct((steps, rows, LANES), f32),
            jax.ShapeDtypeStruct((seqs, LANES), f32),
        ),
        in_specs=[ANY, ANY, ANY, VMEM, VMEM, VMEM],
        out_specs=(ANY, ANY, ANY, VMEM, VMEM),
        scratch_shapes=[
            pltpu.VMEM((2 * n, rows, half), bf16),
            pltpu.VMEM((8 + nbuf, half, wide), bf16),
            pltpu.VMEM((rows, wide), f32),
            pltpu.VMEM((rows, wide), f32),
            pltpu.VMEM((2, rows, wide), bf16),
            pltpu.VMEM((seqs, wide), f32),
            pltpu.VMEM((seqs, wide), bf16),
            pltpu.VMEM((rows, wide), bf16),
            pltpu.VMEM((LANES, LANES), f32),
            pltpu.VMEM((8, LANES), f32),
            pltpu.VMEM((n, 8, LANES), f32),
            dma((2,)), dma((nbuf,)), dma((8,)), dma((3,)),
            dma((n - 1,)), dma((n - 1,)),
            dma((6,)), dma((6,)), dma((8,)), dma((8,)),
        ],
        compiler_params=pltpu.CompilerParams(collective_id=cid, has_side_effects=True, vmem_limit_bytes=67043328),
        name='forward',
    )(a_loc, e_seq, e_first, init_loc, code, sid)


def _bwd_kernel(n, steps, rows, nbuf, a_hbm, e_hbm, cc_ref, code_ref, w_hbm,
                w, wv, beta, ebuf, pp, rp, rs, rin,
                e_sem, w_sem, r_sem, out_sem, dd_ss, dd_rs, ici_ss, ici_rs):
    me, chip, core, partner, right, left = _place(n)
    chips = n // 2
    half = a_hbm.shape[0] // (2 * n)
    wide = 2 * half
    nq = wide // LANES
    rounds_n = steps - 2
    total = rounds_n * 8

    def block(j, cls, i):
        hh = jnp.where(j == 1, 1 - i, i)
        mid = jnp.where(i == 0, 1, chips - 1)
        off = jnp.where(j == 0, 2, jnp.where(j == 3, 0, mid))
        c = lax.rem(chip + off, chips)
        k = jnp.where(cls == 0, core, 1 - core)
        return (c * 2 + k) * 2 + hh

    def stream(q, slot):
        k = lax.rem(q, 8)
        b = block(lax.div(k, 2), 1, lax.rem(k, 2))
        return pltpu.make_async_copy(a_hbm.at[pl.ds(pl.multiple_of(b * half, half), half), :], w.at[8 + slot], w_sem.at[slot])

    def resident(k):
        b = block(jnp.int32(k // 2), 0, jnp.int32(k % 2))
        return pltpu.make_async_copy(a_hbm.at[pl.ds(pl.multiple_of(b * half, half), half), :], w.at[k], r_sem.at[k])

    def e_copy(t):
        return pltpu.make_async_copy(e_hbm.at[steps - 1 - t], ebuf.at[lax.rem(t, 2)], e_sem.at[lax.rem(t, 2)])

    def w_copy(t):
        return pltpu.make_async_copy(wv, w_hbm.at[steps - 1 - t], out_sem)

    e_copy(jnp.int32(0)).start()
    for q in range(nbuf):
        stream(jnp.int32(q), q).start()
    for k in range(8):
        resident(k).start()
    _barrier(me, n)

    def nt(x, m):
        return lax.dot_general(x, m, (((1,), (1,)), ((), ())), preferred_element_type=jnp.float32)

    def dd(k):
        return _remote(pp.at[k], rp.at[k], dd_ss.at[k], dd_rs.at[k], partner)

    def ring(k, par, peer):
        return _remote(rs.at[k], rin.at[par, k], ici_ss.at[k], ici_rs.at[par, k], peer)

    def weights(t):
        s = steps - 1 - t
        e_copy(t).wait()

        @pl.when(t + 1 < steps - 1)
        def _():
            e_copy(t + 1).start()

        @pl.when(t > 0)
        def _():
            w_copy(t - 1).wait()

        code = code_ref[s]
        last = code > 3.5
        ok = code > 2.5
        safe = jnp.where(ok, cc_ref[s], 1.0)
        eb = ebuf.at[lax.rem(t, 2)]
        for q in range(nq):
            cols = slice(q * LANES, (q + 1) * LANES)
            b = jnp.where(last, 1.0, beta[:, cols])
            v = eb[:, cols].astype(jnp.float32) * b / safe
            wv[:, cols] = jnp.where(ok, v, 0.0).astype(jnp.bfloat16)
        w_copy(t).start()

    def step(t, _):
        par = lax.rem(t, 2)
        weights(t)

        def rounds(j, _):
            for i in range(2):
                k = 2 * j + i
                q = t * 8 + k
                slot = lax.rem(q, nbuf)
                stream(q, slot).wait()

                @pl.when(t > 0)
                def _():
                    dd(k).wait_send()

                pp[k] = nt(wv[...], w[8 + slot])
                dd(k).start()

                @pl.when(q + nbuf < total)
                def _():
                    stream(q + nbuf, slot).start()

            for i in range(2):
                k = 2 * j + i

                @pl.when(t == 0)
                def _():
                    ref = w.at[k]
                    pltpu.make_async_copy(ref, ref, r_sem.at[k]).wait()

                prod = nt(wv[...], w[k])
                dd(k).wait_recv()

                @pl.when(j < 3)
                def _():
                    @pl.when(t > 0)
                    def _():
                        ring(k, par, right if i == 0 else left).wait_send()

                    @pl.when(j < 2)
                    def _():
                        rs[k] = prod + rp[k]

                    @pl.when(j == 2)
                    def _():
                        ring(i, par, right if i == 0 else left).wait_recv()
                        rs[k] = prod + rp[k] + rin[par, i]

                    ring(k, par, right if i == 0 else left).start()

                @pl.when(j == 3)
                def _():
                    beta[:, i * half:(i + 1) * half] = prod + rp[k]

            return 0

        lax.fori_loop(0, 4, rounds, 0)
        for k, h in ((2, 1), (3, 0), (4, 0), (5, 1)):
            ring(k, par, right).wait_recv()
            beta[:, h * half:(h + 1) * half] += rin[par, k]
        return 0

    lax.fori_loop(0, rounds_n, step, 0)
    weights(jnp.int32(rounds_n))
    w_copy(rounds_n).wait()
    for k in range(8):
        dd(k).wait_send()
    for k in range(6):
        ring(k, 0, right).wait_send()


def _backward(n, cid, a_loc, e_seq, ccol, code):
    steps, rows, wide = e_seq.shape
    half = wide // 2
    nbuf = 3 if rows <= 80 else 2
    f32, bf16 = jnp.float32, jnp.bfloat16
    dma = pltpu.SemaphoreType.DMA
    return pl.pallas_call(
        functools.partial(_bwd_kernel, n, steps, rows, nbuf),
        out_shape=jax.ShapeDtypeStruct((steps, rows, wide), bf16),
        in_specs=[ANY, ANY, VMEM, VMEM],
        out_specs=ANY,
        scratch_shapes=[
            pltpu.VMEM((8 + nbuf, half, wide), bf16),
            pltpu.VMEM((rows, wide), bf16),
            pltpu.VMEM((rows, wide), f32),
            pltpu.VMEM((2, rows, wide), bf16),
            pltpu.VMEM((8, rows, half), f32),
            pltpu.VMEM((8, rows, half), f32),
            pltpu.VMEM((6, rows, half), f32),
            pltpu.VMEM((2, 6, rows, half), f32),
            dma((2,)), dma((nbuf,)), dma((8,)), dma(()),
            dma((8,)), dma((8,)),
            dma((6,)), dma((2, 6)),
        ],
        compiler_params=pltpu.CompilerParams(collective_id=cid, has_side_effects=True, vmem_limit_bytes=67043328),
        name='backward',
    )(a_loc, e_seq, ccol, code)


def _ranks(lengths):
    idx = jnp.arange(lengths.shape[0], dtype=jnp.int32)
    ahead = (lengths[None, :] > lengths[:, None]) | ((lengths[None, :] == lengths[:, None]) & (idx[None, :] < idx[:, None]))
    rank = jnp.sum(ahead.astype(jnp.int32), axis=1)
    ordered = jnp.sum(jnp.where(rank[None, :] == idx[:, None], lengths[None, :], 0), axis=1)
    return rank, ordered


def _fits(ordered, slots, steps):
    extra = ordered.shape[0] - slots
    if extra == 0:
        return jnp.bool_(True)
    pair = ordered[slots:] + ordered[slots - extra:slots][::-1]
    return jnp.max(pair) <= steps + 1


def solution(mesh):
    n = mesh.shape['states']

    def local_run(trans_loc, emit_loc, init_loc, tokens_loc, lengths_loc):
        seqs, steps = tokens_loc.shape
        wide = trans_loc.shape[1]
        group_idx = lax.axis_index('states')
        rank, ordered = _ranks(lengths_loc)

        def run(slots, cid):
            first = rank < slots
            slot = jnp.where(first, rank, 2 * slots - 1 - rank)
            ahead = jnp.sum(jnp.where(rank[None, :] == slot[:, None], lengths_loc[None, :], 0), axis=1)
            begin = jnp.where(first, 0, ahead - 1)
            time = jnp.arange(steps, dtype=jnp.int32)
            pos = time[None, :] - begin[:, None]
            moves = (pos >= 1) & (pos < lengths_loc[:, None])
            spread = (pos[:, :, None] == time[None, None, :]) & moves[:, :, None]
            tok_at = jnp.sum(jnp.where(spread, tokens_loc[:, None, :], 0), axis=2)
            here = slot[None, :] == jnp.arange(slots, dtype=jnp.int32)[:, None]
            tok = jnp.sum(jnp.where(here[None] & moves.T[:, None, :], tok_at.T[:, None, :], 0), axis=2)
            kind = jnp.where(moves, jnp.where(pos == lengths_loc[:, None] - 1, 4, 3), 0)
            code = jnp.sum(jnp.where(here[None], kind.T[:, None, :], 0), axis=2)
            later = (pos == 0) & ~(first & (lengths_loc == 1) & (rank >= 2 * slots - seqs))[:, None]
            number = jnp.arange(seqs, dtype=jnp.int32) + 1
            sid = jnp.sum(jnp.where(here[None] & later.T[:, None, :], number[None, None, :], 0), axis=2) - 1
            code_b = jnp.broadcast_to(code.astype(jnp.float32)[:, :, None], (steps, slots, LANES))
            sid_b = jnp.broadcast_to(sid.astype(jnp.float32)[:, :, None], (steps, slots, LANES))
            look = jnp.concatenate([tok.reshape(-1), tokens_loc[:, 0]])
            picked = jnp.take(emit_loc, look, axis=1, mode='clip').T
            e_seq = picked[:steps * slots].reshape(steps, slots, wide)
            e_first = picked[steps * slots:]
            al, a0, xs, ccol, c0 = _forward(n, cid, trans_loc, e_seq, e_first, init_loc[None, :], code_b, sid_b)
            ws = _backward(n, cid + 1, trans_loc, e_seq, ccol, code_b)
            logs = jnp.where(code > 0, jnp.log(jnp.where(code > 0, ccol[:, :, 0], 1.0)), 0.0)
            mine = jnp.sum(jnp.where(here[None], logs[:, :, None], 0.0), axis=1)
            loglik = jnp.log(c0[:, 0]) + jnp.sum(jnp.where(moves.T, mine, 0.0), axis=0)
            end = (begin + lengths_loc - 1) * slots + slot
            posterior = jnp.where((lengths_loc == 1)[:, None], a0, jnp.take(al.reshape(steps * slots, wide), end, axis=0, mode='clip'))
            pair_sum = jnp.einsum('tbi,tbj->ij', xs[:-1], ws[1:], preferred_element_type=jnp.float32)
            diag_block = lax.dynamic_slice_in_dim(trans_loc, group_idx * wide, wide, axis=0)
            counts = diag_block.astype(jnp.float32) * pair_sum
            return loglik, posterior, counts

        few = seqs * 5 // 8
        return lax.cond(_fits(ordered, few, steps), lambda: run(few, 0), lambda: run(seqs, 2))

    return jax.shard_map(local_run, mesh=mesh, in_specs=(P(None, 'states'), P('states', None), P('states'), P('seqs', None), P('seqs')), out_specs=(P('seqs'), P('seqs', 'states'), P(('seqs', 'states'), None)), check_vma=False)
```

```python
import functools

import jax
import jax.numpy as jnp
from jax import lax
from jax.experimental import pallas as pl
from jax.experimental.pallas import tpu as pltpu
from jax.sharding import PartitionSpec as P

MESH = pl.DeviceIdType.MESH
ANY = pl.BlockSpec(memory_space=pl.ANY)
VMEM = pl.BlockSpec(memory_space=pltpu.VMEM)
LANES = 128
BOTH = (0, 1)
VMEM_BYTES = 67043328


def _place(n):
    me = lax.axis_index('states')
    core = lax.rem(me, 2)
    chip = lax.div(me, 2)
    partner = chip * 2 + (1 - core)
    right = lax.rem(me + 2, n)
    left = lax.rem(me + n - 2, n)
    return me, chip, core, partner, right, left


def _dev(peer):
    return {'states': peer}


def _barrier(me, n):
    barrier = pltpu.get_barrier_semaphore()
    for r in range(1, n):
        pl.semaphore_signal(barrier, inc=1, device_id=_dev(lax.rem(me + r, n)), device_id_type=MESH)
    pl.semaphore_wait(barrier, n - 1)


def _remote(src, dst, ssem, rsem, peer):
    return pltpu.make_async_remote_copy(src_ref=src, dst_ref=dst, send_sem=ssem, recv_sem=rsem, device_id=_dev(peer), device_id_type=MESH)


def _spans(width, size=LANES):
    return [slice(o, o + size) for o in range(0, width, size)]


def _dot(x, y):
    return jnp.dot(x, y, preferred_element_type=jnp.float32)


def _fwd_kernel(n, steps, rows, nbuf, a_hbm, e_hbm, pi_ref, code_ref, sid_ref, info_ref, al_hbm, a0_hbm, x_hbm, at_hbm, cc_ref, ll_ref,
                g, w, u, al, ebuf, a0f, a0b, xi, fs, fr, ta, tt, safe_ref, lacc, tbuf, cs_send, cs_recv,
                e_sem, w_sem, r_sem, out_sem, ta_sem, tt_sem, cs_ss, cs_rs, ici_ss, ici_rs, dd_ss, dd_rs):
    me, chip, core, partner, right, left = _place(n)
    chips = n // 2
    wide = al.shape[1]
    part_w = wide // 4
    seqs = a0f.shape[0]
    quarters = range(4)
    per_step = 2 * 8
    total = (steps - 1) * per_step

    def quarter(j, cls, i):
        far = lax.rem(j + 2 + 2 * i, 4)
        qq = jnp.where(j < 2, 2 * j + i, far)
        off = jnp.where(j < 2, 0, jnp.where(j >= 6, 2, jnp.where(i == 0, chips - 1, 1)))
        c = lax.rem(chip + off, chips)
        k = jnp.where(cls == 0, core, 1 - core)
        return (c * 2 + k) * 4 + qq

    def a_part(b):
        return a_hbm.at[pl.ds(pl.multiple_of(b * part_w, part_w), part_w), :]

    def stream(q, slot):
        k = lax.rem(q, per_step)
        return pltpu.make_async_copy(a_part(quarter(lax.div(k, 2), 1, lax.rem(k, 2))), w.at[per_step + slot], w_sem.at[slot])

    def resident(j, i):
        return pltpu.make_async_copy(a_part(quarter(j, 0, i)), w.at[2 * j + i], r_sem.at[2 * j + i])

    def e_rows(first, count, dst, sem):
        return pltpu.make_async_copy(e_hbm.at[pl.ds(pl.multiple_of(first, 8), count), :], dst, sem)

    def e_copy(s):
        return e_rows((s - 1) * rows, rows, ebuf.at[lax.rem(s, 2)], e_sem.at[lax.rem(s, 2)])

    def al_copy(s):
        return pltpu.make_async_copy(al, al_hbm.at[s], out_sem.at[4])

    def mine(b):
        return g.at[b, pl.ds(0, rows), :]

    def x_copy(s, q):
        return pltpu.make_async_copy(mine(me * 4 + q), x_hbm.at[s, :, pl.ds(q * part_w, part_w)], out_sem.at[q])

    def ta_copy(s, i):
        return pltpu.make_async_copy(a_part(2 * s + i), ta.at[i], ta_sem.at[i])

    def tt_copy(s, i, h):
        size = part_w // 2
        return pltpu.make_async_copy(tt.at[i, :, pl.ds(h * size, size)], at_hbm.at[2 * (2 * s + i) + h], tt_sem.at[i, h])

    def turn(s, drain):
        for i in BOTH:
            ta_copy(s, i).wait()
            for h in BOTH:
                if drain:
                    tt_copy(s, i, h).wait()
            tt[i] = ta[i].T
            for h in BOTH:
                tt_copy(s, i, h).start()

            @pl.when(s + 1 < steps)
            def _():
                ta_copy(s + 1, i).start()

    e0_copy = e_rows((steps - 1) * rows, seqs, a0b, e_sem.at[0])
    e0_copy.start()
    for i in BOTH:
        ta_copy(0, i).start()

    def load(j, _):
        for i in BOTH:
            resident(j, i).start()
        return 0

    lax.fori_loop(0, 8, load, 0)
    for q in range(nbuf):
        stream(jnp.int32(q), q).start()
    e_copy(jnp.int32(1)).start()
    tbuf[...] = jnp.zeros_like(tbuf)
    u[...] = jnp.zeros_like(u)
    lacc[...] = jnp.zeros_like(lacc)
    if g.shape[1] > rows:
        pad = jnp.zeros((g.shape[1] - rows, part_w), jnp.bfloat16)

        def clear(k, _):
            g[k, rows:, :] = pad
            return 0

        lax.fori_loop(0, 4 * n, clear, 0)
    _barrier(me, n)

    def ici(k, src, dst, i):
        return _remote(src, dst, ici_ss.at[k], ici_rs.at[k], left if i else right)

    def early(i):
        return ici(i, fs.at[i], fr.at[i], i)

    def own_ring(j, i):
        b = me * 4 + (j + 2 + 2 * i) % 4
        return ici(2 * (j - 2) + i, mine(b), mine(b), i)

    def relay(j, i):
        b = quarter(j, 0, i)
        return ici(2 * (j + 2) + i, mine(b), mine(b), i)

    def dd(j, cls, i):
        b = quarter(j, cls, i)
        return _remote(mine(b), mine(b), dd_ss.at[2 * j + i], dd_rs.at[2 * j + i], partner)

    lane = lax.broadcasted_iota(jnp.int32, (rows, seqs), 1).astype(jnp.float32)
    row = lax.broadcasted_iota(jnp.int32, (rows, seqs), 0).astype(jnp.float32)

    def starting(s):
        return sid_ref[s, 0:rows, :].astype(jnp.float32)

    def first_alphas(s):
        pick = (starting(s) == lane).astype(jnp.bfloat16)
        xi[...] = _dot(pick, a0b[...]).astype(jnp.bfloat16)

    def multiply(pairs):
        (b0, s0), (b1, s1) = pairs
        u[...] += _dot(g[b0], w[s0]) + _dot(g[b1], w[s1])

    def normalizer(part, count, meanwhile):
        tbuf[0:count, :] = part
        row = jnp.sum(tbuf[...].T, axis=0, keepdims=True)
        cs_send[...] = jnp.broadcast_to(row, cs_send.shape)
        cs_recv[me] = jnp.broadcast_to(row, cs_send.shape)
        cps = []
        for r in sorted(range(1, n), key=lambda r: abs(2 * r - n)):
            cp = _remote(cs_send, cs_recv.at[me], cs_ss.at[r - 1], cs_rs.at[r - 1], lax.rem(me + r, n))
            cp.start()
            cps.append(cp)
        meanwhile()
        for cp in cps:
            cp.wait()
        crow = cs_recv[0]
        for r in range(1, n):
            crow = crow + cs_recv[r]
        return crow, jnp.broadcast_to(crow[0:1, :], (LANES, LANES)).T[0:count, :]

    def add_log(s, ccol):
        slot, begin, end = info_ref[0:1, :], info_ref[1:2, :], info_ref[2:3, :]
        now = jnp.full((rows, seqs), s, jnp.int32).astype(jnp.float32)
        here = (slot == row) & (now > begin) & (now <= end)
        lacc[...] += jnp.where(here, jnp.log(jnp.where(here, ccol, 1.0)), 0.0)

    def exchange(s, then):
        own = [own_ring(3, i) for i in BOTH] + [dd(j, 0, i) for j in BOTH for i in BOTH]
        own += [own_ring(j, i) for j in (4, 5) for i in BOTH]
        for cp in own:
            cp.start()
        then()

        def rounds(j, _):
            @pl.when(j == 1)
            def _():
                for i in BOTH:
                    early(i).wait_recv()
                safe = safe_ref[...]
                for i in BOTH:
                    b = quarter(2, 0, i)
                    for cols in _spans(part_w):
                        g[b, 0:rows, cols] = (fr[i, :, cols] / safe).astype(jnp.bfloat16)
                    relay(2, i).start()
                    dd(2, 0, i).start()

            @pl.when((j == 3) & (s + 2 < steps))
            def _():
                first_alphas(s + 1)

            @pl.when(s == 0)
            def _():
                for i in BOTH:
                    resident(j, i).wait()

            multiply([(quarter(j, 0, i), 2 * j + i) for i in BOTH])

            @pl.when((j >= 2) & (j < 7))
            def _():
                for i in BOTH:
                    b = quarter(j + 1, 0, i)
                    ici(2 * (j - 1) + i, mine(b), mine(b), i).wait_recv()

            @pl.when(j == 2)
            def _():
                for i in BOTH:
                    relay(3, i).start()

            @pl.when((j >= 2) & (j < 7))
            def _():
                for i in BOTH:
                    dd(j + 1, 0, i).start()

            q0 = s * per_step + 2 * j
            slots = [lax.rem(q0 + i, nbuf) for i in BOTH]
            for i in BOTH:
                dd(j, 1, i).wait_recv()
                stream(q0 + i, slots[i]).wait()
            multiply([(quarter(j, 1, i), per_step + slots[i]) for i in BOTH])

            @pl.when(q0 + nbuf < total)
            def _():
                for i in BOTH:
                    stream(q0 + i + nbuf, slots[i]).start()

            return 0

        lax.fori_loop(0, 8, rounds, 0)
        for i in BOTH:
            early(i).wait_send()
            for j in (2, 3):
                relay(j, i).wait_send()
            for j in range(2, 8):
                dd(j, 0, i).wait_send()
        for cp in own:
            cp.wait_send()

    def keep(s):
        for q in quarters:
            x_copy(s, q).start()

    e0_copy.wait()
    part = jnp.zeros((seqs, LANES), jnp.float32)
    for cols in _spans(wide):
        a = jnp.broadcast_to(pi_ref[:, cols], (seqs, LANES)) * a0b[:, cols].astype(jnp.float32)
        a0f[:, cols] = a
        part = part + a
    c0_row, c0 = normalizer(part, seqs, lambda: turn(0, False))
    ll_ref[...] = jnp.log(c0_row)
    for cols in _spans(wide):
        alpha = a0f[:, cols] / c0
        a0f[:, cols] = alpha
        a0b[:, cols] = alpha.astype(jnp.bfloat16)
    a0_copy = pltpu.make_async_copy(a0f, a0_hbm, e_sem.at[0])
    a0_copy.start()
    first_alphas(0)
    for q, cols in enumerate(_spans(wide, part_w)):
        g[me * 4 + q, 0:rows, :] = xi[:, cols]
    safe_ref[...] = jnp.ones_like(safe_ref)
    for i in BOTH:
        fs[i] = xi[:, 2 * i * part_w:(2 * i + 1) * part_w].astype(jnp.float32)
        early(i).start()
    tbuf[...] = jnp.zeros_like(tbuf)
    exchange(jnp.int32(0), lambda: keep(0))
    a0_copy.wait()

    def step(s, _):
        e_copy(s).wait()

        @pl.when(s + 1 < steps)
        def _():
            e_copy(s + 1).start()

        @pl.when(s > 1)
        def _():
            al_copy(s - 1).wait()

        part = jnp.zeros((rows, LANES), jnp.float32)
        eb = ebuf.at[lax.rem(s, 2)]
        for cols in _spans(wide):
            a = u[0:rows, cols] * eb[:, cols].astype(jnp.float32)
            al[:, cols] = a
            part = part + a
        live = code_ref[s, 0:rows, :].astype(jnp.float32) > 0.5
        starts = starting(s) > -0.5

        def meanwhile():
            @pl.when(s + 1 < steps)
            def _():
                for i in BOTH:
                    for cols in _spans(part_w):
                        from_col = 2 * i * part_w + cols.start
                        src = slice(from_col, from_col + LANES)
                        v = jnp.where(live, al[:, src], 0.0)
                        fs[i, :, cols] = jnp.where(starts, xi[:, src].astype(jnp.float32), v)
                    early(i).start()

            turn(s, True)
            u[...] = jnp.zeros_like(u)

            @pl.when(s > 1)
            def _():
                add_log(s - 1, cc_ref[s - 1])

            for q in quarters:
                x_copy(s - 1, q).wait()

        _, ccol = normalizer(part, rows, meanwhile)
        cc_ref[s] = ccol
        safe = jnp.where(live, ccol, 1.0)
        safe_ref[...] = jnp.where(starts, 1.0, safe)
        for q, block in enumerate(_spans(wide, part_w)):
            for cols in _spans(part_w):
                src = slice(block.start + cols.start, block.start + cols.stop)
                alpha = jnp.where(live, al[:, src] / safe, 0.0)
                al[:, src] = alpha
                x = jnp.where(starts, xi[:, src].astype(jnp.float32), alpha)
                g[me * 4 + q, 0:rows, cols] = x.astype(jnp.bfloat16)

        al_copy(s).start()

        @pl.when(s + 1 < steps)
        def _():
            exchange(s, lambda: keep(s))

        return 0

    lax.fori_loop(1, steps, step, 0)
    add_log(steps - 1, cc_ref[steps - 1])
    ll_ref[...] += jnp.sum(lacc[...], axis=0, keepdims=True)
    al_copy(steps - 1).wait()
    for i in BOTH:
        for h in BOTH:
            tt_copy(steps - 1, i, h).wait()


def _forward(n, cid, rows, a_loc, e_rows, init_loc, code, sid, info):
    wide = a_loc.shape[1]
    steps, seqs, _ = code.shape
    part_w = wide // 4
    full = max(LANES, rows)
    nbuf = 4
    f32, bf16 = jnp.float32, jnp.bfloat16
    dma = pltpu.SemaphoreType.DMA
    return pl.pallas_call(
        functools.partial(_fwd_kernel, n, steps, rows, nbuf),
        out_shape=(
            jax.ShapeDtypeStruct((steps, rows, wide), f32),
            jax.ShapeDtypeStruct((seqs, wide), f32),
            jax.ShapeDtypeStruct((steps - 1, rows, wide), bf16),
            jax.ShapeDtypeStruct((2 * a_loc.shape[0] // part_w, wide, part_w // 2), bf16),
            jax.ShapeDtypeStruct((steps, rows, LANES), f32),
            jax.ShapeDtypeStruct((8, LANES), f32),
        ),
        in_specs=[ANY, ANY, VMEM, VMEM, VMEM, VMEM],
        out_specs=(ANY, ANY, ANY, ANY, VMEM, VMEM),
        scratch_shapes=[
            pltpu.VMEM((4 * n, full, part_w), bf16),
            pltpu.VMEM((2 * n + nbuf, part_w, wide), bf16),
            pltpu.VMEM((full, wide), f32),
            pltpu.VMEM((rows, wide), f32),
            pltpu.VMEM((2, rows, wide), bf16),
            pltpu.VMEM((seqs, wide), f32),
            pltpu.VMEM((seqs, wide), bf16),
            pltpu.VMEM((rows, wide), bf16),
            pltpu.VMEM((2, rows, part_w), f32),
            pltpu.VMEM((2, rows, part_w), f32),
            pltpu.VMEM((2, part_w, wide), bf16),
            pltpu.VMEM((2, wide, part_w), bf16),
            pltpu.VMEM((rows, LANES), f32),
            pltpu.VMEM((rows, LANES), f32),
            pltpu.VMEM((LANES, LANES), f32),
            pltpu.VMEM((8, LANES), f32),
            pltpu.VMEM((n, 8, LANES), f32),
            dma((2,)), dma((nbuf,)), dma((2 * n,)), dma((5,)), dma((2,)), dma((2, 2)),
            dma((n - 1,)), dma((n - 1,)),
            dma((12,)), dma((12,)), dma((2 * n,)), dma((2 * n,)),
        ],
        compiler_params=pltpu.CompilerParams(collective_id=cid, has_side_effects=True, vmem_limit_bytes=VMEM_BYTES),
        name='forward',
    )(a_loc, e_rows, init_loc, code, sid, info)


def _bwd_kernel(n, steps, rows, nbuf, at_hbm, e_hbm, cc_ref, code_ref, w_hbm,
                w, wv, ebuf, pp, rp, rs, rin,
                e_sem, w_sem, r_sem, out_sem, dd_ss, dd_rs, ici_ss, ici_rs):
    me, chip, core, partner, right, left = _place(n)
    chips = n // 2
    wide = wv.shape[1]
    size = at_hbm.shape[2]
    per = wide // size // 2
    trips = steps - 2
    rounds_n = 4 * per
    count = 2 * rounds_n
    ringed = 6 * per
    total = trips * rounds_n

    def piece(j, cls, i):
        p, e = lax.div(j, per), lax.rem(j, per)
        hh = jnp.where(p == 1, 1 - i, i)
        off = jnp.where(p == 0, 2, jnp.where(p == 3, 0, chips - 1 if i else 1))
        c = lax.rem(chip + off, chips)
        k = 1 - core if cls else core
        return (c * 2 + k) * 2 * per + hh * per + e

    def fetch(j, cls, i, slot, sem):
        return pltpu.make_async_copy(at_hbm.at[piece(j, cls, i)], w.at[slot, :, pl.ds(i * size, size)], sem)

    def stream(j, i, slot):
        return fetch(j, 1, i, rounds_n + slot, w_sem.at[slot, i])

    def resident(j, i):
        return fetch(j, 0, i, j, r_sem.at[j, i])

    def e_copy(t):
        first = pl.multiple_of((steps - 2 - t) * rows, 8)
        return pltpu.make_async_copy(e_hbm.at[pl.ds(first, rows), :], ebuf.at[lax.rem(t, 2)], e_sem.at[lax.rem(t, 2)])

    def w_copy(t):
        return pltpu.make_async_copy(wv.at[pl.ds(0, rows), :], w_hbm.at[steps - 2 - t], out_sem)

    for t in BOTH:
        e_copy(jnp.int32(t)).start()
    for q in range(nbuf):
        for i in BOTH:
            stream(jnp.int32(q), i, q).start()
            resident(jnp.int32(q), i).start()

    def load(j, _):
        for i in BOTH:
            resident(j, i).start()
        return 0

    lax.fori_loop(nbuf, rounds_n, load, 0)
    if wv.shape[0] > rows:
        wv[rows:, :] = jnp.zeros((wv.shape[0] - rows, wide), jnp.bfloat16)
    _barrier(me, n)

    def dd(k):
        return _remote(pp.at[k], rp.at[k], dd_ss.at[k], dd_rs.at[k], partner)

    def ring(k, par, i):
        return _remote(rs.at[k], rin.at[par, k], ici_ss.at[k], ici_rs.at[par, k], left if i else right)

    def weigh(s, eb, o, beta):
        code = code_ref[s, 0:rows, :].astype(jnp.float32)
        ok = code > 2.5
        safe = jnp.where(ok, cc_ref[s], 1.0)
        for cols in _spans(size):
            dst = slice(o + cols.start, o + cols.stop)
            b = 1.0 if beta is None else jnp.where(code > 3.5, 1.0, beta[:, cols])
            v = eb[:, dst].astype(jnp.float32) * b / safe
            wv[0:rows, dst] = jnp.where(ok, v, 0.0).astype(jnp.bfloat16)

    e_copy(jnp.int32(0)).wait()
    for cols in _spans(wide, size):
        weigh(steps - 1, ebuf.at[0], cols.start, None)
    w_copy(jnp.int32(0)).start()

    def step(t, _):
        par = lax.rem(t, 2)

        def finish(j):
            p = lax.div(j, per)
            for i in BOTH:
                dd(2 * j + i).wait_recv()

            @pl.when(p == 2)
            def _():
                for i in BOTH:
                    k = 2 * j + i
                    c = k - 4 * per
                    ring(c, par, i).wait_recv()
                    rp[k] += rin[par, c]

            for i in BOTH:
                k = 2 * j + i
                rs[k] += rp[k]

            @pl.when(p < 3)
            def _():
                for i in BOTH:
                    ring(2 * j + i, par, i).start()

        def rounds(j, _):
            q = t * rounds_n + j
            slot = lax.rem(q, nbuf)
            for i in BOTH:
                stream(j, i, slot).wait()
            prod = _dot(wv[...], w[rounds_n + slot])
            for i, cols in enumerate(_spans(2 * size, size)):
                k = 2 * j + i
                pp[k] = prod[0:rows, cols]
                dd(k).start()

            @pl.when(q + nbuf < total)
            def _():
                for i in BOTH:
                    stream(lax.rem(j + nbuf, rounds_n), i, slot).start()

            @pl.when(j > 0)
            def _():
                finish(j - 1)

            @pl.when(t == 0)
            def _():
                for i in BOTH:
                    resident(j, i).wait()

            prod = _dot(wv[...], w[j])
            for i, cols in enumerate(_spans(2 * size, size)):
                rs[2 * j + i] = prod[0:rows, cols]
            return 0

        lax.fori_loop(0, rounds_n, rounds, 0)
        finish(jnp.int32(rounds_n - 1))

        def gone(k, _):
            dd(k).wait_send()
            return 0

        def sent(k, _):
            ring(k, par, 0).wait_send()
            return 0

        lax.fori_loop(0, count, gone, 0)
        lax.fori_loop(0, 4 * per, sent, 0)
        nxt = t + 1
        e_copy(nxt).wait()

        @pl.when(nxt + 1 < steps - 1)
        def _():
            e_copy(nxt + 1).start()

        w_copy(t).wait()
        eb = ebuf.at[lax.rem(nxt, 2)]
        for e in range(per):
            for i in BOTH:
                near, late = 2 * (per + e) + 1 - i, 2 * (2 * per + e) + i
                ring(near, par, 1 - i).wait_recv()
                ring(late, par, i).wait_recv()
                beta = rs[ringed + 2 * e + i] + rin[par, near] + rin[par, late]
                weigh(steps - 1 - nxt, eb, (i * per + e) * size, beta)
        w_copy(nxt).start()
        lax.fori_loop(4 * per, ringed, sent, 0)
        return 0

    lax.fori_loop(0, trips, step, 0)
    w_copy(jnp.int32(trips)).wait()


def _backward(n, cid, at_loc, e_rows, ccol, code):
    pieces, wide, size = at_loc.shape
    steps, rows, _ = ccol.shape
    full = max(LANES, rows)
    count = pieces // 2
    nbuf = 6 if rows <= 80 else 4
    ringed = 3 * count // 4
    f32, bf16 = jnp.float32, jnp.bfloat16
    dma = pltpu.SemaphoreType.DMA
    return pl.pallas_call(
        functools.partial(_bwd_kernel, n, steps, rows, nbuf),
        out_shape=jax.ShapeDtypeStruct((steps - 1, rows, wide), bf16),
        in_specs=[ANY, ANY, VMEM, VMEM],
        out_specs=ANY,
        scratch_shapes=[
            pltpu.VMEM((count // 2 + nbuf, wide, 2 * size), bf16),
            pltpu.VMEM((full, wide), bf16),
            pltpu.VMEM((2, rows, wide), bf16),
            pltpu.VMEM((count, rows, size), f32),
            pltpu.VMEM((count, rows, size), f32),
            pltpu.VMEM((count, rows, size), f32),
            pltpu.VMEM((2, ringed, rows, size), f32),
            dma((2,)), dma((nbuf, 2)), dma((count // 2, 2)), dma(()),
            dma((count,)), dma((count,)),
            dma((ringed,)), dma((2, ringed)),
        ],
        compiler_params=pltpu.CompilerParams(collective_id=cid, has_side_effects=True, vmem_limit_bytes=VMEM_BYTES),
        name='backward',
    )(at_loc, e_rows, ccol, code)


def _pair_kernel(group_ref, a_ref, x_ref, w_ref, o_ref):
    pair_sum = lax.dot_general(x_ref[...], w_ref[...], (((0,), (0,)), ((), ())), preferred_element_type=jnp.float32)
    o_ref[...] = a_ref[...].astype(jnp.float32) * pair_sum


def _pairs(group, a_loc, xs, ws):
    depth, wide = ws.shape
    size = wide // 8
    tiles = wide // size
    return pl.pallas_call(
        _pair_kernel,
        out_shape=jax.ShapeDtypeStruct((wide, wide), jnp.float32),
        grid_spec=pltpu.PrefetchScalarGridSpec(
            num_scalar_prefetch=1,
            grid=(tiles,),
            in_specs=[
                pl.BlockSpec((size, wide), lambda i, group_ref: (group_ref[0] * tiles + i, 0)),
                pl.BlockSpec((depth, size), lambda i, group_ref: (0, i)),
                pl.BlockSpec((depth, wide), lambda i, group_ref: (0, 0)),
            ],
            out_specs=pl.BlockSpec((size, wide), lambda i, group_ref: (i, 0)),
        ),
        compiler_params=pltpu.CompilerParams(vmem_limit_bytes=VMEM_BYTES),
        name='pairs',
    )(group, a_loc, xs, ws)


def _plan_kernel(options, len_ref, tok_ref, code_ref, sid_ref, look_ref, info_ref, pick_ref):
    seqs = len_ref.shape[1]
    steps = tok_ref.shape[0]
    f32, bf16 = jnp.float32, jnp.bfloat16
    square = (seqs, seqs)
    up = lax.broadcasted_iota(jnp.int32, square, 0).astype(f32)
    across = lax.broadcasted_iota(jnp.int32, square, 1).astype(f32)

    def spread(row):
        return jnp.broadcast_to(row, square)

    def total(x):
        return jnp.sum(x, axis=0, keepdims=True)

    length = len_ref[...].astype(f32)
    l_row = spread(length)
    l_col = l_row.T
    ahead = (l_col > l_row) | ((l_col == l_row) & (up < across))
    rank = total(jnp.where(ahead, 1.0, 0.0))
    rank_col = spread(rank).T

    def mates(slots):
        slot = jnp.where(rank < slots, rank, 2 * slots - 1 - rank)
        return slot, total(jnp.where(rank_col == spread(slot), l_col, 0.0))

    slots = jnp.full((1, 1), seqs, jnp.int32).astype(f32)
    pick = jnp.full((1, 1), len(options) - 1, jnp.int32)
    for k in reversed(range(len(options) - 1)):
        _, first = mates(options[k])
        worst = jnp.max(jnp.where(rank < options[k], 0.0, first + length), axis=1, keepdims=True)
        fits = worst <= steps + 1
        slots = jnp.where(fits, options[k], slots)
        pick = jnp.where(fits, k, pick)
    pick_ref[...] = pick
    slot, first = mates(slots)
    opens = rank < slots
    begin = jnp.where(opens, 0.0, first - 1)
    end = begin + length - 1
    info_ref[0:1, :] = slot
    info_ref[1:2, :] = begin
    info_ref[2:3, :] = end
    info_ref[3:4, :] = end * slots + slot

    double = total(jnp.where((spread(slot).T == spread(slot)) & (up != across), 1.0, 0.0))
    shadowed = opens & (length < 1.5) & (double > 0.5)
    home = (spread(slot) == up).astype(bf16)
    slot_col, begin_col, end_col = spread(slot).T, spread(begin).T, spread(end).T
    hidden_col = spread(jnp.where(shadowed, 1.0, 0.0)).T
    for s in range(steps):
        moves = (begin_col < s) & (end_col >= s)
        kind = jnp.where(moves, jnp.where(end_col == s, 4.0, 3.0), 0.0)
        code_ref[s] = _dot(home, kind.astype(bf16)).astype(bf16)
        number = jnp.where((begin_col == s) & (hidden_col < 0.5), up + 1, 0.0)
        sid_ref[s] = (_dot(home, number.astype(bf16)) - 1).astype(bf16)
    away = (slot_col == across).astype(bf16)
    shape = (steps, seqs)
    pos = lax.broadcasted_iota(jnp.int32, shape, 0).astype(f32) - jnp.broadcast_to(begin, shape)
    tok = jnp.zeros(shape, f32)
    for t in range(1, steps):
        there = (pos == t) & (jnp.broadcast_to(length, shape) > t)
        tok = tok + jnp.where(there, jnp.broadcast_to(tok_ref[t:t + 1, :].astype(f32), shape), 0.0)
    high = jnp.floor(tok / LANES)
    low = tok - high * LANES
    look = _dot(high.astype(bf16), away) * LANES + _dot(low.astype(bf16), away)
    look_ref[...] = look.astype(jnp.int32)


def _plan(options, lengths, tokens):
    steps, seqs = tokens.shape
    bf16 = jnp.bfloat16
    return pl.pallas_call(
        functools.partial(_plan_kernel, options),
        out_shape=(
            jax.ShapeDtypeStruct((steps, seqs, LANES), bf16),
            jax.ShapeDtypeStruct((steps, seqs, LANES), bf16),
            jax.ShapeDtypeStruct((steps, seqs), jnp.int32),
            jax.ShapeDtypeStruct((8, seqs), jnp.float32),
            jax.ShapeDtypeStruct((1, 1), jnp.int32),
        ),
        in_specs=[VMEM, VMEM],
        out_specs=(VMEM, VMEM, VMEM, VMEM, VMEM),
        name='plan',
    )(lengths[None, :], tokens)


def solution(mesh):
    n = mesh.shape['states']

    def local_run(trans_loc, emit_loc, init_loc, tokens_loc, lengths_loc):
        seqs, steps = tokens_loc.shape
        wide = trans_loc.shape[1]
        group = lax.axis_index('states').astype(jnp.int32)[None]
        options = (seqs * 9 // 16, seqs * 5 // 8, seqs)
        code, sid, look, info, pick = _plan(options, lengths_loc, tokens_loc.T)

        def run(k):
            rows = options[k]
            tokens = jnp.concatenate([look[1:, 0:rows].reshape(-1), tokens_loc[:, 0]])
            e_rows = jnp.take(emit_loc, tokens, axis=1, mode='clip').T
            al, a0, xs, at_loc, ccol, ll = _forward(n, 2 * k, rows, trans_loc, e_rows, init_loc[None, :], code, sid, info)
            ws = _backward(n, 2 * k + 1, at_loc, e_rows, ccol, code)
            counts = _pairs(group, trans_loc, xs.reshape(-1, wide), ws.reshape(-1, wide))
            last = jnp.take(al.reshape(steps * rows, wide), info[3].astype(jnp.int32), axis=0, mode='clip')
            return ll[0], jnp.where((lengths_loc == 1)[:, None], a0, last), counts

        return lax.switch(pick[0, 0], [functools.partial(run, k) for k in range(len(options))])

    return jax.shard_map(local_run, mesh=mesh, in_specs=(P(None, 'states'), P('states', None), P('states'), P('seqs', None), P('seqs')), out_specs=(P('seqs'), P('seqs', 'states'), P(('seqs', 'states'), None)), check_vma=False)
```

```python
import functools

import jax
import jax.numpy as jnp
from jax import lax
from jax.experimental import pallas as pl
from jax.experimental.pallas import tpu as pltpu
from jax.sharding import PartitionSpec as P

MESH = pl.DeviceIdType.MESH
ANY = pl.BlockSpec(memory_space=pl.ANY)
VMEM = pl.BlockSpec(memory_space=pltpu.VMEM)
LANES = 128
BOTH = (0, 1)
VMEM_BYTES = 67043328


def _place(n):
    me = lax.axis_index('states')
    core = lax.rem(me, 2)
    chip = lax.div(me, 2)
    partner = chip * 2 + (1 - core)
    right = lax.rem(me + 2, n)
    left = lax.rem(me + n - 2, n)
    return me, chip, core, partner, right, left


def _dev(peer):
    return {'states': peer}


def _arrive(me, n):
    for r in range(1, n):
        pl.semaphore_signal(pltpu.get_barrier_semaphore(), inc=1, device_id=_dev(lax.rem(me + r, n)), device_id_type=MESH)


def _all_here(n):
    pl.semaphore_wait(pltpu.get_barrier_semaphore(), n - 1)


def _remote(src, dst, ssem, rsem, peer):
    return pltpu.make_async_remote_copy(src_ref=src, dst_ref=dst, send_sem=ssem, recv_sem=rsem, device_id=_dev(peer), device_id_type=MESH)


def _spans(width, size=LANES):
    return [slice(o, o + size) for o in range(0, width, size)]


def _dot(x, y):
    return jnp.dot(x, y, preferred_element_type=jnp.float32)


def _fwd_kernel(n, steps, rows, nbuf, a_hbm, e_hbm, pi_ref, code_ref, sid_ref, info_ref, al_hbm, a0_hbm, x_hbm, at_hbm, cc_ref, ll_ref,
                g, w, u, al, ebuf, a0b, xi, fs, fr, ta, tt, safe_ref, lacc, tbuf, cs_send, cs_recv,
                e_sem, w_sem, r_sem, out_sem, ta_sem, tt_sem, cs_ss, cs_rs, ici_ss, ici_rs, dd_ss, dd_rs):
    me, chip, core, partner, right, left = _place(n)
    chips = n // 2
    wide = al.shape[1]
    part_w = wide // 4
    seqs = a0b.shape[0]
    a0f = u.at[pl.ds(0, seqs), :]
    quarters = range(4)
    per_step = 2 * 8
    total = (steps - 1) * per_step

    def quarter(j, cls, i):
        far = lax.rem(j + 2 + 2 * i, 4)
        qq = jnp.where(j < 2, 2 * j + i, far)
        off = jnp.where(j < 2, 0, jnp.where(j >= 6, 2, jnp.where(i == 0, chips - 1, 1)))
        c = lax.rem(chip + off, chips)
        k = jnp.where(cls == 0, core, 1 - core)
        return (c * 2 + k) * 4 + qq

    def a_part(b):
        return a_hbm.at[pl.ds(pl.multiple_of(b * part_w, part_w), part_w), :]

    def stream(q, slot):
        k = lax.rem(q, per_step)
        return pltpu.make_async_copy(a_part(quarter(lax.div(k, 2), 1, lax.rem(k, 2))), w.at[per_step + slot], w_sem.at[slot])

    def resident(j, i):
        return pltpu.make_async_copy(a_part(quarter(j, 0, i)), w.at[2 * j + i], r_sem.at[2 * j + i])

    def e_rows(first, count, dst, sem):
        return pltpu.make_async_copy(e_hbm.at[pl.ds(pl.multiple_of(first, 8), count), :], dst, sem)

    def e_copy(s):
        return e_rows((s - 1) * rows, rows, ebuf.at[lax.rem(s, 2)], e_sem.at[lax.rem(s, 2)])

    def al_copy(s):
        return pltpu.make_async_copy(al, al_hbm.at[s], out_sem.at[4])

    def mine(b):
        return g.at[b, pl.ds(0, rows), :]

    def x_copy(s, q):
        return pltpu.make_async_copy(mine(me * 4 + q), x_hbm.at[s, :, pl.ds(q * part_w, part_w)], out_sem.at[q])

    pieces, depth, size = at_hbm.shape[0], ta.shape[0], ta.shape[1]

    def ta_copy(c):
        slot = lax.rem(c, depth)
        return pltpu.make_async_copy(a_hbm.at[pl.ds(pl.multiple_of(c * size, size), size), :], ta.at[slot], ta_sem.at[slot])

    def tt_copy(c):
        slot = lax.rem(c, depth)
        return pltpu.make_async_copy(tt.at[slot], at_hbm.at[c], tt_sem.at[slot])

    def turn(s):
        def one(c, _):
            ta_copy(c).wait()

            @pl.when(c >= depth)
            def _():
                tt_copy(c - depth).wait()

            slot = lax.rem(c, depth)
            tt[slot] = ta[slot].T
            tt_copy(c).start()

            @pl.when(c + depth < pieces)
            def _():
                ta_copy(c + depth).start()

            return 0

        lax.fori_loop(lax.div((s - 1) * pieces, steps - 1), lax.div(s * pieces, steps - 1), one, 0)

    e0_copy = e_rows((steps - 1) * rows, seqs, a0b, e_sem.at[0])
    e0_copy.start()
    _arrive(me, n)

    def load(j, _):
        for i in BOTH:
            resident(j, i).start()
        return 0

    for c in range(depth):
        ta_copy(jnp.int32(c)).start()
    for q in range(nbuf):
        stream(jnp.int32(q), q).start()
    lax.fori_loop(0, 2, load, 0)
    e_copy(jnp.int32(1)).start()
    tbuf[...] = jnp.zeros_like(tbuf)
    lacc[...] = jnp.zeros_like(lacc)
    if g.shape[1] > rows:
        pad = jnp.zeros((g.shape[1] - rows, part_w), jnp.bfloat16)

        def clear(k, _):
            g[k, rows:, :] = pad
            return 0

        lax.fori_loop(0, 4 * n, clear, 0)

    def ici(k, src, dst, i):
        return _remote(src, dst, ici_ss.at[k], ici_rs.at[k], left if i else right)

    def early(i):
        return ici(i, fs.at[i], fr.at[i], i)

    def own_ring(j, i):
        b = me * 4 + (j + 2 + 2 * i) % 4
        return ici(2 * (j - 2) + i, mine(b), mine(b), i)

    def relay(j, i):
        b = quarter(j, 0, i)
        return ici(2 * (j + 2) + i, mine(b), mine(b), i)

    def dd(j, cls, i):
        b = quarter(j, cls, i)
        return _remote(mine(b), mine(b), dd_ss.at[2 * j + i], dd_rs.at[2 * j + i], partner)

    lane = lax.broadcasted_iota(jnp.int32, (rows, seqs), 1).astype(jnp.float32)
    row = lax.broadcasted_iota(jnp.int32, (rows, seqs), 0).astype(jnp.float32)

    def starting(s):
        return sid_ref[s, 0:rows, :].astype(jnp.float32)

    def first_alphas(s):
        pick = (starting(s) == lane).astype(jnp.bfloat16)
        xi[...] = _dot(pick, a0b[...]).astype(jnp.bfloat16)

    def normalizer(part, count, meanwhile):
        tbuf[0:count, :] = part
        row = jnp.sum(tbuf[...].T, axis=0, keepdims=True)
        cs_send[...] = jnp.broadcast_to(row, cs_send.shape)
        cs_recv[me] = jnp.broadcast_to(row, cs_send.shape)
        cps = []
        for r in sorted(range(1, n), key=lambda r: abs(2 * r - n)):
            cp = _remote(cs_send, cs_recv.at[me], cs_ss.at[r - 1], cs_rs.at[r - 1], lax.rem(me + r, n))
            cp.start()
            cps.append(cp)
        meanwhile()
        for cp in cps:
            cp.wait()
        crow = cs_recv[0]
        for r in range(1, n):
            crow = crow + cs_recv[r]
        return crow, jnp.broadcast_to(crow[0:1, :], (LANES, LANES)).T[0:count, :]

    def add_log(s, ccol):
        slot, begin, end = info_ref[0:1, :], info_ref[1:2, :], info_ref[2:3, :]
        now = jnp.full((rows, seqs), s, jnp.int32).astype(jnp.float32)
        here = (slot == row) & (now > begin) & (now <= end)
        lacc[...] += jnp.where(here, jnp.log(jnp.where(here, ccol, 1.0)), 0.0)

    def exchange(s, then):
        own = [own_ring(3, i) for i in BOTH] + [dd(j, 0, i) for j in BOTH for i in BOTH]
        own += [own_ring(j, i) for j in (4, 5) for i in BOTH]
        for cp in own:
            cp.start()
        then()

        def arrived(j):
            for i in BOTH:
                b = quarter(j, 0, i)
                ici(2 * (j - 2) + i, mine(b), mine(b), i).wait_recv()

        def pass_on(j):
            for i in BOTH:
                dd(j, 0, i).start()

        def rounds(h, _):
            j, k = 2 * h, 2 * h + 1

            @pl.when(h == 1)
            def _():
                for i in BOTH:
                    early(i).wait_recv()
                safe = safe_ref[...]
                for i in BOTH:
                    b = quarter(2, 0, i)
                    for cols in _spans(part_w):
                        g[b, 0:rows, cols] = (fr[i, :, cols] / safe).astype(jnp.bfloat16)
                    relay(2, i).start()
                pass_on(2)

            @pl.when((h == 2) & (s + 2 < steps))
            def _():
                first_alphas(s + 1)

            @pl.when(s == 0)
            def _():
                for r in (j, k):
                    for i in BOTH:
                        resident(r, i).wait()

                    @pl.when(h < 2)
                    def _():
                        load(r + 4, 0)

            @pl.when(h >= 2)
            def _():
                arrived(j)
                pass_on(j)

            def own_class(r):
                return sum(_dot(g[quarter(r, 0, i)], w[2 * r + i]) for i in BOTH)

            def other_class(r):
                q = s * per_step + 2 * r
                slots = [lax.rem(q + i, nbuf) for i in BOTH]
                for i in BOTH:
                    dd(r, 1, i).wait_recv()
                    stream(q + i, slots[i]).wait()
                out = sum(_dot(g[quarter(r, 1, i)], w[per_step + slots[i]]) for i in BOTH)

                for i in BOTH:
                    @pl.when(q + i + nbuf < total)
                    def _():
                        stream(q + i + nbuf, slots[i]).start()

                return out

            prod = own_class(j)

            @pl.when(h >= 1)
            def _():
                arrived(k)

            @pl.when(h == 1)
            def _():
                for i in BOTH:
                    relay(3, i).start()

            @pl.when(h >= 1)
            def _():
                pass_on(k)

            u[...] += prod + own_class(k)
            u[...] += other_class(j)
            u[...] += other_class(k)
            return 0

        lax.fori_loop(0, 4, rounds, 0)
        for i in BOTH:
            early(i).wait_send()
            for j in (2, 3):
                relay(j, i).wait_send()
            for j in range(2, 8):
                dd(j, 0, i).wait_send()
        for cp in own:
            cp.wait_send()

    def keep(s):
        for q in quarters:
            x_copy(s, q).start()

    e0_copy.wait()
    def lanes(q):
        return pl.ds(pl.multiple_of(q * LANES, LANES), LANES)

    def first_mass(q, part):
        a = jnp.broadcast_to(pi_ref[:, lanes(q)], (seqs, LANES)) * a0b[:, lanes(q)].astype(jnp.float32)
        a0f[:, lanes(q)] = a
        return part + a

    part = lax.fori_loop(0, wide // LANES, first_mass, jnp.zeros((seqs, LANES), jnp.float32))
    _all_here(n)

    c0_row, c0 = normalizer(part, seqs, lambda: lax.fori_loop(2, 4, load, 0))
    ll_ref[...] = jnp.log(c0_row)

    def first_alpha(q, _):
        alpha = a0f[:, lanes(q)] / c0
        a0f[:, lanes(q)] = alpha
        a0b[:, lanes(q)] = alpha.astype(jnp.bfloat16)
        return 0

    lax.fori_loop(0, wide // LANES, first_alpha, 0)
    a0_copy = pltpu.make_async_copy(a0f, a0_hbm, e_sem.at[0])
    a0_copy.start()
    first_alphas(0)
    for q, cols in enumerate(_spans(wide, part_w)):
        g[me * 4 + q, 0:rows, :] = xi[:, cols]
    safe_ref[...] = jnp.ones_like(safe_ref)
    for i in BOTH:
        fs[i] = xi[:, 2 * i * part_w:(2 * i + 1) * part_w].astype(jnp.float32)
        early(i).start()
    tbuf[...] = jnp.zeros_like(tbuf)
    a0_copy.wait()
    u[...] = jnp.zeros_like(u)

    def step(s, _):
        exchange(s - 1, lambda: keep(s - 1))
        e_copy(s).wait()

        @pl.when(s + 1 < steps)
        def _():
            e_copy(s + 1).start()

        @pl.when(s > 1)
        def _():
            al_copy(s - 1).wait()

        part = jnp.zeros((rows, LANES), jnp.float32)
        eb = ebuf.at[lax.rem(s, 2)]
        for cols in _spans(wide):
            a = u[0:rows, cols] * eb[:, cols].astype(jnp.float32)
            al[:, cols] = a
            part = part + a
        live = code_ref[s, 0:rows, :].astype(jnp.float32) > 0.5
        starts = starting(s) > -0.5

        def meanwhile():
            @pl.when(s + 1 < steps)
            def _():
                for i in BOTH:
                    for cols in _spans(part_w):
                        from_col = 2 * i * part_w + cols.start
                        src = slice(from_col, from_col + LANES)
                        v = jnp.where(live, al[:, src], 0.0)
                        fs[i, :, cols] = jnp.where(starts, xi[:, src].astype(jnp.float32), v)
                    early(i).start()

            turn(s)
            u[...] = jnp.zeros_like(u)

            @pl.when(s > 1)
            def _():
                add_log(s - 1, cc_ref[s - 1])

            for q in quarters:
                x_copy(s - 1, q).wait()

        _, ccol = normalizer(part, rows, meanwhile)
        cc_ref[s] = ccol
        safe = jnp.where(live, ccol, 1.0)
        safe_ref[...] = jnp.where(starts, 1.0, safe)
        for q, block in enumerate(_spans(wide, part_w)):
            for cols in _spans(part_w):
                src = slice(block.start + cols.start, block.start + cols.stop)
                alpha = jnp.where(live, al[:, src] / safe, 0.0)
                al[:, src] = alpha
                x = jnp.where(starts, xi[:, src].astype(jnp.float32), alpha)
                g[me * 4 + q, 0:rows, cols] = x.astype(jnp.bfloat16)

        al_copy(s).start()
        return 0

    lax.fori_loop(1, steps, step, 0)
    add_log(steps - 1, cc_ref[steps - 1])
    ll_ref[...] += jnp.sum(lacc[...], axis=0, keepdims=True)
    al_copy(steps - 1).wait()
    for c in range(depth):
        tt_copy(pieces - depth + c).wait()


def _forward(n, cid, rows, a_loc, e_rows, init_loc, code, sid, info):
    wide = a_loc.shape[1]
    steps, seqs, _ = code.shape
    part_w = wide // 4
    full = max(LANES, rows)
    nbuf = 6 if rows <= 80 else 4
    f32, bf16 = jnp.float32, jnp.bfloat16
    dma = pltpu.SemaphoreType.DMA
    return pl.pallas_call(
        functools.partial(_fwd_kernel, n, steps, rows, nbuf),
        out_shape=(
            jax.ShapeDtypeStruct((steps, rows, wide), f32),
            jax.ShapeDtypeStruct((seqs, wide), f32),
            jax.ShapeDtypeStruct((steps - 1, rows, wide), bf16),
            jax.ShapeDtypeStruct((2 * a_loc.shape[0] // part_w, wide, part_w // 2), bf16),
            jax.ShapeDtypeStruct((steps, rows, LANES), f32),
            jax.ShapeDtypeStruct((8, LANES), f32),
        ),
        in_specs=[ANY, ANY, VMEM, VMEM, VMEM, VMEM],
        out_specs=(ANY, ANY, ANY, ANY, VMEM, VMEM),
        scratch_shapes=[
            pltpu.VMEM((4 * n, full, part_w), bf16),
            pltpu.VMEM((2 * n + nbuf, part_w, wide), bf16),
            pltpu.VMEM((full, wide), f32),
            pltpu.VMEM((rows, wide), f32),
            pltpu.VMEM((2, rows, wide), bf16),
            pltpu.VMEM((seqs, wide), bf16),
            pltpu.VMEM((rows, wide), bf16),
            pltpu.VMEM((2, rows, part_w), f32),
            pltpu.VMEM((2, rows, part_w), f32),
            pltpu.VMEM((4, part_w // 2, wide), bf16),
            pltpu.VMEM((4, wide, part_w // 2), bf16),
            pltpu.VMEM((rows, LANES), f32),
            pltpu.VMEM((rows, LANES), f32),
            pltpu.VMEM((LANES, LANES), f32),
            pltpu.VMEM((8, LANES), f32),
            pltpu.VMEM((n, 8, LANES), f32),
            dma((2,)), dma((nbuf,)), dma((2 * n,)), dma((5,)), dma((4,)), dma((4,)),
            dma((n - 1,)), dma((n - 1,)),
            dma((12,)), dma((12,)), dma((2 * n,)), dma((2 * n,)),
        ],
        compiler_params=pltpu.CompilerParams(collective_id=cid, has_side_effects=True, vmem_limit_bytes=VMEM_BYTES),
        name='forward',
    )(a_loc, e_rows, init_loc, code, sid, info)


def _bwd_kernel(n, steps, rows, nbuf, at_hbm, e_hbm, cc_ref, code_ref, w_hbm,
                w, wv, ebuf, pp, rp, rs, rin,
                e_sem, w_sem, r_sem, out_sem, dd_ss, dd_rs, ici_ss, ici_rs):
    me, chip, core, partner, right, left = _place(n)
    chips = n // 2
    wide = wv.shape[1]
    size = at_hbm.shape[2]
    per = wide // size // 2
    trips = steps - 2
    rounds_n = 4 * per
    count = 2 * rounds_n
    ringed = 6 * per
    total = trips * rounds_n

    def piece(j, cls, i):
        p, e = lax.div(j, per), lax.rem(j, per)
        hh = jnp.where(p == 1, 1 - i, i)
        off = jnp.where(p == 0, 2, jnp.where(p == 3, 0, chips - 1 if i else 1))
        c = lax.rem(chip + off, chips)
        k = 1 - core if cls else core
        return (c * 2 + k) * 2 * per + hh * per + e

    def fetch(j, cls, i, slot, sem):
        return pltpu.make_async_copy(at_hbm.at[piece(j, cls, i)], w.at[slot, :, pl.ds(i * size, size)], sem)

    def stream(j, i, slot):
        return fetch(j, 1, i, rounds_n + slot, w_sem.at[slot, i])

    def resident(j, i):
        return fetch(j, 0, i, j, r_sem.at[j, i])

    def e_copy(t):
        first = pl.multiple_of((steps - 2 - t) * rows, 8)
        return pltpu.make_async_copy(e_hbm.at[pl.ds(first, rows), :], ebuf.at[lax.rem(t, 2)], e_sem.at[lax.rem(t, 2)])

    def w_copy(t):
        return pltpu.make_async_copy(wv.at[pl.ds(0, rows), :], w_hbm.at[steps - 2 - t], out_sem)

    for t in BOTH:
        e_copy(jnp.int32(t)).start()
    _arrive(me, n)

    def load(j, _):
        for i in BOTH:
            resident(j, i).start()
        return 0

    for q in BOTH:
        for i in BOTH:
            stream(jnp.int32(q), i, q).start()
        load(jnp.int32(q), 0)
    if wv.shape[0] > rows:
        wv[rows:, :] = jnp.zeros((wv.shape[0] - rows, wide), jnp.bfloat16)

    def dd(k):
        return _remote(pp.at[k], rp.at[k], dd_ss.at[k], dd_rs.at[k], partner)

    def ring(k, par, i):
        return _remote(rs.at[k], rin.at[par, k], ici_ss.at[k], ici_rs.at[par, k], left if i else right)

    def weigh(s, eb, o, beta):
        code = code_ref[s, 0:rows, :].astype(jnp.float32)
        ok = code > 2.5
        safe = jnp.where(ok, cc_ref[s], 1.0)
        for cols in _spans(size):
            dst = slice(o + cols.start, o + cols.stop)
            b = 1.0 if beta is None else jnp.where(code > 3.5, 1.0, beta[:, cols])
            v = eb[:, dst].astype(jnp.float32) * b / safe
            wv[0:rows, dst] = jnp.where(ok, v, 0.0).astype(jnp.bfloat16)

    e_copy(jnp.int32(0)).wait()
    for cols in _spans(wide, size):
        weigh(steps - 1, ebuf.at[0], cols.start, None)
    ahead = 4
    for q in range(2, nbuf):
        for i in BOTH:
            stream(jnp.int32(q), i, q).start()
    for q in range(2, ahead):
        load(jnp.int32(q), 0)
    w_copy(jnp.int32(0)).start()
    _all_here(n)

    def step(t, _):
        par = lax.rem(t, 2)

        def finish(j):
            p = lax.div(j, per)
            for i in BOTH:
                dd(2 * j + i).wait_recv()

            @pl.when(p == 2)
            def _():
                for i in BOTH:
                    k = 2 * j + i
                    c = k - 4 * per
                    ring(c, par, i).wait_recv()
                    rp[k] += rin[par, c]

            for i in BOTH:
                k = 2 * j + i
                rs[k] += rp[k]

            @pl.when(p < 3)
            def _():
                for i in BOTH:
                    ring(2 * j + i, par, i).start()

        def rounds(j, _):
            q = t * rounds_n + j
            slot = lax.rem(q, nbuf)
            for i in BOTH:
                stream(j, i, slot).wait()
            prod = _dot(wv[...], w[rounds_n + slot])
            for i, cols in enumerate(_spans(2 * size, size)):
                k = 2 * j + i
                pp[k] = prod[0:rows, cols]
                dd(k).start()

            @pl.when(q + nbuf < total)
            def _():
                for i in BOTH:
                    stream(lax.rem(j + nbuf, rounds_n), i, slot).start()

            @pl.when(j > 0)
            def _():
                finish(j - 1)

            @pl.when(t == 0)
            def _():
                for i in BOTH:
                    resident(j, i).wait()

                @pl.when(j < rounds_n - ahead)
                def _():
                    load(j + ahead, 0)

            prod = _dot(wv[...], w[j])
            for i, cols in enumerate(_spans(2 * size, size)):
                rs[2 * j + i] = prod[0:rows, cols]
            return 0

        lax.fori_loop(0, rounds_n, rounds, 0)
        finish(jnp.int32(rounds_n - 1))

        def gone(k, _):
            dd(k).wait_send()
            return 0

        def sent(k, _):
            ring(k, par, 0).wait_send()
            return 0

        lax.fori_loop(0, count, gone, 0)
        lax.fori_loop(0, 4 * per, sent, 0)
        nxt = t + 1
        e_copy(nxt).wait()

        @pl.when(nxt + 1 < steps - 1)
        def _():
            e_copy(nxt + 1).start()

        w_copy(t).wait()
        eb = ebuf.at[lax.rem(nxt, 2)]
        for e in range(per):
            for i in BOTH:
                near, late = 2 * (per + e) + 1 - i, 2 * (2 * per + e) + i
                ring(near, par, 1 - i).wait_recv()
                ring(late, par, i).wait_recv()
                beta = rs[ringed + 2 * e + i] + rin[par, near] + rin[par, late]
                weigh(steps - 1 - nxt, eb, (i * per + e) * size, beta)
        w_copy(nxt).start()
        lax.fori_loop(4 * per, ringed, sent, 0)
        return 0

    lax.fori_loop(0, trips, step, 0)
    w_copy(jnp.int32(trips)).wait()


def _backward(n, cid, at_loc, e_rows, ccol, code):
    pieces, wide, size = at_loc.shape
    steps, rows, _ = ccol.shape
    full = max(LANES, rows)
    count = pieces // 2
    nbuf = 6 if rows <= 80 else 4
    ringed = 3 * count // 4
    f32, bf16 = jnp.float32, jnp.bfloat16
    dma = pltpu.SemaphoreType.DMA
    return pl.pallas_call(
        functools.partial(_bwd_kernel, n, steps, rows, nbuf),
        out_shape=jax.ShapeDtypeStruct((steps - 1, rows, wide), bf16),
        in_specs=[ANY, ANY, VMEM, VMEM],
        out_specs=ANY,
        scratch_shapes=[
            pltpu.VMEM((count // 2 + nbuf, wide, 2 * size), bf16),
            pltpu.VMEM((full, wide), bf16),
            pltpu.VMEM((2, rows, wide), bf16),
            pltpu.VMEM((count, rows, size), f32),
            pltpu.VMEM((count, rows, size), f32),
            pltpu.VMEM((count, rows, size), f32),
            pltpu.VMEM((2, ringed, rows, size), f32),
            dma((2,)), dma((nbuf, 2)), dma((count // 2, 2)), dma(()),
            dma((count,)), dma((count,)),
            dma((ringed,)), dma((2, ringed)),
        ],
        compiler_params=pltpu.CompilerParams(collective_id=cid, has_side_effects=True, vmem_limit_bytes=VMEM_BYTES),
        name='backward',
    )(at_loc, e_rows, ccol, code)


def _pair_kernel(group_ref, a_ref, x_ref, w_ref, o_ref):
    pair_sum = lax.dot_general(x_ref[...], w_ref[...], (((0,), (0,)), ((), ())), preferred_element_type=jnp.float32)
    o_ref[...] = a_ref[...].astype(jnp.float32) * pair_sum


def _pairs(group, a_loc, xs, ws):
    depth, wide = ws.shape
    size = wide // 8
    tiles = wide // size
    return pl.pallas_call(
        _pair_kernel,
        out_shape=jax.ShapeDtypeStruct((wide, wide), jnp.float32),
        grid_spec=pltpu.PrefetchScalarGridSpec(
            num_scalar_prefetch=1,
            grid=(tiles,),
            in_specs=[
                pl.BlockSpec((size, wide), lambda i, group_ref: (group_ref[0] * tiles + i, 0)),
                pl.BlockSpec((depth, size), lambda i, group_ref: (0, i)),
                pl.BlockSpec((depth, wide), lambda i, group_ref: (0, 0)),
            ],
            out_specs=pl.BlockSpec((size, wide), lambda i, group_ref: (i, 0)),
        ),
        compiler_params=pltpu.CompilerParams(vmem_limit_bytes=VMEM_BYTES),
        name='pairs',
    )(group, a_loc, xs, ws)


def _plan_kernel(options, len_ref, tok_ref, code_ref, sid_ref, look_ref, info_ref, pick_ref):
    seqs = len_ref.shape[1]
    steps = tok_ref.shape[0]
    f32, bf16 = jnp.float32, jnp.bfloat16
    square = (seqs, seqs)
    up = lax.broadcasted_iota(jnp.int32, square, 0).astype(f32)
    across = lax.broadcasted_iota(jnp.int32, square, 1).astype(f32)

    def spread(row):
        return jnp.broadcast_to(row, square)

    def total(x):
        return jnp.sum(x, axis=0, keepdims=True)

    length = len_ref[...].astype(f32)
    l_row = spread(length)
    l_col = l_row.T
    ahead = (l_col > l_row) | ((l_col == l_row) & (up < across))
    rank = total(jnp.where(ahead, 1.0, 0.0))
    rank_col = spread(rank).T

    def mates(slots):
        slot = jnp.where(rank < slots, rank, 2 * slots - 1 - rank)
        return slot, total(jnp.where(rank_col == spread(slot), l_col, 0.0))

    slots = jnp.full((1, 1), seqs, jnp.int32).astype(f32)
    pick = jnp.full((1, 1), len(options) - 1, jnp.int32)
    for k in reversed(range(len(options) - 1)):
        _, first = mates(options[k])
        worst = jnp.max(jnp.where(rank < options[k], 0.0, first + length), axis=1, keepdims=True)
        fits = worst <= steps + 1
        slots = jnp.where(fits, options[k], slots)
        pick = jnp.where(fits, k, pick)
    pick_ref[...] = pick
    slot, first = mates(slots)
    opens = rank < slots
    begin = jnp.where(opens, 0.0, first - 1)
    end = begin + length - 1
    info_ref[0:1, :] = slot
    info_ref[1:2, :] = begin
    info_ref[2:3, :] = end
    info_ref[3:4, :] = end * slots + slot

    double = total(jnp.where((spread(slot).T == spread(slot)) & (up != across), 1.0, 0.0))
    shadowed = opens & (length < 1.5) & (double > 0.5)
    home = (spread(slot) == up).astype(bf16)
    slot_col, begin_col, end_col = spread(slot).T, spread(begin).T, spread(end).T
    hidden_col = spread(jnp.where(shadowed, 1.0, 0.0)).T

    for s in range(steps):
        moves = (begin_col < s) & (end_col >= s)
        kind = jnp.where(moves, jnp.where(end_col == s, 4.0, 3.0), 0.0)
        code_ref[s] = _dot(home, kind.astype(bf16)).astype(bf16)
        number = jnp.where((begin_col == s) & (hidden_col < 0.5), up + 1, 0.0)
        sid_ref[s] = (_dot(home, number.astype(bf16)) - 1).astype(bf16)
    away = (slot_col == across).astype(bf16)
    shape = (steps, seqs)
    pos = lax.broadcasted_iota(jnp.int32, shape, 0).astype(f32) - jnp.broadcast_to(begin, shape)
    tok = jnp.zeros(shape, f32)
    for t in range(1, steps):
        there = (pos == t) & (jnp.broadcast_to(length, shape) > t)
        tok = tok + jnp.where(there, jnp.broadcast_to(tok_ref[t:t + 1, :].astype(f32), shape), 0.0)
    high = jnp.floor(tok / LANES)
    low = tok - high * LANES
    look = _dot(high.astype(bf16), away) * LANES + _dot(low.astype(bf16), away)
    look_ref[...] = look.astype(jnp.int32)


def _plan(options, lengths, tokens):
    steps, seqs = tokens.shape
    bf16 = jnp.bfloat16
    return pl.pallas_call(
        functools.partial(_plan_kernel, options),
        out_shape=(
            jax.ShapeDtypeStruct((steps, seqs, LANES), bf16),
            jax.ShapeDtypeStruct((steps, seqs, LANES), bf16),
            jax.ShapeDtypeStruct((steps, seqs), jnp.int32),
            jax.ShapeDtypeStruct((8, seqs), jnp.float32),
            jax.ShapeDtypeStruct((1, 1), jnp.int32),
        ),
        in_specs=[VMEM, VMEM],
        out_specs=(VMEM, VMEM, VMEM, VMEM, VMEM),
        name='plan',
    )(lengths[None, :], tokens)


def solution(mesh):
    n = mesh.shape['states']

    def local_run(trans_loc, emit_loc, init_loc, tokens_loc, lengths_loc):
        seqs, steps = tokens_loc.shape
        wide = trans_loc.shape[1]
        group = lax.axis_index('states').astype(jnp.int32)[None]
        options = (seqs * 9 // 16, seqs * 5 // 8, seqs)
        code, sid, look, info, pick = _plan(options, lengths_loc, tokens_loc.T)

        def run(k):
            rows = options[k]
            tokens = jnp.concatenate([look[1:, 0:rows].reshape(-1), tokens_loc[:, 0]])
            e_rows = jnp.take(emit_loc, tokens, axis=1, mode='clip').T
            al, a0, xs, at_loc, ccol, ll = _forward(n, 2 * k, rows, trans_loc, e_rows, init_loc[None, :], code, sid, info)
            ws = _backward(n, 2 * k + 1, at_loc, e_rows, ccol, code)
            counts = _pairs(group, trans_loc, xs.reshape(-1, wide), ws.reshape(-1, wide))
            last = jnp.take(al.reshape(steps * rows, wide), info[3].astype(jnp.int32), axis=0, mode='clip')
            return ll[0], jnp.where((lengths_loc == 1)[:, None], a0, last), counts

        return lax.switch(pick[0, 0], [functools.partial(run, k) for k in range(len(options))])

    return jax.shard_map(local_run, mesh=mesh, in_specs=(P(None, 'states'), P('states', None), P('states'), P('seqs', None), P('seqs')), out_specs=(P('seqs'), P('seqs', 'states'), P(('seqs', 'states'), None)), check_vma=False)
```

```python
import functools

import jax
import jax.numpy as jnp
from jax import lax
from jax.experimental import pallas as pl
from jax.experimental.pallas import tpu as pltpu
from jax.sharding import PartitionSpec as P

MESH = pl.DeviceIdType.MESH
ANY = pl.BlockSpec(memory_space=pl.ANY)
VMEM = pl.BlockSpec(memory_space=pltpu.VMEM)
LANES = 128
BOTH = (0, 1)
VMEM_BYTES = 67043328


def _place(n):
    me = lax.axis_index('states')
    core = lax.rem(me, 2)
    chip = lax.div(me, 2)
    partner = chip * 2 + (1 - core)
    right = lax.rem(partner + 2, n)
    left = lax.rem(partner + n - 2, n)
    return me, chip, core, partner, right, left


def _dev(peer):
    return {'states': peer}


def _arrive(me, n):
    for r in range(1, n):
        pl.semaphore_signal(pltpu.get_barrier_semaphore(), inc=1, device_id=_dev(lax.rem(me + r, n)), device_id_type=MESH)


def _all_here(n):
    pl.semaphore_wait(pltpu.get_barrier_semaphore(), n - 1)


def _remote(src, dst, ssem, rsem, peer):
    return pltpu.make_async_remote_copy(src_ref=src, dst_ref=dst, send_sem=ssem, recv_sem=rsem, device_id=_dev(peer), device_id_type=MESH)


def _spans(width, size=LANES):
    return [slice(o, o + size) for o in range(0, width, size)]


def _dot(x, y):
    return jnp.dot(x, y, preferred_element_type=jnp.float32)


def _fwd_kernel(n, steps, rows, nbuf, a_hbm, e_hbm, pi_ref, code_ref, sid_ref, info_ref, al_hbm, a0_hbm, x_hbm, at_hbm, cc_ref, ll_ref,
                g, w, u, al, ebuf, a0b, xi, fs, fr, ta, tt, safe_ref, lacc, tbuf, cs_send, cs_recv,
                e_sem, w_sem, r_sem, out_sem, ta_sem, tt_sem, cs_ss, cs_rs, ici_ss, ici_rs, dd_ss, dd_rs):
    me, chip, core, partner, right, left = _place(n)
    chips = n // 2
    wide = al.shape[1]
    part_w = wide // 4
    seqs = a0b.shape[0]
    a0f = u.at[pl.ds(0, seqs), :]
    quarters = range(4)
    per_step = 2 * 8
    total = (steps - 1) * per_step

    def quarter(j, cls, i):
        far = lax.rem(j + 2 + 2 * i, 4)
        qq = jnp.where(j < 2, 2 * j + i, far)
        off = jnp.where(j < 2, 0, jnp.where(j >= 6, 2, jnp.where(i == 0, chips - 1, 1)))
        c = lax.rem(chip + off, chips)
        k = jnp.where((j >= 2) & (j < 6), cls == 0, cls != 0)
        return (c * 2 + jnp.where(k, 1 - core, core)) * 4 + qq

    def a_part(b):
        return a_hbm.at[pl.ds(pl.multiple_of(b * part_w, part_w), part_w), :]

    def stream(q, slot):
        k = lax.rem(q, per_step)
        return pltpu.make_async_copy(a_part(quarter(lax.div(k, 2), 1, lax.rem(k, 2))), w.at[per_step + slot], w_sem.at[slot])

    def resident(j, i):
        return pltpu.make_async_copy(a_part(quarter(j, 0, i)), w.at[2 * j + i], r_sem.at[2 * j + i])

    def e_rows(first, count, dst, sem):
        return pltpu.make_async_copy(e_hbm.at[pl.ds(pl.multiple_of(first, 8), count), :], dst, sem)

    def e_copy(s):
        return e_rows((s - 1) * rows, rows, ebuf.at[lax.rem(s, 2)], e_sem.at[lax.rem(s, 2)])

    def al_copy(s):
        return pltpu.make_async_copy(al, al_hbm.at[s], out_sem.at[4])

    def mine(b):
        return g.at[b, pl.ds(0, rows), :]

    def x_copy(s, q):
        return pltpu.make_async_copy(mine(me * 4 + q), x_hbm.at[s, :, pl.ds(q * part_w, part_w)], out_sem.at[q])

    pieces, size = at_hbm.shape[0], ta.shape[1]
    fed, depth = ta.shape[0], tt.shape[0]

    def ta_copy(c):
        slot = lax.rem(c, fed)
        return pltpu.make_async_copy(a_hbm.at[pl.ds(pl.multiple_of(c * size, size), size), :], ta.at[slot], ta_sem.at[slot])

    def tt_copy(c):
        slot = lax.rem(c, depth)
        return pltpu.make_async_copy(tt.at[slot], at_hbm.at[c], tt_sem.at[slot])

    def turn(s):
        def one(c, _):
            ta_copy(c).wait()

            @pl.when(c >= depth)
            def _():
                tt_copy(c - depth).wait()

            slot = lax.rem(c, depth)
            tt[slot] = ta[lax.rem(c, fed)].T
            tt_copy(c).start()

            @pl.when(c + fed < pieces)
            def _():
                ta_copy(c + fed).start()

            return 0

        lax.fori_loop(lax.div((s - 1) * pieces, steps - 1), lax.div(s * pieces, steps - 1), one, 0)

    e0_copy = e_rows((steps - 1) * rows, seqs, a0b, e_sem.at[0])
    e0_copy.start()
    _arrive(me, n)

    def load(j, _):
        for i in BOTH:
            resident(j, i).start()
        return 0

    for c in range(fed):
        ta_copy(jnp.int32(c)).start()
    for q in range(nbuf):
        stream(jnp.int32(q), q).start()
    lax.fori_loop(0, 2, load, 0)
    e_copy(jnp.int32(1)).start()
    tbuf[...] = jnp.zeros_like(tbuf)
    lacc[...] = jnp.zeros_like(lacc)
    if g.shape[1] > rows:
        pad = jnp.zeros((g.shape[1] - rows, part_w), jnp.bfloat16)

        def clear(k, _):
            g[k, rows:, :] = pad
            return 0

        lax.fori_loop(0, 4 * n, clear, 0)

    def ici(k, src, dst, i):
        return _remote(src, dst, ici_ss.at[k], ici_rs.at[k], left if i else right)

    def early(i):
        return ici(i, fs.at[i], fr.at[i], i)

    def own_ring(j, i):
        b = me * 4 + (j + 2 + 2 * i) % 4
        return ici(2 * (j - 2) + i, mine(b), mine(b), i)

    def relay(j, i):
        b = quarter(j, 0, i)
        return ici(2 * (j + 2) + i, mine(b), mine(b), i)

    def dd(j, cls, i):
        b = quarter(j, cls, i)
        return _remote(mine(b), mine(b), dd_ss.at[2 * j + i], dd_rs.at[2 * j + i], partner)

    lane = lax.broadcasted_iota(jnp.int32, (rows, seqs), 1).astype(jnp.float32)
    row = lax.broadcasted_iota(jnp.int32, (rows, seqs), 0).astype(jnp.float32)

    def starting(s):
        return sid_ref[s, 0:rows, :].astype(jnp.float32)

    def first_alphas(s):
        pick = (starting(s) == lane).astype(jnp.bfloat16)
        xi[...] = _dot(pick, a0b[...]).astype(jnp.bfloat16)

    def normalizer(part, count, meanwhile):
        tbuf[0:count, :] = part
        row = jnp.sum(tbuf[...].T, axis=0, keepdims=True)
        cs_send[...] = jnp.broadcast_to(row, cs_send.shape)
        cs_recv[me] = jnp.broadcast_to(row, cs_send.shape)
        cps = []
        for r in sorted(range(1, n), key=lambda r: abs(2 * r - n)):
            cp = _remote(cs_send, cs_recv.at[me], cs_ss.at[r - 1], cs_rs.at[r - 1], lax.rem(me + r, n))
            cp.start()
            cps.append(cp)
        meanwhile()
        for cp in cps:
            cp.wait()
        crow = cs_recv[0]
        for r in range(1, n):
            crow = crow + cs_recv[r]
        return crow, jnp.broadcast_to(crow[0:1, :], (LANES, LANES)).T[0:count, :]

    def add_log(s, ccol):
        slot, begin, end = info_ref[0:1, :], info_ref[1:2, :], info_ref[2:3, :]
        now = jnp.full((rows, seqs), s, jnp.int32).astype(jnp.float32)
        here = (slot == row) & (now > begin) & (now <= end)
        lacc[...] += jnp.where(here, jnp.log(jnp.where(here, ccol, 1.0)), 0.0)

    def exchange(s, then):
        own = [own_ring(3, i) for i in BOTH] + [dd(j, 0, i) for j in BOTH for i in BOTH]
        own += [own_ring(j, i) for j in (4, 5) for i in BOTH]
        for cp in own:
            cp.start()
        then()

        def arrived(j):
            for i in BOTH:
                b = quarter(j, 0, i)
                ici(2 * (j - 2) + i, mine(b), mine(b), i).wait_recv()

        def pass_on(j):
            for i in BOTH:
                dd(j, 0, i).start()

        def rounds(h, _):
            j, k = 2 * h, 2 * h + 1

            @pl.when(h == 1)
            def _():
                for i in BOTH:
                    early(i).wait_recv()
                safe = safe_ref[...]
                for i in BOTH:
                    b = quarter(2, 0, i)
                    for cols in _spans(part_w):
                        g[b, 0:rows, cols] = (fr[i, :, cols] / safe).astype(jnp.bfloat16)
                    relay(2, i).start()
                pass_on(2)
                first_alphas(s + 1)

            @pl.when(s == 0)
            def _():
                for r in (j, k):
                    for i in BOTH:
                        resident(r, i).wait()

                    @pl.when(h < 2)
                    def _():
                        load(r + 4, 0)

            @pl.when(h >= 2)
            def _():
                arrived(j)
                pass_on(j)

            def own_class(r):
                return sum(_dot(g[quarter(r, 0, i)], w[2 * r + i]) for i in BOTH)

            def other_class(r):
                q = s * per_step + 2 * r
                slots = [lax.rem(q + i, nbuf) for i in BOTH]
                for i in BOTH:
                    dd(r, 1, i).wait_recv()
                    stream(q + i, slots[i]).wait()
                out = sum(_dot(g[quarter(r, 1, i)], w[per_step + slots[i]]) for i in BOTH)

                for i in BOTH:
                    @pl.when(q + i + nbuf < total)
                    def _():
                        stream(q + i + nbuf, slots[i]).start()

                return out

            prod = own_class(j)

            @pl.when(h >= 1)
            def _():
                arrived(k)

            @pl.when(h == 1)
            def _():
                for i in BOTH:
                    relay(3, i).start()

            @pl.when(h >= 1)
            def _():
                pass_on(k)

            u[...] += prod + own_class(k)
            u[...] += other_class(j)
            u[...] += other_class(k)
            return 0

        lax.fori_loop(0, 4, rounds, 0)
        for i in BOTH:
            early(i).wait_send()
            for j in (2, 3):
                relay(j, i).wait_send()
            for j in range(2, 8):
                dd(j, 0, i).wait_send()
        for cp in own:
            cp.wait_send()

    def keep(s):
        for q in quarters:
            x_copy(s, q).start()

    e0_copy.wait()
    def lanes(q):
        return pl.ds(pl.multiple_of(q * LANES, LANES), LANES)

    def first_mass(q, part):
        a = jnp.broadcast_to(pi_ref[:, lanes(q)], (seqs, LANES)) * a0b[:, lanes(q)].astype(jnp.float32)
        a0f[:, lanes(q)] = a
        return part + a

    part = lax.fori_loop(0, wide // LANES, first_mass, jnp.zeros((seqs, LANES), jnp.float32))
    _all_here(n)

    c0_row, c0 = normalizer(part, seqs, lambda: lax.fori_loop(2, 4, load, 0))
    ll_ref[...] = jnp.log(c0_row)

    def first_alpha(q, _):
        alpha = a0f[:, lanes(q)] / c0
        a0f[:, lanes(q)] = alpha
        a0b[:, lanes(q)] = alpha.astype(jnp.bfloat16)
        return 0

    lax.fori_loop(0, wide // LANES, first_alpha, 0)
    a0_copy = pltpu.make_async_copy(a0f, a0_hbm, e_sem.at[0])
    a0_copy.start()
    first_alphas(0)
    for q, cols in enumerate(_spans(wide, part_w)):
        g[me * 4 + q, 0:rows, :] = xi[:, cols]
    safe_ref[...] = jnp.ones_like(safe_ref)
    for i in BOTH:
        fs[i] = xi[:, 2 * i * part_w:(2 * i + 1) * part_w].astype(jnp.float32)
        early(i).start()
    tbuf[...] = jnp.zeros_like(tbuf)
    a0_copy.wait()
    u[...] = jnp.zeros_like(u)

    def step(s, _):
        exchange(s - 1, lambda: keep(s - 1))
        e_copy(s).wait()

        @pl.when(s + 1 < steps)
        def _():
            e_copy(s + 1).start()

        @pl.when(s > 1)
        def _():
            al_copy(s - 1).wait()

        part = jnp.zeros((rows, LANES), jnp.float32)
        eb = ebuf.at[lax.rem(s, 2)]
        for cols in _spans(wide):
            a = u[0:rows, cols] * eb[:, cols].astype(jnp.float32)
            al[:, cols] = a
            part = part + a
        live = code_ref[s, 0:rows, :].astype(jnp.float32) > 0.5
        starts = starting(s) > -0.5

        def meanwhile():
            @pl.when(s + 1 < steps)
            def _():
                for i in BOTH:
                    for cols in _spans(part_w):
                        from_col = 2 * i * part_w + cols.start
                        src = slice(from_col, from_col + LANES)
                        v = jnp.where(live, al[:, src], 0.0)
                        fs[i, :, cols] = jnp.where(starts, xi[:, src].astype(jnp.float32), v)
                    early(i).start()

            turn(s)
            u[...] = jnp.zeros_like(u)

            @pl.when(s > 1)
            def _():
                add_log(s - 1, cc_ref[s - 1])

            for q in quarters:
                x_copy(s - 1, q).wait()

        _, ccol = normalizer(part, rows, meanwhile)
        cc_ref[s] = ccol
        safe = jnp.where(live, ccol, 1.0)
        safe_ref[...] = jnp.where(starts, 1.0, safe)
        for q, block in enumerate(_spans(wide, part_w)):
            for cols in _spans(part_w):
                src = slice(block.start + cols.start, block.start + cols.stop)
                alpha = jnp.where(live, al[:, src] / safe, 0.0)
                al[:, src] = alpha
                x = jnp.where(starts, xi[:, src].astype(jnp.float32), alpha)
                g[me * 4 + q, 0:rows, cols] = x.astype(jnp.bfloat16)

        al_copy(s).start()
        return 0

    lax.fori_loop(1, steps, step, 0)
    add_log(steps - 1, cc_ref[steps - 1])
    ll_ref[...] += jnp.sum(lacc[...], axis=0, keepdims=True)
    al_copy(steps - 1).wait()
    for c in range(depth):
        tt_copy(pieces - depth + c).wait()


def _forward(n, cid, rows, a_loc, e_rows, init_loc, code, sid, info):
    wide = a_loc.shape[1]
    steps, seqs, _ = code.shape
    part_w = wide // 4
    full = max(LANES, rows)
    nbuf = 6 if rows <= 80 else 4
    f32, bf16 = jnp.float32, jnp.bfloat16
    dma = pltpu.SemaphoreType.DMA
    return pl.pallas_call(
        functools.partial(_fwd_kernel, n, steps, rows, nbuf),
        out_shape=(
            jax.ShapeDtypeStruct((steps, rows, wide), f32),
            jax.ShapeDtypeStruct((seqs, wide), f32),
            jax.ShapeDtypeStruct((steps - 1, rows, wide), bf16),
            jax.ShapeDtypeStruct((2 * a_loc.shape[0] // part_w, wide, part_w // 2), bf16),
            jax.ShapeDtypeStruct((steps, rows, LANES), f32),
            jax.ShapeDtypeStruct((8, LANES), f32),
        ),
        in_specs=[ANY, ANY, VMEM, VMEM, VMEM, VMEM],
        out_specs=(ANY, ANY, ANY, ANY, VMEM, VMEM),
        scratch_shapes=[
            pltpu.VMEM((4 * n, full, part_w), bf16),
            pltpu.VMEM((2 * n + nbuf, part_w, wide), bf16),
            pltpu.VMEM((full, wide), f32),
            pltpu.VMEM((rows, wide), f32),
            pltpu.VMEM((2, rows, wide), bf16),
            pltpu.VMEM((seqs, wide), bf16),
            pltpu.VMEM((rows, wide), bf16),
            pltpu.VMEM((2, rows, part_w), f32),
            pltpu.VMEM((2, rows, part_w), f32),
            pltpu.VMEM((5, part_w // 2, wide), bf16),
            pltpu.VMEM((4, wide, part_w // 2), bf16),
            pltpu.VMEM((rows, LANES), f32),
            pltpu.VMEM((rows, LANES), f32),
            pltpu.VMEM((LANES, LANES), f32),
            pltpu.VMEM((8, LANES), f32),
            pltpu.VMEM((n, 8, LANES), f32),
            dma((2,)), dma((nbuf,)), dma((2 * n,)), dma((5,)), dma((5,)), dma((4,)),
            dma((n - 1,)), dma((n - 1,)),
            dma((12,)), dma((12,)), dma((2 * n,)), dma((2 * n,)),
        ],
        compiler_params=pltpu.CompilerParams(collective_id=cid, has_side_effects=True, vmem_limit_bytes=VMEM_BYTES),
        name='forward',
    )(a_loc, e_rows, init_loc, code, sid, info)


def _bwd_kernel(n, steps, rows, nbuf, at_hbm, e_hbm, cc_ref, code_ref, w_hbm,
                w, wv, ebuf, pp, rp, rs, rin,
                e_sem, w_sem, r_sem, out_sem, dd_ss, dd_rs, ici_ss, ici_rs):
    me, chip, core, partner, right, left = _place(n)
    chips = n // 2
    wide = wv.shape[1]
    size = at_hbm.shape[2]
    per = wide // size // 2
    trips = steps - 2
    rounds_n = 4 * per
    count = 2 * rounds_n
    ringed = 6 * per
    total = trips * rounds_n

    def piece(j, cls, i):
        p, e = lax.div(j, per), lax.rem(j, per)
        hh = jnp.where(p == 1, 1 - i, i)
        off = jnp.where(p == 0, 2, jnp.where(p == 3, 0, chips - 1 if i else 1))
        c = lax.rem(chip + off, chips)
        hop = (p == 1) | (p == 2)
        k = jnp.where(hop, core if cls else 1 - core, 1 - core if cls else core)
        return (c * 2 + k) * 2 * per + hh * per + e

    def fetch(j, cls, i, slot, sem):
        return pltpu.make_async_copy(at_hbm.at[piece(j, cls, i)], w.at[slot, :, pl.ds(i * size, size)], sem)

    def stream(j, i, slot):
        return fetch(j, 1, i, rounds_n + slot, w_sem.at[slot, i])

    def resident(j, i):
        return fetch(j, 0, i, j, r_sem.at[j, i])

    def e_copy(t):
        first = pl.multiple_of((steps - 2 - t) * rows, 8)
        return pltpu.make_async_copy(e_hbm.at[pl.ds(first, rows), :], ebuf.at[lax.rem(t, 2)], e_sem.at[lax.rem(t, 2)])

    def w_copy(t):
        return pltpu.make_async_copy(wv.at[pl.ds(0, rows), :], w_hbm.at[steps - 2 - t], out_sem)

    for t in BOTH:
        e_copy(jnp.int32(t)).start()
    _arrive(me, n)

    def load(j, _):
        for i in BOTH:
            resident(j, i).start()
        return 0

    for q in BOTH:
        for i in BOTH:
            stream(jnp.int32(q), i, q).start()
        load(jnp.int32(q), 0)
    if wv.shape[0] > rows:
        wv[rows:, :] = jnp.zeros((wv.shape[0] - rows, wide), jnp.bfloat16)

    def dd(k):
        return _remote(pp.at[k], rp.at[k], dd_ss.at[k], dd_rs.at[k], partner)

    def ring(k, par, i):
        return _remote(rs.at[k], rin.at[par, k], ici_ss.at[k], ici_rs.at[par, k], left if i else right)

    def weigh(s, eb, o, beta):
        code = code_ref[s, 0:rows, :].astype(jnp.float32)
        ok = code > 2.5
        safe = jnp.where(ok, cc_ref[s], 1.0)
        for cols in _spans(size):
            dst = slice(o + cols.start, o + cols.stop)
            b = 1.0 if beta is None else jnp.where(code > 3.5, 1.0, beta[:, cols])
            v = eb[:, dst].astype(jnp.float32) * b / safe
            wv[0:rows, dst] = jnp.where(ok, v, 0.0).astype(jnp.bfloat16)

    e_copy(jnp.int32(0)).wait()
    for cols in _spans(wide, size):
        weigh(steps - 1, ebuf.at[0], cols.start, None)
    ahead = 4
    for q in range(2, nbuf):
        for i in BOTH:
            stream(jnp.int32(q), i, q).start()
    for q in range(2, ahead):
        load(jnp.int32(q), 0)
    w_copy(jnp.int32(0)).start()
    _all_here(n)

    def step(t, _):
        par = lax.rem(t, 2)

        def finish(j):
            p = lax.div(j, per)
            for i in BOTH:
                dd(2 * j + i).wait_recv()

            @pl.when(p == 2)
            def _():
                for i in BOTH:
                    k = 2 * j + i
                    c = k - 4 * per
                    ring(c, par, i).wait_recv()
                    rp[k] += rin[par, c]

            for i in BOTH:
                k = 2 * j + i
                rs[k] += rp[k]

            @pl.when(p < 3)
            def _():
                for i in BOTH:
                    ring(2 * j + i, par, i).start()

        def rounds(j, _):
            q = t * rounds_n + j
            slot = lax.rem(q, nbuf)
            for i in BOTH:
                stream(j, i, slot).wait()
            prod = _dot(wv[...], w[rounds_n + slot])
            for i, cols in enumerate(_spans(2 * size, size)):
                k = 2 * j + i
                pp[k] = prod[0:rows, cols]
                dd(k).start()

            @pl.when(q + nbuf < total)
            def _():
                for i in BOTH:
                    stream(lax.rem(j + nbuf, rounds_n), i, slot).start()

            @pl.when(j > 0)
            def _():
                finish(j - 1)

            @pl.when(t == 0)
            def _():
                for i in BOTH:
                    resident(j, i).wait()

                @pl.when(j < rounds_n - ahead)
                def _():
                    load(j + ahead, 0)

            prod = _dot(wv[...], w[j])
            for i, cols in enumerate(_spans(2 * size, size)):
                rs[2 * j + i] = prod[0:rows, cols]
            return 0

        lax.fori_loop(0, rounds_n, rounds, 0)
        finish(jnp.int32(rounds_n - 1))

        def gone(k, _):
            dd(k).wait_send()
            return 0

        def sent(k, _):
            ring(k, par, 0).wait_send()
            return 0

        lax.fori_loop(0, count, gone, 0)
        lax.fori_loop(0, 4 * per, sent, 0)
        nxt = t + 1
        e_copy(nxt).wait()

        @pl.when(nxt + 1 < steps - 1)
        def _():
            e_copy(nxt + 1).start()

        w_copy(t).wait()
        eb = ebuf.at[lax.rem(nxt, 2)]
        for e in range(per):
            for i in BOTH:
                near, late = 2 * (per + e) + 1 - i, 2 * (2 * per + e) + i
                ring(near, par, 1 - i).wait_recv()
                ring(late, par, i).wait_recv()
                beta = rs[ringed + 2 * e + i] + rin[par, near] + rin[par, late]
                weigh(steps - 1 - nxt, eb, (i * per + e) * size, beta)
        w_copy(nxt).start()
        lax.fori_loop(4 * per, ringed, sent, 0)
        return 0

    lax.fori_loop(0, trips, step, 0)
    w_copy(jnp.int32(trips)).wait()


def _backward(n, cid, at_loc, e_rows, ccol, code):
    pieces, wide, size = at_loc.shape
    steps, rows, _ = ccol.shape
    full = max(LANES, rows)
    count = pieces // 2
    nbuf = 6 if rows <= 80 else 4
    ringed = 3 * count // 4
    f32, bf16 = jnp.float32, jnp.bfloat16
    dma = pltpu.SemaphoreType.DMA
    return pl.pallas_call(
        functools.partial(_bwd_kernel, n, steps, rows, nbuf),
        out_shape=jax.ShapeDtypeStruct((steps - 1, rows, wide), bf16),
        in_specs=[ANY, ANY, VMEM, VMEM],
        out_specs=ANY,
        scratch_shapes=[
            pltpu.VMEM((count // 2 + nbuf, wide, 2 * size), bf16),
            pltpu.VMEM((full, wide), bf16),
            pltpu.VMEM((2, rows, wide), bf16),
            pltpu.VMEM((count, rows, size), f32),
            pltpu.VMEM((count, rows, size), f32),
            pltpu.VMEM((count, rows, size), f32),
            pltpu.VMEM((2, ringed, rows, size), f32),
            dma((2,)), dma((nbuf, 2)), dma((count // 2, 2)), dma(()),
            dma((count,)), dma((count,)),
            dma((ringed,)), dma((2, ringed)),
        ],
        compiler_params=pltpu.CompilerParams(collective_id=cid, has_side_effects=True, vmem_limit_bytes=VMEM_BYTES),
        name='backward',
    )(at_loc, e_rows, ccol, code)


def _pair_kernel(group_ref, a_ref, x_ref, w_ref, o_ref):
    pair_sum = lax.dot_general(x_ref[...], w_ref[...], (((0,), (0,)), ((), ())), preferred_element_type=jnp.float32)
    o_ref[...] = a_ref[...].astype(jnp.float32) * pair_sum


def _pairs(group, a_loc, xs, ws):
    depth, wide = ws.shape
    size = wide // 8
    tiles = wide // size
    return pl.pallas_call(
        _pair_kernel,
        out_shape=jax.ShapeDtypeStruct((wide, wide), jnp.float32),
        grid_spec=pltpu.PrefetchScalarGridSpec(
            num_scalar_prefetch=1,
            grid=(tiles,),
            in_specs=[
                pl.BlockSpec((size, wide), lambda i, group_ref: (group_ref[0] * tiles + i, 0)),
                pl.BlockSpec((depth, size), lambda i, group_ref: (0, i)),
                pl.BlockSpec((depth, wide), lambda i, group_ref: (0, 0)),
            ],
            out_specs=pl.BlockSpec((size, wide), lambda i, group_ref: (i, 0)),
        ),
        compiler_params=pltpu.CompilerParams(vmem_limit_bytes=VMEM_BYTES),
        name='pairs',
    )(group, a_loc, xs, ws)


def _plan_kernel(options, len_ref, tok_ref, code_ref, sid_ref, look_ref, info_ref, pick_ref):
    seqs = len_ref.shape[1]
    steps = tok_ref.shape[0]
    f32, bf16 = jnp.float32, jnp.bfloat16
    square = (seqs, seqs)
    up = lax.broadcasted_iota(jnp.int32, square, 0).astype(f32)
    across = lax.broadcasted_iota(jnp.int32, square, 1).astype(f32)

    def spread(row):
        return jnp.broadcast_to(row, square)

    def total(x):
        return jnp.sum(x, axis=0, keepdims=True)

    length = len_ref[...].astype(f32)
    l_row = spread(length)
    l_col = l_row.T
    ahead = (l_col > l_row) | ((l_col == l_row) & (up < across))
    rank = total(jnp.where(ahead, 1.0, 0.0))
    rank_col = spread(rank).T

    def mates(slots):
        slot = jnp.where(rank < slots, rank, 2 * slots - 1 - rank)
        return slot, total(jnp.where(rank_col == spread(slot), l_col, 0.0))

    slots = jnp.full((1, 1), seqs, jnp.int32).astype(f32)
    pick = jnp.full((1, 1), len(options) - 1, jnp.int32)
    for k in reversed(range(len(options) - 1)):
        _, first = mates(options[k])
        worst = jnp.max(jnp.where(rank < options[k], 0.0, first + length), axis=1, keepdims=True)
        fits = worst <= steps + 1
        slots = jnp.where(fits, options[k], slots)
        pick = jnp.where(fits, k, pick)
    pick_ref[...] = pick
    slot, first = mates(slots)
    opens = rank < slots
    begin = jnp.where(opens, 0.0, first - 1)
    end = begin + length - 1
    info_ref[0:1, :] = slot
    info_ref[1:2, :] = begin
    info_ref[2:3, :] = end
    info_ref[3:4, :] = end * slots + slot

    double = total(jnp.where((spread(slot).T == spread(slot)) & (up != across), 1.0, 0.0))
    shadowed = opens & (length < 1.5) & (double > 0.5)
    home = (spread(slot) == up).astype(bf16)
    slot_col, begin_col, end_col = spread(slot).T, spread(begin).T, spread(end).T
    hidden_col = spread(jnp.where(shadowed, 1.0, 0.0)).T

    for s in range(steps):
        moves = (begin_col < s) & (end_col >= s)
        kind = jnp.where(moves, jnp.where(end_col == s, 4.0, 3.0), 0.0)
        code_ref[s] = _dot(home, kind.astype(bf16)).astype(bf16)
        number = jnp.where((begin_col == s) & (hidden_col < 0.5), up + 1, 0.0)
        sid_ref[s] = (_dot(home, number.astype(bf16)) - 1).astype(bf16)
    away = (slot_col == across).astype(bf16)
    shape = (steps, seqs)
    pos = lax.broadcasted_iota(jnp.int32, shape, 0).astype(f32) - jnp.broadcast_to(begin, shape)
    tok = jnp.zeros(shape, f32)
    for t in range(1, steps):
        there = (pos == t) & (jnp.broadcast_to(length, shape) > t)
        tok = tok + jnp.where(there, jnp.broadcast_to(tok_ref[t:t + 1, :].astype(f32), shape), 0.0)
    high = jnp.floor(tok / LANES)
    low = tok - high * LANES
    look = _dot(high.astype(bf16), away) * LANES + _dot(low.astype(bf16), away)
    look_ref[...] = look.astype(jnp.int32)


def _plan(options, lengths, tokens):
    steps, seqs = tokens.shape
    bf16 = jnp.bfloat16
    return pl.pallas_call(
        functools.partial(_plan_kernel, options),
        out_shape=(
            jax.ShapeDtypeStruct((steps, seqs, LANES), bf16),
            jax.ShapeDtypeStruct((steps, seqs, LANES), bf16),
            jax.ShapeDtypeStruct((steps, seqs), jnp.int32),
            jax.ShapeDtypeStruct((8, seqs), jnp.float32),
            jax.ShapeDtypeStruct((1, 1), jnp.int32),
        ),
        in_specs=[VMEM, VMEM],
        out_specs=(VMEM, VMEM, VMEM, VMEM, VMEM),
        name='plan',
    )(lengths[None, :], tokens)


def solution(mesh):
    n = mesh.shape['states']

    def local_run(trans_loc, emit_loc, init_loc, tokens_loc, lengths_loc):
        seqs, steps = tokens_loc.shape
        wide = trans_loc.shape[1]
        group = lax.axis_index('states').astype(jnp.int32)[None]
        options = (seqs * 9 // 16, seqs * 5 // 8, seqs)
        code, sid, look, info, pick = _plan(options, lengths_loc, tokens_loc.T)

        def run(k):
            rows = options[k]
            tokens = jnp.concatenate([look[1:, 0:rows].reshape(-1), tokens_loc[:, 0]])
            e_rows = jnp.take(emit_loc, tokens, axis=1, mode='clip').T
            al, a0, xs, at_loc, ccol, ll = _forward(n, 2 * k, rows, trans_loc, e_rows, init_loc[None, :], code, sid, info)
            ws = _backward(n, 2 * k + 1, at_loc, e_rows, ccol, code)
            counts = _pairs(group, trans_loc, xs.reshape(-1, wide), ws.reshape(-1, wide))
            last = jnp.take(al.reshape(steps * rows, wide), info[3].astype(jnp.int32), axis=0, mode='clip')
            return ll[0], jnp.where((lengths_loc == 1)[:, None], a0, last), counts

        return lax.switch(pick[0, 0], [functools.partial(run, k) for k in range(len(options))])

    return jax.shard_map(local_run, mesh=mesh, in_specs=(P(None, 'states'), P('states', None), P('states'), P('seqs', None), P('seqs')), out_specs=(P('seqs'), P('seqs', 'states'), P(('seqs', 'states'), None)), check_vma=False)
```

```python
import functools

import jax
import jax.numpy as jnp
from jax import lax
from jax.experimental import pallas as pl
from jax.experimental.pallas import tpu as pltpu
from jax.sharding import PartitionSpec as P

MESH = pl.DeviceIdType.MESH
ANY = pl.BlockSpec(memory_space=pl.ANY)
VMEM = pl.BlockSpec(memory_space=pltpu.VMEM)
LANES = 128
BOTH = (0, 1)
VMEM_BYTES = 67043328


def _place(n):
    me = lax.axis_index('states')
    core = lax.rem(me, 2)
    chip = lax.div(me, 2)
    partner = chip * 2 + (1 - core)
    right = lax.rem(partner + 2, n)
    left = lax.rem(partner + n - 2, n)
    return me, chip, core, partner, right, left


def _dev(peer):
    return {'states': peer}


def _arrive(me, n):
    for r in range(1, n):
        pl.semaphore_signal(pltpu.get_barrier_semaphore(), inc=1, device_id=_dev(lax.rem(me + r, n)), device_id_type=MESH)


def _all_here(n):
    pl.semaphore_wait(pltpu.get_barrier_semaphore(), n - 1)


def _remote(src, dst, ssem, rsem, peer):
    return pltpu.make_async_remote_copy(src_ref=src, dst_ref=dst, send_sem=ssem, recv_sem=rsem, device_id=_dev(peer), device_id_type=MESH)


def _spans(width, size=LANES):
    return [slice(o, o + size) for o in range(0, width, size)]


def _dot(x, y):
    return jnp.dot(x, y, preferred_element_type=jnp.float32)


def _fwd_kernel(n, steps, rows, nbuf, a_hbm, e_hbm, pi_ref, code_ref, sid_ref, info_ref, al_hbm, x_hbm, at_hbm, cc_ref, ll_ref,
                g, w, u, al, ebuf, a0b, xi, fs, fr, ta, tt, safe_ref, lacc, tbuf, cs_send, cs_recv,
                e_sem, w_sem, r_sem, out_sem, ta_sem, tt_sem, cs_ss, cs_rs, ici_ss, ici_rs, dd_ss, dd_rs):
    me, chip, core, partner, right, left = _place(n)
    chips = n // 2
    wide = al.shape[1]
    part_w = wide // 4
    seqs = a0b.shape[0]
    a0f = u.at[pl.ds(0, seqs), :]
    quarters = range(4)
    per_step = 2 * 8
    total = (steps - 1) * per_step

    def quarter(j, cls, i):
        far = lax.rem(j + 2 + 2 * i, 4)
        qq = jnp.where(j < 2, 2 * j + i, far)
        off = jnp.where(j < 2, 0, jnp.where(j >= 6, 2, jnp.where(i == 0, chips - 1, 1)))
        c = lax.rem(chip + off, chips)
        k = jnp.where((j >= 2) & (j < 6), cls == 0, cls != 0)
        return (c * 2 + jnp.where(k, 1 - core, core)) * 4 + qq

    def a_part(b):
        return a_hbm.at[pl.ds(pl.multiple_of(b * part_w, part_w), part_w), :]

    def stream(q, slot):
        k = lax.rem(q, per_step)
        return pltpu.make_async_copy(a_part(quarter(lax.div(k, 2), 1, lax.rem(k, 2))), w.at[per_step + slot], w_sem.at[slot])

    def resident(j, i):
        return pltpu.make_async_copy(a_part(quarter(j, 0, i)), w.at[2 * j + i], r_sem.at[2 * j + i])

    def e_rows(first, count, dst, sem):
        return pltpu.make_async_copy(e_hbm.at[pl.ds(pl.multiple_of(first, 8), count), :], dst, sem)

    def e_copy(s):
        return e_rows((s - 1) * rows, rows, ebuf.at[lax.rem(s, 2)], e_sem.at[lax.rem(s, 2)])

    def al_copy(s):
        return pltpu.make_async_copy(al, al_hbm.at[pl.ds(pl.multiple_of((s - 1) * rows, 8), rows), :], out_sem.at[4])

    def mine(b):
        return g.at[b, pl.ds(0, rows), :]

    def x_copy(s, q):
        return pltpu.make_async_copy(mine(me * 4 + q), x_hbm.at[s, :, pl.ds(q * part_w, part_w)], out_sem.at[q])

    pieces, size = at_hbm.shape[0], ta.shape[1]
    fed, depth = ta.shape[0], tt.shape[0]

    def ta_copy(c):
        slot = lax.rem(c, fed)
        return pltpu.make_async_copy(a_hbm.at[pl.ds(pl.multiple_of(c * size, size), size), :], ta.at[slot], ta_sem.at[slot])

    def tt_copy(c):
        slot = lax.rem(c, depth)
        return pltpu.make_async_copy(tt.at[slot], at_hbm.at[c], tt_sem.at[slot])

    def turn(s):
        def one(c, _):
            ta_copy(c).wait()

            @pl.when(c >= depth)
            def _():
                tt_copy(c - depth).wait()

            slot = lax.rem(c, depth)
            tt[slot] = ta[lax.rem(c, fed)].T
            tt_copy(c).start()

            @pl.when(c + fed < pieces)
            def _():
                ta_copy(c + fed).start()

            return 0

        @pl.when(s == 1)
        def _():
            for c in range(fed):
                ta_copy(jnp.int32(c)).start()

        lax.fori_loop(lax.div(jnp.maximum(s - 2, 0) * pieces, steps - 2), lax.div((s - 1) * pieces, steps - 2), one, 0)

    e0_copy = e_rows((steps - 1) * rows, seqs, a0b, e_sem.at[0])
    e0_copy.start()
    _arrive(me, n)

    def load(j, _):
        for i in BOTH:
            resident(j, i).start()
        return 0

    for q in range(nbuf):
        stream(jnp.int32(q), q).start()
    lax.fori_loop(0, 2, load, 0)
    e_copy(jnp.int32(1)).start()
    tbuf[...] = jnp.zeros_like(tbuf)
    lacc[...] = jnp.zeros_like(lacc)
    if g.shape[1] > rows:
        pad = jnp.zeros((g.shape[1] - rows, part_w), jnp.bfloat16)

        def clear(k, _):
            g[k, rows:, :] = pad
            return 0

        lax.fori_loop(0, 4 * n, clear, 0)

    def ici(k, src, dst, i):
        return _remote(src, dst, ici_ss.at[k], ici_rs.at[k], left if i else right)

    def early(i):
        return ici(i, fs.at[i], fr.at[i], i)

    def own_ring(j, i):
        b = me * 4 + (j + 2 + 2 * i) % 4
        return ici(2 * (j - 2) + i, mine(b), mine(b), i)

    def relay(j, i):
        b = quarter(j, 0, i)
        return ici(2 * (j + 2) + i, mine(b), mine(b), i)

    def dd(j, cls, i):
        b = quarter(j, cls, i)
        return _remote(mine(b), mine(b), dd_ss.at[2 * j + i], dd_rs.at[2 * j + i], partner)

    lane = lax.broadcasted_iota(jnp.int32, (rows, seqs), 1).astype(jnp.float32)
    row = lax.broadcasted_iota(jnp.int32, (rows, seqs), 0).astype(jnp.float32)

    def starting(s):
        return sid_ref[s, 0:rows, :].astype(jnp.float32)

    def first_alphas(s):
        pick = (starting(s) == lane).astype(jnp.bfloat16)
        xi[...] = _dot(pick, a0b[...]).astype(jnp.bfloat16)

    def normalizer(part, count, meanwhile):
        tbuf[0:count, :] = part
        row = jnp.sum(tbuf[...].T, axis=0, keepdims=True)
        cs_send[...] = jnp.broadcast_to(row, cs_send.shape)
        cs_recv[me] = jnp.broadcast_to(row, cs_send.shape)
        cps = []
        for r in sorted(range(1, n), key=lambda r: abs(2 * r - n)):
            cp = _remote(cs_send, cs_recv.at[me], cs_ss.at[r - 1], cs_rs.at[r - 1], lax.rem(me + r, n))
            cp.start()
            cps.append(cp)
        meanwhile()
        for cp in cps:
            cp.wait()
        crow = cs_recv[0]
        for r in range(1, n):
            crow = crow + cs_recv[r]
        return crow, jnp.broadcast_to(crow[0:1, :], (LANES, LANES)).T[0:count, :]

    def add_log(s, ccol):
        slot, begin, end = info_ref[0:1, :], info_ref[1:2, :], info_ref[2:3, :]
        now = jnp.full((rows, seqs), s, jnp.int32).astype(jnp.float32)
        here = (slot == row) & (now > begin) & (now <= end)
        lacc[...] += jnp.where(here, jnp.log(jnp.where(here, ccol, 1.0)), 0.0)

    def exchange(s, then):
        own = [dd(j, 0, i) for j in BOTH for i in BOTH]
        own += [own_ring(j, i) for j in (4, 5) for i in BOTH]
        for cp in own:
            cp.start()
        then()

        def arrived(j):
            for i in BOTH:
                b = quarter(j, 0, i)
                ici(2 * (j - 2) + i, mine(b), mine(b), i).wait_recv()

        def pass_on(j):
            for i in BOTH:
                dd(j, 0, i).start()

        def rounds(h, _):
            j, k = 2 * h, 2 * h + 1

            @pl.when(h == 1)
            def _():
                for i in BOTH:
                    early(i).wait_recv()
                safe = safe_ref[...]
                for i in BOTH:
                    b = quarter(2, 0, i)
                    for cols in _spans(part_w):
                        g[b, 0:rows, cols] = (fr[i, :, cols] / safe).astype(jnp.bfloat16)
                    relay(2, i).start()
                pass_on(2)
                first_alphas(s + 1)

            @pl.when(s == 0)
            def _():
                for r in (j, k):
                    for i in BOTH:
                        resident(r, i).wait()

                    @pl.when(h < 2)
                    def _():
                        load(r + 4, 0)

            @pl.when(h >= 2)
            def _():
                arrived(j)
                pass_on(j)

            def own_class(r):
                return sum(_dot(g[quarter(r, 0, i)], w[2 * r + i]) for i in BOTH)

            def other_class(r):
                q = s * per_step + 2 * r
                slots = [lax.rem(q + i, nbuf) for i in BOTH]
                for i in BOTH:
                    dd(r, 1, i).wait_recv()
                    stream(q + i, slots[i]).wait()
                out = sum(_dot(g[quarter(r, 1, i)], w[per_step + slots[i]]) for i in BOTH)

                for i in BOTH:
                    @pl.when(q + i + nbuf < total)
                    def _():
                        stream(q + i + nbuf, slots[i]).start()

                return out

            prod = own_class(j)

            @pl.when(h >= 1)
            def _():
                arrived(k)

            @pl.when(h == 1)
            def _():
                for i in BOTH:
                    relay(3, i).start()

            @pl.when(h >= 1)
            def _():
                pass_on(k)

            u[...] += prod + own_class(k)
            u[...] += other_class(j)
            u[...] += other_class(k)
            return 0

        lax.fori_loop(0, 4, rounds, 0)
        for i in BOTH:
            early(i).wait_send()
            for j in (2, 3):
                relay(j, i).wait_send()
            for j in range(2, 8):
                dd(j, 0, i).wait_send()
        for cp in own + [own_ring(3, i) for i in BOTH]:
            cp.wait_send()

    def keep(s):
        for q in quarters:
            x_copy(s, q).start()

    e0_copy.wait()
    def lanes(q):
        return pl.ds(pl.multiple_of(q * LANES, LANES), LANES)

    def first_mass(q, part):
        a = jnp.broadcast_to(pi_ref[:, lanes(q)], (seqs, LANES)) * a0b[:, lanes(q)].astype(jnp.float32)
        a0f[:, lanes(q)] = a
        return part + a

    part = lax.fori_loop(0, wide // LANES, first_mass, jnp.zeros((seqs, LANES), jnp.float32))
    _all_here(n)

    c0_row, c0 = normalizer(part, seqs, lambda: lax.fori_loop(2, 4, load, 0))
    ll_ref[...] = jnp.log(c0_row)

    def first_alpha(q, _):
        alpha = a0f[:, lanes(q)] / c0
        a0f[:, lanes(q)] = alpha
        a0b[:, lanes(q)] = alpha.astype(jnp.bfloat16)
        return 0

    lax.fori_loop(0, wide // LANES, first_alpha, 0)
    a0_copy = pltpu.make_async_copy(a0f, al_hbm.at[pl.ds((steps - 1) * rows, seqs), :], e_sem.at[0])
    a0_copy.start()
    first_alphas(0)
    for q, cols in enumerate(_spans(wide, part_w)):
        g[me * 4 + q, 0:rows, :] = xi[:, cols]
    for i in BOTH:
        own_ring(3, i).start()
    safe_ref[...] = jnp.ones_like(safe_ref)
    for i in BOTH:
        fs[i] = xi[:, 2 * i * part_w:(2 * i + 1) * part_w].astype(jnp.float32)
        early(i).start()
    tbuf[...] = jnp.zeros_like(tbuf)
    a0_copy.wait()
    u[...] = jnp.zeros_like(u)

    def step(s, _):
        exchange(s - 1, lambda: keep(s - 1))
        e_copy(s).wait()

        @pl.when(s + 1 < steps)
        def _():
            e_copy(s + 1).start()

        @pl.when(s > 1)
        def _():
            al_copy(s - 1).wait()

        part = jnp.zeros((rows, LANES), jnp.float32)
        eb = ebuf.at[lax.rem(s, 2)]
        for cols in _spans(wide):
            a = u[0:rows, cols] * eb[:, cols].astype(jnp.float32)
            al[:, cols] = a
            part = part + a
        live = code_ref[s, 0:rows, :].astype(jnp.float32) > 0.5
        starts = starting(s) > -0.5

        def meanwhile():
            @pl.when(s + 1 < steps)
            def _():
                for i in BOTH:
                    for cols in _spans(part_w):
                        from_col = 2 * i * part_w + cols.start
                        src = slice(from_col, from_col + LANES)
                        v = jnp.where(live, al[:, src], 0.0)
                        fs[i, :, cols] = jnp.where(starts, xi[:, src].astype(jnp.float32), v)
                    early(i).start()

            turn(s)
            u[...] = jnp.zeros_like(u)

            @pl.when(s > 1)
            def _():
                add_log(s - 1, cc_ref[s - 1])

            for q in quarters:
                x_copy(s - 1, q).wait()

        _, ccol = normalizer(part, rows, meanwhile)
        cc_ref[s] = ccol
        safe = jnp.where(live, ccol, 1.0)
        safe_ref[...] = jnp.where(starts, 1.0, safe)
        blocks = _spans(wide, part_w)
        for q in (1, 3, 0, 2):
            for cols in _spans(part_w):
                src = slice(blocks[q].start + cols.start, blocks[q].start + cols.stop)
                alpha = jnp.where(live, al[:, src] / safe, 0.0)
                al[:, src] = alpha
                x = jnp.where(starts, xi[:, src].astype(jnp.float32), alpha)
                g[me * 4 + q, 0:rows, cols] = x.astype(jnp.bfloat16)

            if q % 2:
                @pl.when(s + 1 < steps)
                def _():
                    own_ring(3, q // 2).start()

        al_copy(s).start()
        return 0

    lax.fori_loop(1, steps, step, 0)
    add_log(steps - 1, cc_ref[steps - 1])
    ll_ref[...] += jnp.sum(lacc[...], axis=0, keepdims=True)
    al_copy(steps - 1).wait()
    for c in range(depth):
        tt_copy(pieces - depth + c).wait()


def _forward(n, cid, rows, a_loc, e_rows, init_loc, code, sid, info):
    wide = a_loc.shape[1]
    steps, seqs, _ = code.shape
    part_w = wide // 4
    full = max(LANES, rows)
    nbuf = 6 if rows <= 80 else 4
    f32, bf16 = jnp.float32, jnp.bfloat16
    dma = pltpu.SemaphoreType.DMA
    return pl.pallas_call(
        functools.partial(_fwd_kernel, n, steps, rows, nbuf),
        out_shape=(
            jax.ShapeDtypeStruct(((steps - 1) * rows + seqs, wide), f32),
            jax.ShapeDtypeStruct((steps - 1, rows, wide), bf16),
            jax.ShapeDtypeStruct((2 * a_loc.shape[0] // part_w, wide, part_w // 2), bf16),
            jax.ShapeDtypeStruct((steps, rows, LANES), f32),
            jax.ShapeDtypeStruct((8, LANES), f32),
        ),
        in_specs=[ANY, ANY, VMEM, VMEM, VMEM, VMEM],
        out_specs=(ANY, ANY, ANY, VMEM, VMEM),
        scratch_shapes=[
            pltpu.VMEM((4 * n, full, part_w), bf16),
            pltpu.VMEM((2 * n + nbuf, part_w, wide), bf16),
            pltpu.VMEM((full, wide), f32),
            pltpu.VMEM((rows, wide), f32),
            pltpu.VMEM((2, rows, wide), bf16),
            pltpu.VMEM((seqs, wide), bf16),
            pltpu.VMEM((rows, wide), bf16),
            pltpu.VMEM((2, rows, part_w), f32),
            pltpu.VMEM((2, rows, part_w), f32),
            pltpu.VMEM((5, part_w // 2, wide), bf16),
            pltpu.VMEM((4, wide, part_w // 2), bf16),
            pltpu.VMEM((rows, LANES), f32),
            pltpu.VMEM((rows, LANES), f32),
            pltpu.VMEM((LANES, LANES), f32),
            pltpu.VMEM((8, LANES), f32),
            pltpu.VMEM((n, 8, LANES), f32),
            dma((2,)), dma((nbuf,)), dma((2 * n,)), dma((5,)), dma((5,)), dma((4,)),
            dma((n - 1,)), dma((n - 1,)),
            dma((12,)), dma((12,)), dma((2 * n,)), dma((2 * n,)),
        ],
        compiler_params=pltpu.CompilerParams(collective_id=cid, has_side_effects=True, vmem_limit_bytes=VMEM_BYTES),
        name='forward',
    )(a_loc, e_rows, init_loc, code, sid, info)


def _bwd_kernel(n, steps, rows, nbuf, at_hbm, e_hbm, cc_ref, code_ref, w_hbm,
                w, wv, ebuf, pp, rp, rs, rin,
                e_sem, w_sem, r_sem, out_sem, dd_ss, dd_rs, ici_ss, ici_rs):
    me, chip, core, partner, right, left = _place(n)
    chips = n // 2
    wide = wv.shape[1]
    size = at_hbm.shape[2]
    per = wide // size // 2
    trips = steps - 2
    rounds_n = 4 * per
    count = 2 * rounds_n
    ringed = 6 * per
    total = trips * rounds_n

    def piece(j, cls, i):
        p, e = lax.div(j, per), lax.rem(j, per)
        hh = jnp.where(p == 1, 1 - i, i)
        off = jnp.where(p == 0, 2, jnp.where(p == 3, 0, chips - 1 if i else 1))
        c = lax.rem(chip + off, chips)
        hop = (p == 1) | (p == 2)
        k = jnp.where(hop, core if cls else 1 - core, 1 - core if cls else core)
        return (c * 2 + k) * 2 * per + hh * per + e

    def fetch(j, cls, i, slot, sem):
        return pltpu.make_async_copy(at_hbm.at[piece(j, cls, i)], w.at[slot, :, pl.ds(i * size, size)], sem)

    def stream(j, i, slot):
        return fetch(j, 1, i, rounds_n + slot, w_sem.at[slot, i])

    def resident(j, i):
        return fetch(j, 0, i, j, r_sem.at[j, i])

    def e_copy(t):
        first = pl.multiple_of((steps - 2 - t) * rows, 8)
        return pltpu.make_async_copy(e_hbm.at[pl.ds(first, rows), :], ebuf.at[lax.rem(t, 2)], e_sem.at[lax.rem(t, 2)])

    def w_copy(t):
        return pltpu.make_async_copy(wv.at[pl.ds(0, rows), :], w_hbm.at[steps - 2 - t], out_sem)

    for t in BOTH:
        e_copy(jnp.int32(t)).start()
    _arrive(me, n)

    def load(j, _):
        for i in BOTH:
            resident(j, i).start()
        return 0

    for q in BOTH:
        for i in BOTH:
            stream(jnp.int32(q), i, q).start()
        load(jnp.int32(q), 0)
    if wv.shape[0] > rows:
        wv[rows:, :] = jnp.zeros((wv.shape[0] - rows, wide), jnp.bfloat16)

    def dd(k):
        return _remote(pp.at[k], rp.at[k], dd_ss.at[k], dd_rs.at[k], partner)

    def ring(k, par, i):
        return _remote(rs.at[k], rin.at[par, k], ici_ss.at[k], ici_rs.at[par, k], left if i else right)

    def weigh(s, eb, o, beta):
        code = code_ref[s, 0:rows, :].astype(jnp.float32)
        ok = code > 2.5
        safe = jnp.where(ok, cc_ref[s], 1.0)
        for cols in _spans(size):
            dst = slice(o + cols.start, o + cols.stop)
            b = 1.0 if beta is None else jnp.where(code > 3.5, 1.0, beta[:, cols])
            v = eb[:, dst].astype(jnp.float32) * b / safe
            wv[0:rows, dst] = jnp.where(ok, v, 0.0).astype(jnp.bfloat16)

    e_copy(jnp.int32(0)).wait()
    for cols in _spans(wide, size):
        weigh(steps - 1, ebuf.at[0], cols.start, None)
    ahead = 4
    for q in range(2, nbuf):
        for i in BOTH:
            stream(jnp.int32(q), i, q).start()
    for q in range(2, ahead):
        load(jnp.int32(q), 0)
    w_copy(jnp.int32(0)).start()
    _all_here(n)

    def step(t, _):
        par = lax.rem(t, 2)

        def finish(j):
            p = lax.div(j, per)
            for i in BOTH:
                dd(2 * j + i).wait_recv()

            @pl.when(p == 2)
            def _():
                for i in BOTH:
                    k = 2 * j + i
                    c = k - 4 * per
                    ring(c, par, i).wait_recv()
                    rp[k] += rin[par, c]

            for i in BOTH:
                k = 2 * j + i
                rs[k] += rp[k]

            @pl.when(p < 3)
            def _():
                for i in BOTH:
                    ring(2 * j + i, par, i).start()

        def rounds(j, _):
            q = t * rounds_n + j
            slot = lax.rem(q, nbuf)
            for i in BOTH:
                stream(j, i, slot).wait()
            prod = _dot(wv[...], w[rounds_n + slot])
            for i, cols in enumerate(_spans(2 * size, size)):
                k = 2 * j + i
                pp[k] = prod[0:rows, cols]
                dd(k).start()

            @pl.when(q + nbuf < total)
            def _():
                for i in BOTH:
                    stream(lax.rem(j + nbuf, rounds_n), i, slot).start()

            @pl.when(j > 0)
            def _():
                finish(j - 1)

            @pl.when(t == 0)
            def _():
                for i in BOTH:
                    resident(j, i).wait()

                @pl.when(j < rounds_n - ahead)
                def _():
                    load(j + ahead, 0)

            prod = _dot(wv[...], w[j])
            for i, cols in enumerate(_spans(2 * size, size)):
                rs[2 * j + i] = prod[0:rows, cols]
            return 0

        lax.fori_loop(0, rounds_n, rounds, 0)
        finish(jnp.int32(rounds_n - 1))

        def gone(k, _):
            dd(k).wait_send()
            return 0

        def sent(k, _):
            ring(k, par, 0).wait_send()
            return 0

        lax.fori_loop(0, count, gone, 0)
        lax.fori_loop(0, 4 * per, sent, 0)
        nxt = t + 1
        e_copy(nxt).wait()

        @pl.when(nxt + 1 < steps - 1)
        def _():
            e_copy(nxt + 1).start()

        w_copy(t).wait()
        eb = ebuf.at[lax.rem(nxt, 2)]
        for e in range(per):
            for i in BOTH:
                near, late = 2 * (per + e) + 1 - i, 2 * (2 * per + e) + i
                ring(near, par, 1 - i).wait_recv()
                ring(late, par, i).wait_recv()
                beta = rs[ringed + 2 * e + i] + rin[par, near] + rin[par, late]
                weigh(steps - 1 - nxt, eb, (i * per + e) * size, beta)
        w_copy(nxt).start()
        lax.fori_loop(4 * per, ringed, sent, 0)
        return 0

    lax.fori_loop(0, trips, step, 0)
    w_copy(jnp.int32(trips)).wait()


def _backward(n, cid, at_loc, e_rows, ccol, code):
    pieces, wide, size = at_loc.shape
    steps, rows, _ = ccol.shape
    full = max(LANES, rows)
    count = pieces // 2
    nbuf = 6 if rows <= 80 else 4
    ringed = 3 * count // 4
    f32, bf16 = jnp.float32, jnp.bfloat16
    dma = pltpu.SemaphoreType.DMA
    return pl.pallas_call(
        functools.partial(_bwd_kernel, n, steps, rows, nbuf),
        out_shape=jax.ShapeDtypeStruct((steps - 1, rows, wide), bf16),
        in_specs=[ANY, ANY, VMEM, VMEM],
        out_specs=ANY,
        scratch_shapes=[
            pltpu.VMEM((count // 2 + nbuf, wide, 2 * size), bf16),
            pltpu.VMEM((full, wide), bf16),
            pltpu.VMEM((2, rows, wide), bf16),
            pltpu.VMEM((count, rows, size), f32),
            pltpu.VMEM((count, rows, size), f32),
            pltpu.VMEM((count, rows, size), f32),
            pltpu.VMEM((2, ringed, rows, size), f32),
            dma((2,)), dma((nbuf, 2)), dma((count // 2, 2)), dma(()),
            dma((count,)), dma((count,)),
            dma((ringed,)), dma((2, ringed)),
        ],
        compiler_params=pltpu.CompilerParams(collective_id=cid, has_side_effects=True, vmem_limit_bytes=VMEM_BYTES),
        name='backward',
    )(at_loc, e_rows, ccol, code)


def _pair_kernel(group_ref, a_ref, x_ref, w_ref, o_ref):
    pair_sum = lax.dot_general(x_ref[...], w_ref[...], (((0,), (0,)), ((), ())), preferred_element_type=jnp.float32)
    o_ref[...] = a_ref[...].astype(jnp.float32) * pair_sum


def _pairs(group, a_loc, xs, ws):
    depth, wide = ws.shape
    size = wide // 8
    tiles = wide // size
    return pl.pallas_call(
        _pair_kernel,
        out_shape=jax.ShapeDtypeStruct((wide, wide), jnp.float32),
        grid_spec=pltpu.PrefetchScalarGridSpec(
            num_scalar_prefetch=1,
            grid=(tiles,),
            in_specs=[
                pl.BlockSpec((size, wide), lambda i, group_ref: (group_ref[0] * tiles + i, 0)),
                pl.BlockSpec((depth, size), lambda i, group_ref: (0, i)),
                pl.BlockSpec((depth, wide), lambda i, group_ref: (0, 0)),
            ],
            out_specs=pl.BlockSpec((size, wide), lambda i, group_ref: (i, 0)),
        ),
        compiler_params=pltpu.CompilerParams(vmem_limit_bytes=VMEM_BYTES),
        name='pairs',
    )(group, a_loc, xs, ws)


def _plan_kernel(options, len_ref, tok_ref, code_ref, sid_ref, look_ref, info_ref, pick_ref):
    seqs = len_ref.shape[1]
    steps = tok_ref.shape[0]
    f32, bf16 = jnp.float32, jnp.bfloat16
    square = (seqs, seqs)
    up = lax.broadcasted_iota(jnp.int32, square, 0).astype(f32)
    across = lax.broadcasted_iota(jnp.int32, square, 1).astype(f32)

    def spread(row):
        return jnp.broadcast_to(row, square)

    def total(x):
        return jnp.sum(x, axis=0, keepdims=True)

    length = len_ref[...].astype(f32)
    l_row = spread(length)
    l_col = l_row.T
    ahead = (l_col > l_row) | ((l_col == l_row) & (up < across))
    rank = total(jnp.where(ahead, 1.0, 0.0))
    rank_col = spread(rank).T

    def mates(slots):
        slot = jnp.where(rank < slots, rank, 2 * slots - 1 - rank)
        return slot, total(jnp.where(rank_col == spread(slot), l_col, 0.0))

    slots = jnp.full((1, 1), seqs, jnp.int32).astype(f32)
    pick = jnp.full((1, 1), len(options) - 1, jnp.int32)
    for k in reversed(range(len(options) - 1)):
        _, first = mates(options[k])
        worst = jnp.max(jnp.where(rank < options[k], 0.0, first + length), axis=1, keepdims=True)
        fits = worst <= steps + 1
        slots = jnp.where(fits, options[k], slots)
        pick = jnp.where(fits, k, pick)
    pick_ref[...] = pick
    slot, first = mates(slots)
    opens = rank < slots
    begin = jnp.where(opens, 0.0, first - 1)
    end = begin + length - 1
    info_ref[0:1, :] = slot
    info_ref[1:2, :] = begin
    info_ref[2:3, :] = end
    order = jax.lax.broadcasted_iota(jnp.int32, length.shape, 1).astype(f32)
    info_ref[3:4, :] = jnp.where(length < 1.5, (steps - 1) * slots + order, (end - 1) * slots + slot)

    double = total(jnp.where((spread(slot).T == spread(slot)) & (up != across), 1.0, 0.0))
    shadowed = opens & (length < 1.5) & (double > 0.5)
    home = (spread(slot) == up).astype(bf16)
    slot_col, begin_col, end_col = spread(slot).T, spread(begin).T, spread(end).T
    hidden_col = spread(jnp.where(shadowed, 1.0, 0.0)).T

    for s in range(steps):
        moves = (begin_col < s) & (end_col >= s)
        kind = jnp.where(moves, jnp.where(end_col == s, 4.0, 3.0), 0.0)
        code_ref[s] = _dot(home, kind.astype(bf16)).astype(bf16)
        number = jnp.where((begin_col == s) & (hidden_col < 0.5), up + 1, 0.0)
        sid_ref[s] = (_dot(home, number.astype(bf16)) - 1).astype(bf16)
    away = (slot_col == across).astype(bf16)
    shape = (steps, seqs)
    pos = lax.broadcasted_iota(jnp.int32, shape, 0).astype(f32) - jnp.broadcast_to(begin, shape)
    tok = jnp.zeros(shape, f32)
    for t in range(1, steps):
        there = (pos == t) & (jnp.broadcast_to(length, shape) > t)
        tok = tok + jnp.where(there, jnp.broadcast_to(tok_ref[t:t + 1, :].astype(f32), shape), 0.0)
    high = jnp.floor(tok / LANES)
    low = tok - high * LANES
    look = _dot(high.astype(bf16), away) * LANES + _dot(low.astype(bf16), away)
    look_ref[...] = look.astype(jnp.int32)


def _plan(options, lengths, tokens):
    steps, seqs = tokens.shape
    bf16 = jnp.bfloat16
    return pl.pallas_call(
        functools.partial(_plan_kernel, options),
        out_shape=(
            jax.ShapeDtypeStruct((steps, seqs, LANES), bf16),
            jax.ShapeDtypeStruct((steps, seqs, LANES), bf16),
            jax.ShapeDtypeStruct((steps, seqs), jnp.int32),
            jax.ShapeDtypeStruct((8, seqs), jnp.float32),
            jax.ShapeDtypeStruct((1, 1), jnp.int32),
        ),
        in_specs=[VMEM, VMEM],
        out_specs=(VMEM, VMEM, VMEM, VMEM, VMEM),
        name='plan',
    )(lengths[None, :], tokens)


def solution(mesh):
    n = mesh.shape['states']

    def local_run(trans_loc, emit_loc, init_loc, tokens_loc, lengths_loc):
        seqs, steps = tokens_loc.shape
        wide = trans_loc.shape[1]
        group = lax.axis_index('states').astype(jnp.int32)[None]
        options = (seqs * 9 // 16, seqs * 5 // 8, seqs)
        code, sid, look, info, pick = _plan(options, lengths_loc, tokens_loc.T)

        def run(k):
            rows = options[k]
            tokens = jnp.concatenate([look[1:, 0:rows].reshape(-1), tokens_loc[:, 0]])
            e_rows = jnp.take(emit_loc, tokens, axis=1, mode='clip').T
            al, xs, at_loc, ccol, ll = _forward(n, 2 * k, rows, trans_loc, e_rows, init_loc[None, :], code, sid, info)
            ws = _backward(n, 2 * k + 1, at_loc, e_rows, ccol, code)
            counts = _pairs(group, trans_loc, xs.reshape(-1, wide), ws.reshape(-1, wide))
            return ll[0], jnp.take(al, info[3].astype(jnp.int32), axis=0, mode='clip'), counts

        return lax.switch(pick[0, 0], [functools.partial(run, k) for k in range(len(options))])

    return jax.shard_map(local_run, mesh=mesh, in_specs=(P(None, 'states'), P('states', None), P('states'), P('seqs', None), P('seqs')), out_specs=(P('seqs'), P('seqs', 'states'), P(('seqs', 'states'), None)), check_vma=False)
```

```python
import functools

import jax
import jax.numpy as jnp
from jax import lax
from jax.experimental import pallas as pl
from jax.experimental.pallas import tpu as pltpu
from jax.sharding import PartitionSpec as P

MESH = pl.DeviceIdType.MESH
ANY = pl.BlockSpec(memory_space=pl.ANY)
VMEM = pl.BlockSpec(memory_space=pltpu.VMEM)
LANES = 128
BOTH = (0, 1)
VMEM_BYTES = 67043328


def _place(n):
    me = lax.axis_index('states')
    core = lax.rem(me, 2)
    chip = lax.div(me, 2)
    partner = chip * 2 + (1 - core)
    right = lax.rem(partner + 2, n)
    left = lax.rem(partner + n - 2, n)
    return me, chip, core, partner, right, left


def _dev(peer):
    return {'states': peer}


def _arrive(me, n):
    for r in range(1, n):
        pl.semaphore_signal(pltpu.get_barrier_semaphore(), inc=1, device_id=_dev(lax.rem(me + r, n)), device_id_type=MESH)


def _all_here(n):
    pl.semaphore_wait(pltpu.get_barrier_semaphore(), n - 1)


def _remote(src, dst, ssem, rsem, peer):
    return pltpu.make_async_remote_copy(src_ref=src, dst_ref=dst, send_sem=ssem, recv_sem=rsem, device_id=_dev(peer), device_id_type=MESH)


def _spans(width, size=LANES):
    return [slice(o, o + size) for o in range(0, width, size)]


def _dot(x, y):
    return jnp.dot(x, y, preferred_element_type=jnp.float32)


def _fwd_kernel(n, steps, rows, nbuf, a_hbm, e_hbm, pi_ref, code_ref, sid_ref, info_ref, al_hbm, x_hbm, at_hbm, cc_ref, ll_ref,
                g, w, u, al, ebuf, a0b, xi, fs, fr, ta, tt, safe_ref, lacc, tbuf, cs_send, cs_recv,
                e_sem, w_sem, r_sem, out_sem, ta_sem, tt_sem, cs_ss, cs_rs, ici_ss, ici_rs, dd_ss, dd_rs):
    me, chip, core, partner, right, left = _place(n)
    chips = n // 2
    wide = al.shape[1]
    part_w = wide // 4
    seqs = a0b.shape[0]
    a0f = u.at[pl.ds(0, seqs), :]
    quarters = range(4)
    per_step = 2 * 8
    total = (steps - 1) * per_step

    def quarter(j, cls, i):
        far = lax.rem(j + 2 + 2 * i, 4)
        qq = jnp.where(j < 2, 2 * j + i, far)
        off = jnp.where(j < 2, 0, jnp.where(j >= 6, 2, jnp.where(i == 0, chips - 1, 1)))
        c = lax.rem(chip + off, chips)
        k = jnp.where((j >= 2) & (j < 6), cls == 0, cls != 0)
        return (c * 2 + jnp.where(k, 1 - core, core)) * 4 + qq

    def a_part(b):
        return a_hbm.at[pl.ds(pl.multiple_of(b * part_w, part_w), part_w), :]

    def stream(q, slot):
        k = lax.rem(q, per_step)
        return pltpu.make_async_copy(a_part(quarter(lax.div(k, 2), 1, lax.rem(k, 2))), w.at[per_step + slot], w_sem.at[slot])

    def resident(j, i):
        return pltpu.make_async_copy(a_part(quarter(j, 0, i)), w.at[2 * j + i], r_sem.at[2 * j + i])

    def e_rows(first, count, dst, sem):
        return pltpu.make_async_copy(e_hbm.at[pl.ds(pl.multiple_of(first, 8), count), :], dst, sem)

    def e_copy(s):
        return e_rows((s - 1) * rows, rows, ebuf.at[lax.rem(s, 2)], e_sem.at[lax.rem(s, 2)])

    def al_copy(s):
        return pltpu.make_async_copy(al, al_hbm.at[pl.ds(pl.multiple_of((s - 1) * rows, 8), rows), :], out_sem.at[4])

    def mine(b):
        return g.at[b, pl.ds(0, rows), :]

    def x_copy(s, q):
        return pltpu.make_async_copy(mine(me * 4 + q), x_hbm.at[s, :, pl.ds(q * part_w, part_w)], out_sem.at[q])

    pieces, size = at_hbm.shape[0], ta.shape[1]
    fed, depth = ta.shape[0], tt.shape[0]

    def ta_copy(c):
        slot = lax.rem(c, fed)
        return pltpu.make_async_copy(a_hbm.at[pl.ds(pl.multiple_of(c * size, size), size), :], ta.at[slot], ta_sem.at[slot])

    def tt_copy(c):
        slot = lax.rem(c, depth)
        return pltpu.make_async_copy(tt.at[slot], at_hbm.at[c], tt_sem.at[slot])

    def turn(s):
        def one(c, _):
            ta_copy(c).wait()

            @pl.when(c >= depth)
            def _():
                tt_copy(c - depth).wait()

            slot = lax.rem(c, depth)
            tt[slot] = ta[lax.rem(c, fed)].T
            tt_copy(c).start()

            @pl.when(c + fed < pieces)
            def _():
                ta_copy(c + fed).start()

            return 0

        @pl.when(s == 1)
        def _():
            for c in range(fed):
                ta_copy(jnp.int32(c)).start()

        lax.fori_loop(lax.div(jnp.maximum(s - 2, 0) * pieces, steps - 2), lax.div((s - 1) * pieces, steps - 2), one, 0)

    e0_copy = e_rows((steps - 1) * rows, seqs, a0b, e_sem.at[0])
    e0_copy.start()
    _arrive(me, n)

    def load(j, _):
        for i in BOTH:
            resident(j, i).start()
        return 0

    for q in range(nbuf):
        stream(jnp.int32(q), q).start()
    lax.fori_loop(0, 2, load, 0)
    e_copy(jnp.int32(1)).start()
    tbuf[...] = jnp.zeros_like(tbuf)
    lacc[...] = jnp.zeros_like(lacc)
    if g.shape[1] > rows:
        pad = jnp.zeros((g.shape[1] - rows, part_w), jnp.bfloat16)

        def clear(k, _):
            g[k, rows:, :] = pad
            return 0

        lax.fori_loop(0, 4 * n, clear, 0)

    def ici(k, src, dst, i):
        return _remote(src, dst, ici_ss.at[k], ici_rs.at[k], left if i else right)

    def early(i):
        return ici(i, fs.at[i], fr.at[i], i)

    def own_ring(j, i):
        b = me * 4 + (j + 2 + 2 * i) % 4
        return ici(2 * (j - 2) + i, mine(b), mine(b), i)

    def relay(j, i):
        b = quarter(j, 0, i)
        return ici(2 * (j + 2) + i, mine(b), mine(b), i)

    def dd(j, cls, i):
        b = quarter(j, cls, i)
        return _remote(mine(b), mine(b), dd_ss.at[2 * j + i], dd_rs.at[2 * j + i], partner)

    lane = lax.broadcasted_iota(jnp.int32, (rows, seqs), 1).astype(jnp.float32)
    row = lax.broadcasted_iota(jnp.int32, (rows, seqs), 0).astype(jnp.float32)

    def starting(s):
        return sid_ref[s, 0:rows, :].astype(jnp.float32)

    def first_alphas(s):
        pick = (starting(s) == lane).astype(jnp.bfloat16)
        xi[...] = _dot(pick, a0b[...]).astype(jnp.bfloat16)

    def normalizer(part, count, meanwhile):
        tbuf[0:count, :] = part
        row = jnp.sum(tbuf[...].T, axis=0, keepdims=True)
        cs_send[...] = jnp.broadcast_to(row, cs_send.shape)
        cs_recv[me] = jnp.broadcast_to(row, cs_send.shape)
        cps = []
        for r in sorted(range(1, n), key=lambda r: abs(2 * r - n)):
            cp = _remote(cs_send, cs_recv.at[me], cs_ss.at[r - 1], cs_rs.at[r - 1], lax.rem(me + r, n))
            cp.start()
            cps.append(cp)
        meanwhile()
        for cp in cps:
            cp.wait()
        crow = cs_recv[0]
        for r in range(1, n):
            crow = crow + cs_recv[r]
        return crow, jnp.broadcast_to(crow[0:1, :], (LANES, LANES)).T[0:count, :]

    def add_log(s, ccol):
        slot, begin, end = info_ref[0:1, :], info_ref[1:2, :], info_ref[2:3, :]
        now = jnp.full((rows, seqs), s, jnp.int32).astype(jnp.float32)
        here = (slot == row) & (now > begin) & (now <= end)
        lacc[...] += jnp.where(here, jnp.log(jnp.where(here, ccol, 1.0)), 0.0)

    def exchange(s, then):
        own = [dd(j, 0, i) for j in BOTH for i in BOTH]
        own += [own_ring(j, i) for j in (4, 5) for i in BOTH]
        for cp in own:
            cp.start()
        then()

        def arrived(j):
            for i in BOTH:
                b = quarter(j, 0, i)
                ici(2 * (j - 2) + i, mine(b), mine(b), i).wait_recv()

        def pass_on(j):
            for i in BOTH:
                dd(j, 0, i).start()

        def rounds(h, _):
            j, k = 2 * h, 2 * h + 1

            @pl.when(h == 1)
            def _():
                for i in BOTH:
                    early(i).wait_recv()
                safe = safe_ref[...]
                for i in BOTH:
                    b = quarter(2, 0, i)
                    for cols in _spans(part_w):
                        g[b, 0:rows, cols] = (fr[i, :, cols] / safe).astype(jnp.bfloat16)
                    relay(2, i).start()
                pass_on(2)
                first_alphas(s + 1)

            @pl.when(s == 0)
            def _():
                for r in (j, k):
                    for i in BOTH:
                        resident(r, i).wait()

                    @pl.when(h < 2)
                    def _():
                        load(r + 4, 0)

            @pl.when(h >= 2)
            def _():
                arrived(j)
                pass_on(j)

            def own_class(r):
                return sum(_dot(g[quarter(r, 0, i)], w[2 * r + i]) for i in BOTH)

            def other_class(r):
                q = s * per_step + 2 * r
                slots = [lax.rem(q + i, nbuf) for i in BOTH]
                for i in BOTH:
                    dd(r, 1, i).wait_recv()
                    stream(q + i, slots[i]).wait()
                out = sum(_dot(g[quarter(r, 1, i)], w[per_step + slots[i]]) for i in BOTH)

                for i in BOTH:
                    @pl.when(q + i + nbuf < total)
                    def _():
                        stream(q + i + nbuf, slots[i]).start()

                return out

            prod = own_class(j)

            @pl.when(h >= 1)
            def _():
                arrived(k)

            @pl.when(h == 1)
            def _():
                for i in BOTH:
                    relay(3, i).start()

            @pl.when(h >= 1)
            def _():
                pass_on(k)

            u[...] += prod + own_class(k)
            u[...] += other_class(j)
            u[...] += other_class(k)
            return 0

        lax.fori_loop(0, 4, rounds, 0)
        for i in BOTH:
            early(i).wait_send()
            for j in (2, 3):
                relay(j, i).wait_send()
            for j in range(2, 8):
                dd(j, 0, i).wait_send()
        for cp in own + [own_ring(3, i) for i in BOTH]:
            cp.wait_send()

    def keep(s):
        for q in quarters:
            x_copy(s, q).start()

    e0_copy.wait()
    def lanes(q):
        return pl.ds(pl.multiple_of(q * LANES, LANES), LANES)

    def first_mass(q, part):
        a = jnp.broadcast_to(pi_ref[:, lanes(q)], (seqs, LANES)) * a0b[:, lanes(q)].astype(jnp.float32)
        a0f[:, lanes(q)] = a
        return part + a

    part = lax.fori_loop(0, wide // LANES, first_mass, jnp.zeros((seqs, LANES), jnp.float32))
    _all_here(n)

    c0_row, c0 = normalizer(part, seqs, lambda: lax.fori_loop(2, 4, load, 0))
    ll_ref[...] = jnp.log(c0_row)

    def first_alpha(q, _):
        alpha = a0f[:, lanes(q)] / c0
        a0f[:, lanes(q)] = alpha
        a0b[:, lanes(q)] = alpha.astype(jnp.bfloat16)
        return 0

    lax.fori_loop(0, wide // LANES, first_alpha, 0)
    a0_copy = pltpu.make_async_copy(a0f, al_hbm.at[pl.ds((steps - 1) * rows, seqs), :], e_sem.at[0])
    a0_copy.start()
    first_alphas(0)
    for q, cols in enumerate(_spans(wide, part_w)):
        g[me * 4 + q, 0:rows, :] = xi[:, cols]
    for i in BOTH:
        own_ring(3, i).start()
    safe_ref[...] = jnp.ones_like(safe_ref)
    for i in BOTH:
        fs[i] = xi[:, 2 * i * part_w:(2 * i + 1) * part_w].astype(jnp.float32)
        early(i).start()
    tbuf[...] = jnp.zeros_like(tbuf)
    a0_copy.wait()
    u[...] = jnp.zeros_like(u)

    def step(s, _):
        exchange(s - 1, lambda: keep(s - 1))
        e_copy(s).wait()

        @pl.when(s + 1 < steps)
        def _():
            e_copy(s + 1).start()

        @pl.when(s > 1)
        def _():
            al_copy(s - 1).wait()

        part = jnp.zeros((rows, LANES), jnp.float32)
        eb = ebuf.at[lax.rem(s, 2)]
        for cols in _spans(wide):
            a = u[0:rows, cols] * eb[:, cols].astype(jnp.float32)
            al[:, cols] = a
            part = part + a
        live = code_ref[s, 0:rows, :].astype(jnp.float32) > 0.5
        starts = starting(s) > -0.5

        def meanwhile():
            @pl.when(s + 1 < steps)
            def _():
                for i in BOTH:
                    for cols in _spans(part_w):
                        from_col = 2 * i * part_w + cols.start
                        src = slice(from_col, from_col + LANES)
                        v = jnp.where(live, al[:, src], 0.0)
                        fs[i, :, cols] = jnp.where(starts, xi[:, src].astype(jnp.float32), v)
                    early(i).start()

            turn(s)
            u[...] = jnp.zeros_like(u)

            @pl.when(s > 1)
            def _():
                add_log(s - 1, cc_ref[s - 1])

            for q in quarters:
                x_copy(s - 1, q).wait()

        _, ccol = normalizer(part, rows, meanwhile)
        cc_ref[s] = ccol
        safe = jnp.where(live, ccol, 1.0)
        safe_ref[...] = jnp.where(starts, 1.0, safe)
        blocks = _spans(wide, part_w)
        for q in (1, 3, 0, 2):
            for cols in _spans(part_w):
                src = slice(blocks[q].start + cols.start, blocks[q].start + cols.stop)
                alpha = jnp.where(live, al[:, src] / safe, 0.0)
                al[:, src] = alpha
                x = jnp.where(starts, xi[:, src].astype(jnp.float32), alpha)
                g[me * 4 + q, 0:rows, cols] = x.astype(jnp.bfloat16)

            if q % 2:
                @pl.when(s + 1 < steps)
                def _():
                    own_ring(3, q // 2).start()

        al_copy(s).start()
        return 0

    lax.fori_loop(1, steps, step, 0)
    add_log(steps - 1, cc_ref[steps - 1])
    ll_ref[...] += jnp.sum(lacc[...], axis=0, keepdims=True)
    al_copy(steps - 1).wait()
    for c in range(depth):
        tt_copy(pieces - depth + c).wait()


def _forward(n, cid, rows, a_loc, e_rows, init_loc, code, sid, info):
    wide = a_loc.shape[1]
    steps, seqs, _ = code.shape
    part_w = wide // 4
    full = max(LANES, rows)
    nbuf = 6 if rows <= 80 else 4
    f32, bf16 = jnp.float32, jnp.bfloat16
    dma = pltpu.SemaphoreType.DMA
    return pl.pallas_call(
        functools.partial(_fwd_kernel, n, steps, rows, nbuf),
        out_shape=(
            jax.ShapeDtypeStruct(((steps - 1) * rows + seqs, wide), f32),
            jax.ShapeDtypeStruct((steps - 1, rows, wide), bf16),
            jax.ShapeDtypeStruct((2 * a_loc.shape[0] // part_w, wide, part_w // 2), bf16),
            jax.ShapeDtypeStruct((steps, rows, LANES), f32),
            jax.ShapeDtypeStruct((8, LANES), f32),
        ),
        in_specs=[ANY, ANY, VMEM, VMEM, VMEM, VMEM],
        out_specs=(ANY, ANY, ANY, VMEM, VMEM),
        scratch_shapes=[
            pltpu.VMEM((4 * n, full, part_w), bf16),
            pltpu.VMEM((2 * n + nbuf, part_w, wide), bf16),
            pltpu.VMEM((full, wide), f32),
            pltpu.VMEM((rows, wide), f32),
            pltpu.VMEM((2, rows, wide), bf16),
            pltpu.VMEM((seqs, wide), bf16),
            pltpu.VMEM((rows, wide), bf16),
            pltpu.VMEM((2, rows, part_w), f32),
            pltpu.VMEM((2, rows, part_w), f32),
            pltpu.VMEM((5, part_w // 2, wide), bf16),
            pltpu.VMEM((4, wide, part_w // 2), bf16),
            pltpu.VMEM((rows, LANES), f32),
            pltpu.VMEM((rows, LANES), f32),
            pltpu.VMEM((LANES, LANES), f32),
            pltpu.VMEM((8, LANES), f32),
            pltpu.VMEM((n, 8, LANES), f32),
            dma((2,)), dma((nbuf,)), dma((2 * n,)), dma((5,)), dma((5,)), dma((4,)),
            dma((n - 1,)), dma((n - 1,)),
            dma((12,)), dma((12,)), dma((2 * n,)), dma((2 * n,)),
        ],
        compiler_params=pltpu.CompilerParams(collective_id=cid, has_side_effects=True, vmem_limit_bytes=VMEM_BYTES),
        name='forward',
    )(a_loc, e_rows, init_loc, code, sid, info)


def _bwd_kernel(n, steps, rows, nbuf, at_hbm, e_hbm, cc_ref, code_ref, w_hbm,
                w, wv, ebuf, pp, rp, rs, rin,
                e_sem, w_sem, r_sem, out_sem, dd_ss, dd_rs, ici_ss, ici_rs):
    me, chip, core, partner, right, left = _place(n)
    chips = n // 2
    wide = wv.shape[1]
    size = at_hbm.shape[2]
    per = wide // size // 2
    trips = steps - 2
    rounds_n = 4 * per
    count = 2 * rounds_n
    ringed = 6 * per
    total = trips * rounds_n

    def piece(j, cls, i):
        p, e = lax.div(j, per), lax.rem(j, per)
        hh = jnp.where(p == 1, 1 - i, i)
        off = jnp.where(p == 0, 2, jnp.where(p == 3, 0, chips - 1 if i else 1))
        c = lax.rem(chip + off, chips)
        hop = (p == 1) | (p == 2)
        k = jnp.where(hop, core if cls else 1 - core, 1 - core if cls else core)
        return (c * 2 + k) * 2 * per + hh * per + e

    def fetch(j, cls, i, slot, sem):
        return pltpu.make_async_copy(at_hbm.at[piece(j, cls, i)], w.at[slot, :, pl.ds(i * size, size)], sem)

    def stream(j, i, slot):
        return fetch(j, 1, i, rounds_n + slot, w_sem.at[slot, i])

    def resident(j, i):
        return fetch(j, 0, i, j, r_sem.at[j, i])

    def e_copy(t):
        first = pl.multiple_of((steps - 2 - t) * rows, 8)
        return pltpu.make_async_copy(e_hbm.at[pl.ds(first, rows), :], ebuf.at[lax.rem(t, 2)], e_sem.at[lax.rem(t, 2)])

    def w_copy(t):
        return pltpu.make_async_copy(wv.at[pl.ds(0, rows), :], w_hbm.at[steps - 2 - t], out_sem)

    for t in BOTH:
        e_copy(jnp.int32(t)).start()
    _arrive(me, n)

    def load(j, _):
        for i in BOTH:
            resident(j, i).start()
        return 0

    for q in BOTH:
        for i in BOTH:
            stream(jnp.int32(q), i, q).start()
        load(jnp.int32(q), 0)
    if wv.shape[0] > rows:
        wv[rows:, :] = jnp.zeros((wv.shape[0] - rows, wide), jnp.bfloat16)

    def dd(k):
        return _remote(pp.at[k], rp.at[k], dd_ss.at[k], dd_rs.at[k], partner)

    def ring(k, par, i):
        return _remote(rs.at[k], rin.at[par, k], ici_ss.at[k], ici_rs.at[par, k], left if i else right)

    def weigh(s, eb, o, beta):
        code = code_ref[s, 0:rows, :].astype(jnp.float32)
        ok = code > 2.5
        safe = jnp.where(ok, cc_ref[s], 1.0)
        for cols in _spans(size):
            dst = slice(o + cols.start, o + cols.stop)
            b = 1.0 if beta is None else jnp.where(code > 3.5, 1.0, beta[:, cols])
            v = eb[:, dst].astype(jnp.float32) * b / safe
            wv[0:rows, dst] = jnp.where(ok, v, 0.0).astype(jnp.bfloat16)

    e_copy(jnp.int32(0)).wait()
    for cols in _spans(wide, size):
        weigh(steps - 1, ebuf.at[0], cols.start, None)
    ahead = 4
    for q in range(2, nbuf):
        for i in BOTH:
            stream(jnp.int32(q), i, q).start()
    for q in range(2, ahead):
        load(jnp.int32(q), 0)
    w_copy(jnp.int32(0)).start()
    _all_here(n)

    def step(t, _):
        par = lax.rem(t, 2)

        def finish(j):
            p = lax.div(j, per)
            for i in BOTH:
                dd(2 * j + i).wait_recv()

            @pl.when(p == 2)
            def _():
                for i in BOTH:
                    k = 2 * j + i
                    c = k - 4 * per
                    ring(c, par, i).wait_recv()
                    rp[k] += rin[par, c]

            for i in BOTH:
                k = 2 * j + i
                rs[k] += rp[k]

            @pl.when(p < 3)
            def _():
                for i in BOTH:
                    ring(2 * j + i, par, i).start()

        def rounds(j, _):
            q = t * rounds_n + j
            slot = lax.rem(q, nbuf)
            for i in BOTH:
                stream(j, i, slot).wait()
            prod = _dot(wv[...], w[rounds_n + slot])
            for i, cols in enumerate(_spans(2 * size, size)):
                k = 2 * j + i
                pp[k] = prod[0:rows, cols]
                dd(k).start()

            @pl.when(q + nbuf < total)
            def _():
                for i in BOTH:
                    stream(lax.rem(j + nbuf, rounds_n), i, slot).start()

            @pl.when(j > 0)
            def _():
                finish(j - 1)

            @pl.when(t == 0)
            def _():
                for i in BOTH:
                    resident(j, i).wait()

                @pl.when(j < rounds_n - ahead)
                def _():
                    load(j + ahead, 0)

            prod = _dot(wv[...], w[j])
            for i, cols in enumerate(_spans(2 * size, size)):
                rs[2 * j + i] = prod[0:rows, cols]
            return 0

        lax.fori_loop(0, rounds_n, rounds, 0)
        finish(jnp.int32(rounds_n - 1))

        def gone(k, _):
            dd(k).wait_send()
            return 0

        def sent(k, _):
            ring(k, par, 0).wait_send()
            return 0

        lax.fori_loop(0, count, gone, 0)
        lax.fori_loop(0, 4 * per, sent, 0)
        nxt = t + 1
        e_copy(nxt).wait()

        @pl.when(nxt + 1 < steps - 1)
        def _():
            e_copy(nxt + 1).start()

        w_copy(t).wait()
        eb = ebuf.at[lax.rem(nxt, 2)]
        for e in range(per):
            for i in BOTH:
                near, late = 2 * (per + e) + 1 - i, 2 * (2 * per + e) + i
                ring(near, par, 1 - i).wait_recv()
                ring(late, par, i).wait_recv()
                beta = rs[ringed + 2 * e + i] + rin[par, near] + rin[par, late]
                weigh(steps - 1 - nxt, eb, (i * per + e) * size, beta)
        w_copy(nxt).start()
        lax.fori_loop(4 * per, ringed, sent, 0)
        return 0

    lax.fori_loop(0, trips, step, 0)
    w_copy(jnp.int32(trips)).wait()


def _backward(n, cid, at_loc, e_rows, ccol, code):
    pieces, wide, size = at_loc.shape
    steps, rows, _ = ccol.shape
    full = max(LANES, rows)
    count = pieces // 2
    nbuf = 6 if rows <= 80 else 4
    ringed = 3 * count // 4
    f32, bf16 = jnp.float32, jnp.bfloat16
    dma = pltpu.SemaphoreType.DMA
    return pl.pallas_call(
        functools.partial(_bwd_kernel, n, steps, rows, nbuf),
        out_shape=jax.ShapeDtypeStruct((steps - 1, rows, wide), bf16),
        in_specs=[ANY, ANY, VMEM, VMEM],
        out_specs=ANY,
        scratch_shapes=[
            pltpu.VMEM((count // 2 + nbuf, wide, 2 * size), bf16),
            pltpu.VMEM((full, wide), bf16),
            pltpu.VMEM((2, rows, wide), bf16),
            pltpu.VMEM((count, rows, size), f32),
            pltpu.VMEM((count, rows, size), f32),
            pltpu.VMEM((count, rows, size), f32),
            pltpu.VMEM((2, ringed, rows, size), f32),
            dma((2,)), dma((nbuf, 2)), dma((count // 2, 2)), dma(()),
            dma((count,)), dma((count,)),
            dma((ringed,)), dma((2, ringed)),
        ],
        compiler_params=pltpu.CompilerParams(collective_id=cid, has_side_effects=True, vmem_limit_bytes=VMEM_BYTES),
        name='backward',
    )(at_loc, e_rows, ccol, code)


def _pair_kernel(group_ref, a_ref, x_ref, w_ref, o_ref):
    pair_sum = lax.dot_general(x_ref[...], w_ref[...], (((0,), (0,)), ((), ())), preferred_element_type=jnp.float32)
    o_ref[...] = a_ref[...].astype(jnp.float32) * pair_sum


def _pairs(group, a_loc, xs, ws):
    depth, wide = ws.shape
    size = wide // 8
    tiles = wide // size
    return pl.pallas_call(
        _pair_kernel,
        out_shape=jax.ShapeDtypeStruct((wide, wide), jnp.float32),
        grid_spec=pltpu.PrefetchScalarGridSpec(
            num_scalar_prefetch=1,
            grid=(tiles,),
            in_specs=[
                pl.BlockSpec((size, wide), lambda i, group_ref: (group_ref[0] * tiles + i, 0)),
                pl.BlockSpec((depth, size), lambda i, group_ref: (0, i)),
                pl.BlockSpec((depth, wide), lambda i, group_ref: (0, 0)),
            ],
            out_specs=pl.BlockSpec((size, wide), lambda i, group_ref: (i, 0)),
        ),
        compiler_params=pltpu.CompilerParams(vmem_limit_bytes=VMEM_BYTES),
        name='pairs',
    )(group, a_loc, xs, ws)


def _plan_kernel(options, len_ref, tok_ref, code_ref, sid_ref, look_ref, info_ref, pick_ref):
    seqs = len_ref.shape[1]
    steps = tok_ref.shape[0]
    f32, bf16 = jnp.float32, jnp.bfloat16
    square = (seqs, seqs)
    up = lax.broadcasted_iota(jnp.int32, square, 0).astype(f32)
    across = lax.broadcasted_iota(jnp.int32, square, 1).astype(f32)

    def spread(row):
        return jnp.broadcast_to(row, square)

    def total(x):
        return jnp.sum(x, axis=0, keepdims=True)

    length = len_ref[...].astype(f32)
    l_row = spread(length)
    l_col = l_row.T
    ahead = (l_col > l_row) | ((l_col == l_row) & (up < across))
    rank = total(jnp.where(ahead, 1.0, 0.0))
    rank_col = spread(rank).T

    def mates(slots):
        slot = jnp.where(rank < slots, rank, 2 * slots - 1 - rank)
        return slot, total(jnp.where(rank_col == spread(slot), l_col, 0.0))

    slots = jnp.full((1, 1), seqs, jnp.int32).astype(f32)
    pick = jnp.full((1, 1), len(options) - 1, jnp.int32)
    for k in reversed(range(len(options) - 1)):
        _, first = mates(options[k])
        worst = jnp.max(jnp.where(rank < options[k], 0.0, first + length), axis=1, keepdims=True)
        fits = worst <= steps + 1
        slots = jnp.where(fits, options[k], slots)
        pick = jnp.where(fits, k, pick)
    pick_ref[...] = pick
    slot, first = mates(slots)
    opens = rank < slots
    begin = jnp.where(opens, 0.0, first - 1)
    end = begin + length - 1
    info_ref[0:1, :] = slot
    info_ref[1:2, :] = begin
    info_ref[2:3, :] = end

    double = total(jnp.where((spread(slot).T == spread(slot)) & (up != across), 1.0, 0.0))
    shadowed = opens & (length < 1.5) & (double > 0.5)
    home = (spread(slot) == up).astype(bf16)
    slot_col, begin_col, end_col = spread(slot).T, spread(begin).T, spread(end).T
    hidden_col = spread(jnp.where(shadowed, 1.0, 0.0)).T

    for s in range(steps):
        moves = (begin_col < s) & (end_col >= s)
        kind = jnp.where(moves, jnp.where(end_col == s, 4.0, 3.0), 0.0)
        code_ref[s] = _dot(home, kind.astype(bf16)).astype(bf16)
        number = jnp.where((begin_col == s) & (hidden_col < 0.5), up + 1, 0.0)
        sid_ref[s] = (_dot(home, number.astype(bf16)) - 1).astype(bf16)
    away = (slot_col == across).astype(bf16)
    shape = (steps, seqs)
    pos = lax.broadcasted_iota(jnp.int32, shape, 0).astype(f32) - jnp.broadcast_to(begin, shape)
    tok = jnp.zeros(shape, f32)
    for t in range(1, steps):
        there = (pos == t) & (jnp.broadcast_to(length, shape) > t)
        tok = tok + jnp.where(there, jnp.broadcast_to(tok_ref[t:t + 1, :].astype(f32), shape), 0.0)
    high = jnp.floor(tok / LANES)
    low = tok - high * LANES
    look = _dot(high.astype(bf16), away) * LANES + _dot(low.astype(bf16), away)
    look_ref[...] = look.astype(jnp.int32)


def _plan(options, lengths, tokens):
    steps, seqs = tokens.shape
    bf16 = jnp.bfloat16
    return pl.pallas_call(
        functools.partial(_plan_kernel, options),
        out_shape=(
            jax.ShapeDtypeStruct((steps, seqs, LANES), bf16),
            jax.ShapeDtypeStruct((steps, seqs, LANES), bf16),
            jax.ShapeDtypeStruct((steps, seqs), jnp.int32),
            jax.ShapeDtypeStruct((8, seqs), jnp.float32),
            jax.ShapeDtypeStruct((1, 1), jnp.int32),
        ),
        in_specs=[VMEM, VMEM],
        out_specs=(VMEM, VMEM, VMEM, VMEM, VMEM),
        name='plan',
    )(lengths[None, :], tokens)


def solution(mesh):
    n = mesh.shape['states']

    def local_run(trans_loc, emit_loc, init_loc, tokens_loc, lengths_loc):
        seqs, steps = tokens_loc.shape
        wide = trans_loc.shape[1]
        group = lax.axis_index('states').astype(jnp.int32)[None]
        options = (seqs * 9 // 16, seqs * 5 // 8, seqs)
        code, sid, look, info, pick = _plan(options, lengths_loc, tokens_loc.T)
        branch = lax.pmax(pick[0, 0], 'seqs')

        def run(k):
            rows = options[k]
            tokens = jnp.concatenate([look[1:, 0:rows].reshape(-1), tokens_loc[:, 0]])
            e_rows = jnp.take(emit_loc, tokens, axis=1, mode='clip').T
            al, xs, at_loc, ccol, ll = _forward(n, 2 * k, rows, trans_loc, e_rows, init_loc[None, :], code, sid, info)
            ws = _backward(n, 2 * k + 1, at_loc, e_rows, ccol, code)
            counts = _pairs(group, trans_loc, xs.reshape(-1, wide), ws.reshape(-1, wide))
            slot, end = info[0].astype(jnp.int32), info[2].astype(jnp.int32)
            alone = (steps - 1) * rows + jnp.arange(seqs, dtype=jnp.int32)
            where = jnp.where(lengths_loc == 1, alone, (end - 1) * rows + slot)
            return ll[0], jnp.take(al, where, axis=0, mode='clip'), counts

        return lax.switch(branch, [functools.partial(run, k) for k in range(len(options))])

    return jax.shard_map(local_run, mesh=mesh, in_specs=(P(None, 'states'), P('states', None), P('states'), P('seqs', None), P('seqs')), out_specs=(P('seqs'), P('seqs', 'states'), P(('seqs', 'states'), None)), check_vma=False)
```

```python
import functools

import jax
import jax.numpy as jnp
from jax import lax
from jax.experimental import pallas as pl
from jax.experimental.pallas import tpu as pltpu
from jax.sharding import PartitionSpec as P

MESH = pl.DeviceIdType.MESH
ANY = pl.BlockSpec(memory_space=pl.ANY)
VMEM = pl.BlockSpec(memory_space=pltpu.VMEM)
LANES = 128
BOTH = (0, 1)
VMEM_BYTES = 67043328


def _place(n):
    me = lax.axis_index('states')
    core = lax.rem(me, 2)
    chip = lax.div(me, 2)
    partner = chip * 2 + (1 - core)
    right = lax.rem(partner + 2, n)
    left = lax.rem(partner + n - 2, n)
    return me, chip, core, partner, right, left


def _dev(peer):
    return {'states': peer}


def _arrive(me, n):
    for r in range(1, n):
        pl.semaphore_signal(pltpu.get_barrier_semaphore(), inc=1, device_id=_dev(lax.rem(me + r, n)), device_id_type=MESH)


def _all_here(n):
    pl.semaphore_wait(pltpu.get_barrier_semaphore(), n - 1)


def _remote(src, dst, ssem, rsem, peer):
    return pltpu.make_async_remote_copy(src_ref=src, dst_ref=dst, send_sem=ssem, recv_sem=rsem, device_id=_dev(peer), device_id_type=MESH)


def _spans(width, size=LANES):
    return [slice(o, o + size) for o in range(0, width, size)]


def _dot(x, y):
    return jnp.dot(x, y, preferred_element_type=jnp.float32)


def _fwd_kernel(n, steps, rows, nbuf, a_hbm, e_hbm, pi_ref, code_ref, sid_ref, info_ref, al_hbm, x_hbm, at_hbm, cc_ref, ll_ref,
                g, w, u, al, ebuf, a0b, xi, fs, fr, ta, tt, safe_ref, lacc, tbuf, cs_send, cs_recv,
                e_sem, w_sem, r_sem, out_sem, ta_sem, tt_sem, cs_ss, cs_rs, ici_ss, ici_rs, dd_ss, dd_rs):
    me, chip, core, partner, right, left = _place(n)
    chips = n // 2
    wide = al.shape[1]
    part_w = wide // 4
    seqs = a0b.shape[0]
    a0f = u.at[pl.ds(0, seqs), :]
    quarters = range(4)
    per_step = 2 * 8
    total = (steps - 1) * per_step

    def quarter(j, cls, i):
        far = lax.rem(j + 2 + 2 * i, 4)
        qq = jnp.where(j < 2, 2 * j + i, far)
        off = jnp.where(j < 2, 0, jnp.where(j >= 6, 2, jnp.where(i == 0, chips - 1, 1)))
        c = lax.rem(chip + off, chips)
        k = jnp.where((j >= 2) & (j < 6), cls == 0, cls != 0)
        return (c * 2 + jnp.where(k, 1 - core, core)) * 4 + qq

    def a_part(b):
        return a_hbm.at[pl.ds(pl.multiple_of(b * part_w, part_w), part_w), :]

    def stream(q, slot):
        k = lax.rem(q, per_step)
        return pltpu.make_async_copy(a_part(quarter(lax.div(k, 2), 1, lax.rem(k, 2))), w.at[per_step + slot], w_sem.at[slot])

    def resident(j, i):
        return pltpu.make_async_copy(a_part(quarter(j, 0, i)), w.at[2 * j + i], r_sem.at[2 * j + i])

    def e_rows(first, count, dst, sem):
        return pltpu.make_async_copy(e_hbm.at[pl.ds(pl.multiple_of(first, 8), count), :], dst, sem)

    def e_copy(s):
        return e_rows((s - 1) * rows, rows, ebuf.at[lax.rem(s, 2)], e_sem.at[lax.rem(s, 2)])

    def al_copy(s):
        return pltpu.make_async_copy(al, al_hbm.at[pl.ds(pl.multiple_of((s - 1) * rows, 8), rows), :], out_sem.at[4])

    def mine(b):
        return g.at[b, pl.ds(0, rows), :]

    def x_copy(s, q):
        return pltpu.make_async_copy(mine(me * 4 + q), x_hbm.at[s, :, pl.ds(q * part_w, part_w)], out_sem.at[q])

    pieces, size = at_hbm.shape[0], ta.shape[1]
    fed, depth = ta.shape[0], tt.shape[0]

    def ta_copy(c):
        slot = lax.rem(c, fed)
        return pltpu.make_async_copy(a_hbm.at[pl.ds(pl.multiple_of(c * size, size), size), :], ta.at[slot], ta_sem.at[slot])

    def tt_copy(c):
        slot = lax.rem(c, depth)
        return pltpu.make_async_copy(tt.at[slot], at_hbm.at[c], tt_sem.at[slot])

    def turn(s):
        def one(c, _):
            ta_copy(c).wait()

            @pl.when(c >= depth)
            def _():
                tt_copy(c - depth).wait()

            slot = lax.rem(c, depth)
            tt[slot] = ta[lax.rem(c, fed)].T
            tt_copy(c).start()

            @pl.when(c + fed < pieces)
            def _():
                ta_copy(c + fed).start()

            return 0

        @pl.when(s == 1)
        def _():
            for c in range(fed):
                ta_copy(jnp.int32(c)).start()

        lax.fori_loop(lax.div(jnp.maximum(s - 2, 0) * pieces, steps - 2), lax.div((s - 1) * pieces, steps - 2), one, 0)

    e0_copy = e_rows((steps - 1) * rows, seqs, a0b, e_sem.at[0])
    e0_copy.start()
    _arrive(me, n)

    def load(j, _):
        for i in BOTH:
            resident(j, i).start()
        return 0

    for q in range(nbuf):
        stream(jnp.int32(q), q).start()
    lax.fori_loop(0, 2, load, 0)
    e_copy(jnp.int32(1)).start()
    tbuf[...] = jnp.zeros_like(tbuf)
    lacc[...] = jnp.zeros_like(lacc)
    if g.shape[1] > rows:
        pad = jnp.zeros((g.shape[1] - rows, part_w), jnp.bfloat16)

        def clear(k, _):
            g[k, rows:, :] = pad
            return 0

        lax.fori_loop(0, 4 * n, clear, 0)

    def ici(k, src, dst, i):
        return _remote(src, dst, ici_ss.at[k], ici_rs.at[k], left if i else right)

    def early(i):
        return ici(i, fs.at[i], fr.at[i], i)

    def own_ring(j, i):
        b = me * 4 + (j + 2 + 2 * i) % 4
        return ici(2 * (j - 2) + i, mine(b), mine(b), i)

    def relay(j, i):
        b = quarter(j, 0, i)
        return ici(2 * (j + 2) + i, mine(b), mine(b), i)

    def dd(j, cls, i):
        b = quarter(j, cls, i)
        return _remote(mine(b), mine(b), dd_ss.at[2 * j + i], dd_rs.at[2 * j + i], partner)

    lane = lax.broadcasted_iota(jnp.int32, (rows, seqs), 1).astype(jnp.float32)
    row = lax.broadcasted_iota(jnp.int32, (rows, seqs), 0).astype(jnp.float32)

    def starting(s):
        return sid_ref[s, 0:rows, :].astype(jnp.float32)

    def first_alphas(s):
        pick = (starting(s) == lane).astype(jnp.bfloat16)
        xi[...] = _dot(pick, a0b[...]).astype(jnp.bfloat16)

    def normalizer(part, count, meanwhile):
        tbuf[0:count, :] = part
        row = jnp.sum(tbuf[...].T, axis=0, keepdims=True)
        cs_send[...] = jnp.broadcast_to(row, cs_send.shape)
        cs_recv[me] = jnp.broadcast_to(row, cs_send.shape)
        cps = []
        for r in sorted(range(1, n), key=lambda r: abs(2 * r - n)):
            cp = _remote(cs_send, cs_recv.at[me], cs_ss.at[r - 1], cs_rs.at[r - 1], lax.rem(me + r, n))
            cp.start()
            cps.append(cp)
        meanwhile()
        for cp in cps:
            cp.wait()
        crow = cs_recv[0]
        for r in range(1, n):
            crow = crow + cs_recv[r]
        return crow, jnp.broadcast_to(crow[0:1, :], (LANES, LANES)).T[0:count, :]

    def add_log(s, ccol):
        slot, begin, end = info_ref[0:1, :], info_ref[1:2, :], info_ref[2:3, :]
        now = jnp.full((rows, seqs), s, jnp.int32).astype(jnp.float32)
        here = (slot == row) & (now > begin) & (now <= end)
        lacc[...] += jnp.where(here, jnp.log(jnp.where(here, ccol, 1.0)), 0.0)

    def exchange(s, then):
        own = [dd(j, 0, i) for j in BOTH for i in BOTH]
        own += [own_ring(j, i) for j in (4, 5) for i in BOTH]
        for cp in own:
            cp.start()
        then()

        def arrived(j):
            for i in BOTH:
                b = quarter(j, 0, i)
                ici(2 * (j - 2) + i, mine(b), mine(b), i).wait_recv()

        def pass_on(j):
            for i in BOTH:
                dd(j, 0, i).start()

        def rounds(h, _):
            j, k = 2 * h, 2 * h + 1

            @pl.when(h == 1)
            def _():
                for i in BOTH:
                    early(i).wait_recv()
                safe = safe_ref[...]
                for i in BOTH:
                    b = quarter(2, 0, i)
                    for cols in _spans(part_w):
                        g[b, 0:rows, cols] = (fr[i, :, cols] / safe).astype(jnp.bfloat16)
                    relay(2, i).start()
                pass_on(2)
                first_alphas(s + 1)

            @pl.when(s == 0)
            def _():
                for r in (j, k):
                    for i in BOTH:
                        resident(r, i).wait()

                    @pl.when(h < 2)
                    def _():
                        load(r + 4, 0)

            @pl.when(h >= 2)
            def _():
                arrived(j)
                pass_on(j)

            def own_class(r):
                return sum(_dot(g[quarter(r, 0, i)], w[2 * r + i]) for i in BOTH)

            def other_class(r):
                q = s * per_step + 2 * r
                slots = [lax.rem(q + i, nbuf) for i in BOTH]
                for i in BOTH:
                    dd(r, 1, i).wait_recv()
                    stream(q + i, slots[i]).wait()
                out = sum(_dot(g[quarter(r, 1, i)], w[per_step + slots[i]]) for i in BOTH)

                for i in BOTH:
                    @pl.when(q + i + nbuf < total)
                    def _():
                        stream(q + i + nbuf, slots[i]).start()

                return out

            prod = own_class(j)

            @pl.when(h >= 1)
            def _():
                arrived(k)

            @pl.when(h == 1)
            def _():
                for i in BOTH:
                    relay(3, i).start()

            @pl.when(h >= 1)
            def _():
                pass_on(k)

            u[...] += prod + own_class(k)
            u[...] += other_class(j)
            u[...] += other_class(k)
            return 0

        lax.fori_loop(0, 4, rounds, 0)
        for i in BOTH:
            early(i).wait_send()
            for j in (2, 3):
                relay(j, i).wait_send()
            for j in range(2, 8):
                dd(j, 0, i).wait_send()
        for cp in own + [own_ring(3, i) for i in BOTH]:
            cp.wait_send()

    def keep(s):
        for q in quarters:
            x_copy(s, q).start()

    e0_copy.wait()
    def lanes(q):
        return pl.ds(pl.multiple_of(q * LANES, LANES), LANES)

    def first_mass(q, part):
        a = jnp.broadcast_to(pi_ref[:, lanes(q)], (seqs, LANES)) * a0b[:, lanes(q)].astype(jnp.float32)
        a0f[:, lanes(q)] = a
        return part + a

    part = lax.fori_loop(0, wide // LANES, first_mass, jnp.zeros((seqs, LANES), jnp.float32))
    _all_here(n)

    c0_row, c0 = normalizer(part, seqs, lambda: lax.fori_loop(2, 4, load, 0))
    ll_ref[...] = jnp.log(c0_row)

    def first_alpha(q, _):
        alpha = a0f[:, lanes(q)] / c0
        a0f[:, lanes(q)] = alpha
        a0b[:, lanes(q)] = alpha.astype(jnp.bfloat16)
        return 0

    lax.fori_loop(0, wide // LANES, first_alpha, 0)
    a0_copy = pltpu.make_async_copy(a0f, al_hbm.at[pl.ds((steps - 1) * rows, seqs), :], e_sem.at[0])
    a0_copy.start()
    first_alphas(0)
    for q, cols in enumerate(_spans(wide, part_w)):
        g[me * 4 + q, 0:rows, :] = xi[:, cols]
    for i in BOTH:
        own_ring(3, i).start()
    safe_ref[...] = jnp.ones_like(safe_ref)
    for i in BOTH:
        fs[i] = xi[:, 2 * i * part_w:(2 * i + 1) * part_w].astype(jnp.float32)
        early(i).start()
    tbuf[...] = jnp.zeros_like(tbuf)
    a0_copy.wait()
    u[...] = jnp.zeros_like(u)

    def step(s, _):
        exchange(s - 1, lambda: keep(s - 1))
        e_copy(s).wait()

        @pl.when(s + 1 < steps)
        def _():
            e_copy(s + 1).start()

        @pl.when(s > 1)
        def _():
            al_copy(s - 1).wait()

        part = jnp.zeros((rows, LANES), jnp.float32)
        eb = ebuf.at[lax.rem(s, 2)]
        for cols in _spans(wide):
            a = u[0:rows, cols] * eb[:, cols].astype(jnp.float32)
            al[:, cols] = a
            part = part + a
        live = code_ref[s, 0:rows, :].astype(jnp.float32) > 0.5
        starts = starting(s) > -0.5

        def meanwhile():
            @pl.when(s + 1 < steps)
            def _():
                for i in BOTH:
                    for cols in _spans(part_w):
                        from_col = 2 * i * part_w + cols.start
                        src = slice(from_col, from_col + LANES)
                        v = jnp.where(live, al[:, src], 0.0)
                        fs[i, :, cols] = jnp.where(starts, xi[:, src].astype(jnp.float32), v)
                    early(i).start()

            turn(s)
            u[...] = jnp.zeros_like(u)

            @pl.when(s > 1)
            def _():
                add_log(s - 1, cc_ref[s - 1])

            for q in quarters:
                x_copy(s - 1, q).wait()

        _, ccol = normalizer(part, rows, meanwhile)
        cc_ref[s] = ccol
        safe = jnp.where(live, ccol, 1.0)
        safe_ref[...] = jnp.where(starts, 1.0, safe)
        blocks = _spans(wide, part_w)
        for q in (1, 3, 0, 2):
            for cols in _spans(part_w):
                src = slice(blocks[q].start + cols.start, blocks[q].start + cols.stop)
                alpha = jnp.where(live, al[:, src] / safe, 0.0)
                al[:, src] = alpha
                x = jnp.where(starts, xi[:, src].astype(jnp.float32), alpha)
                g[me * 4 + q, 0:rows, cols] = x.astype(jnp.bfloat16)

            if q % 2:
                @pl.when(s + 1 < steps)
                def _():
                    own_ring(3, q // 2).start()

        al_copy(s).start()
        return 0

    lax.fori_loop(1, steps, step, 0)
    add_log(steps - 1, cc_ref[steps - 1])
    ll_ref[...] += jnp.sum(lacc[...], axis=0, keepdims=True)
    al_copy(steps - 1).wait()
    for c in range(depth):
        tt_copy(pieces - depth + c).wait()


def _forward(n, cid, rows, a_loc, e_rows, init_loc, code, sid, info):
    wide = a_loc.shape[1]
    steps, seqs, _ = code.shape
    part_w = wide // 4
    full = max(LANES, rows)
    nbuf = 6 if rows <= 80 else 4
    f32, bf16 = jnp.float32, jnp.bfloat16
    dma = pltpu.SemaphoreType.DMA
    return pl.pallas_call(
        functools.partial(_fwd_kernel, n, steps, rows, nbuf),
        out_shape=(
            jax.ShapeDtypeStruct(((steps - 1) * rows + seqs, wide), f32),
            jax.ShapeDtypeStruct((steps - 1, rows, wide), bf16),
            jax.ShapeDtypeStruct((2 * a_loc.shape[0] // part_w, wide, part_w // 2), bf16),
            jax.ShapeDtypeStruct((steps, rows, LANES), f32),
            jax.ShapeDtypeStruct((8, LANES), f32),
        ),
        in_specs=[ANY, ANY, VMEM, VMEM, VMEM, VMEM],
        out_specs=(ANY, ANY, ANY, VMEM, VMEM),
        scratch_shapes=[
            pltpu.VMEM((4 * n, full, part_w), bf16),
            pltpu.VMEM((2 * n + nbuf, part_w, wide), bf16),
            pltpu.VMEM((full, wide), f32),
            pltpu.VMEM((rows, wide), f32),
            pltpu.VMEM((2, rows, wide), bf16),
            pltpu.VMEM((seqs, wide), bf16),
            pltpu.VMEM((rows, wide), bf16),
            pltpu.VMEM((2, rows, part_w), f32),
            pltpu.VMEM((2, rows, part_w), f32),
            pltpu.VMEM((5, part_w // 2, wide), bf16),
            pltpu.VMEM((4, wide, part_w // 2), bf16),
            pltpu.VMEM((rows, LANES), f32),
            pltpu.VMEM((rows, LANES), f32),
            pltpu.VMEM((LANES, LANES), f32),
            pltpu.VMEM((8, LANES), f32),
            pltpu.VMEM((n, 8, LANES), f32),
            dma((2,)), dma((nbuf,)), dma((2 * n,)), dma((5,)), dma((5,)), dma((4,)),
            dma((n - 1,)), dma((n - 1,)),
            dma((12,)), dma((12,)), dma((2 * n,)), dma((2 * n,)),
        ],
        compiler_params=pltpu.CompilerParams(collective_id=cid, has_side_effects=True, vmem_limit_bytes=VMEM_BYTES),
        name='forward',
    )(a_loc, e_rows, init_loc, code, sid, info)


def _bwd_kernel(n, steps, rows, nbuf, at_hbm, e_hbm, cc_ref, code_ref, w_hbm,
                w, wv, ebuf, pp, rp, rs, rin,
                e_sem, w_sem, r_sem, out_sem, dd_ss, dd_rs, ici_ss, ici_rs):
    me, chip, core, partner, right, left = _place(n)
    chips = n // 2
    wide = wv.shape[1]
    size = at_hbm.shape[2]
    per = wide // size // 2
    trips = steps - 2
    rounds_n = 4 * per
    count = 2 * rounds_n
    ringed = 6 * per
    total = trips * rounds_n

    def piece(j, cls, i):
        p, e = lax.div(j, per), lax.rem(j, per)
        hh = jnp.where(p == 1, 1 - i, i)
        off = jnp.where(p == 0, 2, jnp.where(p == 3, 0, chips - 1 if i else 1))
        c = lax.rem(chip + off, chips)
        hop = (p == 1) | (p == 2)
        k = jnp.where(hop, core if cls else 1 - core, 1 - core if cls else core)
        return (c * 2 + k) * 2 * per + hh * per + e

    def fetch(j, cls, i, slot, sem):
        return pltpu.make_async_copy(at_hbm.at[piece(j, cls, i)], w.at[slot, :, pl.ds(i * size, size)], sem)

    def stream(j, i, slot):
        return fetch(j, 1, i, rounds_n + slot, w_sem.at[slot, i])

    def resident(j, i):
        return fetch(j, 0, i, j, r_sem.at[j, i])

    def e_copy(t):
        first = pl.multiple_of((steps - 2 - t) * rows, 8)
        return pltpu.make_async_copy(e_hbm.at[pl.ds(first, rows), :], ebuf.at[lax.rem(t, 2)], e_sem.at[lax.rem(t, 2)])

    def w_copy(t):
        return pltpu.make_async_copy(wv.at[pl.ds(0, rows), :], w_hbm.at[steps - 2 - t], out_sem)

    for t in BOTH:
        e_copy(jnp.int32(t)).start()
    _arrive(me, n)

    def load(j, _):
        for i in BOTH:
            resident(j, i).start()
        return 0

    for q in BOTH:
        for i in BOTH:
            stream(jnp.int32(q), i, q).start()
        load(jnp.int32(q), 0)
    if wv.shape[0] > rows:
        wv[rows:, :] = jnp.zeros((wv.shape[0] - rows, wide), jnp.bfloat16)

    def dd(k):
        return _remote(pp.at[k], rp.at[k], dd_ss.at[k], dd_rs.at[k], partner)

    def ring(k, par, i):
        return _remote(rs.at[k], rin.at[par, k], ici_ss.at[k], ici_rs.at[par, k], left if i else right)

    def weigh(s, eb, o, beta):
        code = code_ref[s, 0:rows, :].astype(jnp.float32)
        ok = code > 2.5
        safe = jnp.where(ok, cc_ref[s], 1.0)
        for cols in _spans(size):
            dst = slice(o + cols.start, o + cols.stop)
            b = 1.0 if beta is None else jnp.where(code > 3.5, 1.0, beta[:, cols])
            v = eb[:, dst].astype(jnp.float32) * b / safe
            wv[0:rows, dst] = jnp.where(ok, v, 0.0).astype(jnp.bfloat16)

    e_copy(jnp.int32(0)).wait()
    for cols in _spans(wide, size):
        weigh(steps - 1, ebuf.at[0], cols.start, None)
    ahead = 4
    for q in range(2, nbuf):
        for i in BOTH:
            stream(jnp.int32(q), i, q).start()
    for q in range(2, ahead):
        load(jnp.int32(q), 0)
    w_copy(jnp.int32(0)).start()
    _all_here(n)

    def step(t, _):
        par = lax.rem(t, 2)

        def finish(j):
            p = lax.div(j, per)
            for i in BOTH:
                dd(2 * j + i).wait_recv()

            @pl.when(p == 2)
            def _():
                for i in BOTH:
                    k = 2 * j + i
                    c = k - 4 * per
                    ring(c, par, i).wait_recv()
                    rp[k] += rin[par, c]

            for i in BOTH:
                k = 2 * j + i
                rs[k] += rp[k]

            @pl.when(p < 3)
            def _():
                for i in BOTH:
                    ring(2 * j + i, par, i).start()

        def rounds(j, _):
            q = t * rounds_n + j
            slot = lax.rem(q, nbuf)
            for i in BOTH:
                stream(j, i, slot).wait()
            prod = _dot(wv[...], w[rounds_n + slot])
            for i, cols in enumerate(_spans(2 * size, size)):
                k = 2 * j + i
                pp[k] = prod[0:rows, cols]
                dd(k).start()

            @pl.when(q + nbuf < total)
            def _():
                for i in BOTH:
                    stream(lax.rem(j + nbuf, rounds_n), i, slot).start()

            @pl.when(j > 0)
            def _():
                finish(j - 1)

            @pl.when(t == 0)
            def _():
                for i in BOTH:
                    resident(j, i).wait()

                @pl.when(j < rounds_n - ahead)
                def _():
                    load(j + ahead, 0)

            prod = _dot(wv[...], w[j])
            for i, cols in enumerate(_spans(2 * size, size)):
                rs[2 * j + i] = prod[0:rows, cols]
            return 0

        lax.fori_loop(0, rounds_n, rounds, 0)
        finish(jnp.int32(rounds_n - 1))

        def gone(k, _):
            dd(k).wait_send()
            return 0

        def sent(k, _):
            ring(k, par, 0).wait_send()
            return 0

        lax.fori_loop(0, count, gone, 0)
        lax.fori_loop(0, 4 * per, sent, 0)
        nxt = t + 1
        e_copy(nxt).wait()

        @pl.when(nxt + 1 < steps - 1)
        def _():
            e_copy(nxt + 1).start()

        w_copy(t).wait()
        eb = ebuf.at[lax.rem(nxt, 2)]
        for e in range(per):
            for i in BOTH:
                near, late = 2 * (per + e) + 1 - i, 2 * (2 * per + e) + i
                ring(near, par, 1 - i).wait_recv()
                ring(late, par, i).wait_recv()
                beta = rs[ringed + 2 * e + i] + rin[par, near] + rin[par, late]
                weigh(steps - 1 - nxt, eb, (i * per + e) * size, beta)
        w_copy(nxt).start()
        lax.fori_loop(4 * per, ringed, sent, 0)
        return 0

    lax.fori_loop(0, trips, step, 0)
    w_copy(jnp.int32(trips)).wait()


def _backward(n, cid, at_loc, e_rows, ccol, code):
    pieces, wide, size = at_loc.shape
    steps, rows, _ = ccol.shape
    full = max(LANES, rows)
    count = pieces // 2
    nbuf = 6 if rows <= 80 else 4
    ringed = 3 * count // 4
    f32, bf16 = jnp.float32, jnp.bfloat16
    dma = pltpu.SemaphoreType.DMA
    return pl.pallas_call(
        functools.partial(_bwd_kernel, n, steps, rows, nbuf),
        out_shape=jax.ShapeDtypeStruct((steps - 1, rows, wide), bf16),
        in_specs=[ANY, ANY, VMEM, VMEM],
        out_specs=ANY,
        scratch_shapes=[
            pltpu.VMEM((count // 2 + nbuf, wide, 2 * size), bf16),
            pltpu.VMEM((full, wide), bf16),
            pltpu.VMEM((2, rows, wide), bf16),
            pltpu.VMEM((count, rows, size), f32),
            pltpu.VMEM((count, rows, size), f32),
            pltpu.VMEM((count, rows, size), f32),
            pltpu.VMEM((2, ringed, rows, size), f32),
            dma((2,)), dma((nbuf, 2)), dma((count // 2, 2)), dma(()),
            dma((count,)), dma((count,)),
            dma((ringed,)), dma((2, ringed)),
        ],
        compiler_params=pltpu.CompilerParams(collective_id=cid, has_side_effects=True, vmem_limit_bytes=VMEM_BYTES),
        name='backward',
    )(at_loc, e_rows, ccol, code)


def _pair_kernel(group_ref, a_ref, x_ref, w_ref, o_ref):
    pair_sum = lax.dot_general(x_ref[...], w_ref[...], (((0,), (0,)), ((), ())), preferred_element_type=jnp.float32)
    o_ref[...] = a_ref[...].astype(jnp.float32) * pair_sum


def _pairs(group, a_loc, xs, ws):
    depth, wide = ws.shape
    size = wide // (4 if 2 * depth < wide + LANES else 16)
    tiles = wide // size
    return pl.pallas_call(
        _pair_kernel,
        out_shape=jax.ShapeDtypeStruct((wide, wide), jnp.float32),
        grid_spec=pltpu.PrefetchScalarGridSpec(
            num_scalar_prefetch=1,
            grid=(tiles,),
            in_specs=[
                pl.BlockSpec((size, wide), lambda i, group_ref: (group_ref[0] * tiles + i, 0)),
                pl.BlockSpec((depth, size), lambda i, group_ref: (0, i)),
                pl.BlockSpec((depth, wide), lambda i, group_ref: (0, 0)),
            ],
            out_specs=pl.BlockSpec((size, wide), lambda i, group_ref: (i, 0)),
        ),
        compiler_params=pltpu.CompilerParams(vmem_limit_bytes=VMEM_BYTES),
        name='pairs',
    )(group, a_loc, xs, ws)


def _plan_kernel(options, len_ref, tok_ref, code_ref, sid_ref, look_ref, info_ref, pick_ref):
    seqs = len_ref.shape[1]
    steps = tok_ref.shape[0]
    f32, bf16 = jnp.float32, jnp.bfloat16
    square = (seqs, seqs)
    up = lax.broadcasted_iota(jnp.int32, square, 0).astype(f32)
    across = lax.broadcasted_iota(jnp.int32, square, 1).astype(f32)

    def spread(row):
        return jnp.broadcast_to(row, square)

    def total(x):
        return jnp.sum(x, axis=0, keepdims=True)

    length = len_ref[...].astype(f32)
    l_row = spread(length)
    l_col = l_row.T
    ahead = (l_col > l_row) | ((l_col == l_row) & (up < across))
    rank = total(jnp.where(ahead, 1.0, 0.0))
    rank_col = spread(rank).T

    def mates(slots):
        slot = jnp.where(rank < slots, rank, 2 * slots - 1 - rank)
        return slot, total(jnp.where(rank_col == spread(slot), l_col, 0.0))

    slots = jnp.full((1, 1), seqs, jnp.int32).astype(f32)
    pick = jnp.full((1, 1), len(options) - 1, jnp.int32)
    for k in reversed(range(len(options) - 1)):
        _, first = mates(options[k])
        worst = jnp.max(jnp.where(rank < options[k], 0.0, first + length), axis=1, keepdims=True)
        fits = worst <= steps + 1
        slots = jnp.where(fits, options[k], slots)
        pick = jnp.where(fits, k, pick)
    pick_ref[...] = pick
    slot, first = mates(slots)
    opens = rank < slots
    begin = jnp.where(opens, 0.0, first - 1)
    end = begin + length - 1
    info_ref[0:1, :] = slot
    info_ref[1:2, :] = begin
    info_ref[2:3, :] = end
    order = jax.lax.broadcasted_iota(jnp.int32, length.shape, 1).astype(f32)
    info_ref[3:4, :] = jnp.where(length < 1.5, (steps - 1) * slots + order, (end - 1) * slots + slot)

    double = total(jnp.where((spread(slot).T == spread(slot)) & (up != across), 1.0, 0.0))
    shadowed = opens & (length < 1.5) & (double > 0.5)
    home = (spread(slot) == up).astype(bf16)
    slot_col, begin_col, end_col = spread(slot).T, spread(begin).T, spread(end).T
    hidden_col = spread(jnp.where(shadowed, 1.0, 0.0)).T

    for s in range(steps):
        moves = (begin_col < s) & (end_col >= s)
        kind = jnp.where(moves, jnp.where(end_col == s, 4.0, 3.0), 0.0)
        code_ref[s] = _dot(home, kind.astype(bf16)).astype(bf16)
        number = jnp.where((begin_col == s) & (hidden_col < 0.5), up + 1, 0.0)
        sid_ref[s] = (_dot(home, number.astype(bf16)) - 1).astype(bf16)
    away = (slot_col == across).astype(bf16)
    shape = (steps, seqs)
    pos = lax.broadcasted_iota(jnp.int32, shape, 0).astype(f32) - jnp.broadcast_to(begin, shape)
    tok = jnp.zeros(shape, f32)
    for t in range(1, steps):
        there = (pos == t) & (jnp.broadcast_to(length, shape) > t)
        tok = tok + jnp.where(there, jnp.broadcast_to(tok_ref[t:t + 1, :].astype(f32), shape), 0.0)
    high = jnp.floor(tok / LANES)
    low = tok - high * LANES
    look = _dot(high.astype(bf16), away) * LANES + _dot(low.astype(bf16), away)
    look_ref[...] = look.astype(jnp.int32)


def _plan(options, lengths, tokens):
    steps, seqs = tokens.shape
    bf16 = jnp.bfloat16
    return pl.pallas_call(
        functools.partial(_plan_kernel, options),
        out_shape=(
            jax.ShapeDtypeStruct((steps, seqs, LANES), bf16),
            jax.ShapeDtypeStruct((steps, seqs, LANES), bf16),
            jax.ShapeDtypeStruct((steps, seqs), jnp.int32),
            jax.ShapeDtypeStruct((8, seqs), jnp.float32),
            jax.ShapeDtypeStruct((1, 1), jnp.int32),
        ),
        in_specs=[VMEM, VMEM],
        out_specs=(VMEM, VMEM, VMEM, VMEM, VMEM),
        name='plan',
    )(lengths[None, :], tokens)


def solution(mesh):
    n = mesh.shape['states']

    def local_run(trans_loc, emit_loc, init_loc, tokens_loc, lengths_loc):
        seqs, steps = tokens_loc.shape
        wide = trans_loc.shape[1]
        group = lax.axis_index('states').astype(jnp.int32)[None]
        options = (seqs * 9 // 16, seqs * 5 // 8, seqs)
        code, sid, look, info, pick = _plan(options, lengths_loc, tokens_loc.T)

        def run(k):
            rows = options[k]
            tokens = jnp.concatenate([look[1:, 0:rows].reshape(-1), tokens_loc[:, 0]])
            e_rows = jnp.take(emit_loc, tokens, axis=1, mode='clip').T
            al, xs, at_loc, ccol, ll = _forward(n, 2 * k, rows, trans_loc, e_rows, init_loc[None, :], code, sid, info)
            ws = _backward(n, 2 * k + 1, at_loc, e_rows, ccol, code)
            counts = _pairs(group, trans_loc, xs.reshape(-1, wide), ws.reshape(-1, wide))
            return ll[0], jnp.take(al, info[3].astype(jnp.int32), axis=0, mode='clip'), counts

        return lax.switch(pick[0, 0], [functools.partial(run, k) for k in range(len(options))])

    return jax.shard_map(local_run, mesh=mesh, in_specs=(P(None, 'states'), P('states', None), P('states'), P('seqs', None), P('seqs')), out_specs=(P('seqs'), P('seqs', 'states'), P(('seqs', 'states'), None)), check_vma=False)
```
